32 devices in a mesh: tm: 4 (over x, core), space: 8 (over z, y).
Axes of the slice: x: 2, y: 2, z: 4, core: 2. Of those that a mesh axis runs over, the one named last changes fastest.
Arguments:
- initial_state: float32 [512, 3, 512], P('space'), may hold values from -1 to 1, as said below
- applied_field: float32 [512, 3, 512], P('space'), may hold values from -2 to 2
- coupling: float32 [512, 512], P('space'), may hold values from 0.5 to 2
Outputs:
- slice_states: float32 [4, 512, 3, 512], P('tm', 'space')
The draws below stay inside these ranges and needn't reach their ends.
Inputs may be any that keep to these rules, and one draw needn't show every extreme that they name: `initial_state`: every cell's three components form a vector of length one.
All inputs are finite; a program needn't handle non-finite values.
Results may differ from the reference program's by a relative error of at most 0.00014.
Values sent between devices are 32-bit elements; how exact they have to be, the bound alone decides.
No kernel may reach another device: no remote copies, remote signals or barrier semaphores. Data moves between devices by JAX's collectives and lax.ppermute only.
A program may use at most 128 MiB of HBM per device.

```python
import math
import jax
import jax.numpy as jnp

GRID = 512
FINE = 2
ITERS = 1
SLICES = 4


def base_frame(key):
    frame_key = jax.random.fold_in(key, 7)
    sign_key, tilt_key = jax.random.split(frame_key)
    signs = (2 * jax.random.randint(sign_key, (3,), 0, 2) - 1).astype(jnp.float32)
    tilt = jax.random.uniform(tilt_key, (), jnp.float32, 0.6, 0.9)
    return (signs, tilt)


def draw_initial_state(key, part):
    signs, tilt = base_frame(key)
    noise_key = jax.random.fold_in(key, 11)
    in_plane = jnp.cos(tilt) / math.sqrt(2.0)
    base = jnp.stack([signs[0] * in_plane, signs[1] * in_plane, signs[2] * jnp.sin(tilt)]).reshape(1, 3, 1)
    noise = jax.random.uniform(noise_key, (GRID, 3, GRID), jnp.float32, -0.45, 0.45)
    vector = base + noise
    length = jnp.sqrt(jnp.sum(vector * vector, axis=1, keepdims=True))
    return vector / length


def draw_applied_field(key, part):
    signs, tilt = base_frame(key)
    noise_key = jax.random.fold_in(key, 13)
    field_scale = 2.5 / math.sqrt(2.0)
    base = jnp.stack([-signs[1] * field_scale, signs[0] * field_scale, 0.0 * field_scale]).reshape(1, 3, 1)
    noise = 0.4 * jax.random.normal(noise_key, (GRID, 3, GRID), jnp.float32)
    return jnp.clip(base + noise, -2.0, 2.0)


def shard_levels(rng, dims, cuts, low, top_value):
    def one(dim, blocks):
        steps = jax.random.uniform(jax.random.fold_in(jax.random.fold_in(rng, 6), dim), (blocks,), jnp.float32, low / len(cuts), top_value / len(cuts))
        return jnp.repeat(jnp.exp(steps), dims[dim] // blocks).reshape((-1,) + (1,) * (len(dims) - dim - 1))

    gain = one(*cuts[0])
    for cut in cuts[1:]:
        gain = gain * one(*cut)
    return gain


def setup_inputs(seed: int = 0) -> dict:
    arg_keys = jax.random.split(jax.random.key(seed), 4)
    initial_state = draw_initial_state(jax.random.fold_in(arg_keys[3], 71), 0)
    applied_field = draw_applied_field(jax.random.fold_in(arg_keys[3], 71), 0)
    coupling = jnp.clip(jnp.exp(math.log(2.0) - 1.3862944 * jax.random.uniform(arg_keys[2], (GRID, GRID), jnp.float32) ** shard_levels(arg_keys[2], (GRID, GRID), ((0, 8),), -0.2, 0.2)), 0.5, 2.0)
    return dict(initial_state=initial_state, applied_field=applied_field, coupling=coupling)


step_time = 0.06
damping = 0.02
stiffness = 0.25
thickness = 8.0

def spectral_tensor(row_index, column_index, length):
    half_length = length // 2
    signed_rows = jnp.where(row_index < half_length, row_index, row_index - length).astype(jnp.float32)
    signed_columns = jnp.where(column_index < half_length, column_index, column_index - length).astype(jnp.float32)
    wave_rows = 2.0 * math.pi / length * signed_rows[:, None]
    wave_columns = 2.0 * math.pi / length * signed_columns[None, :]
    squared = wave_rows * wave_rows + wave_columns * wave_columns
    nonzero = squared > 0.0
    safe_square = jnp.where(nonzero, squared, 1.0)
    scaled_wave = jnp.sqrt(safe_square) * thickness
    film_factor = jnp.where(nonzero, (1.0 - jnp.exp(-scaled_wave)) / scaled_wave, 1.0)
    in_plane = (1.0 - film_factor) / safe_square
    nyquist = (row_index[:, None] == half_length) | (column_index[None, :] == half_length)
    normalizer = -1.0 / (length * length)
    tensor_first = in_plane * wave_columns * wave_columns * normalizer
    tensor_second = in_plane * wave_rows * wave_rows * normalizer
    tensor_cross = jnp.where(nyquist, 0.0, in_plane * wave_columns * wave_rows) * normalizer
    tensor_normal = film_factor * normalizer
    return (tensor_first, tensor_second, tensor_cross, tensor_normal)

def exchange_field(padded_state, padded_coupling):
    center_state = padded_state[1:-1]
    center_coupling = padded_coupling[1:-1]
    wide_state = jnp.pad(padded_state, ((0, 0), (0, 0), (1, 1)))
    wide_coupling = jnp.pad(padded_coupling, ((0, 0), (1, 1)))
    neighbour_sum = padded_coupling[2:, None, :] * (padded_state[2:] - center_state)
    neighbour_sum = neighbour_sum + padded_coupling[:-2, None, :] * (padded_state[:-2] - center_state)
    neighbour_sum = neighbour_sum + wide_coupling[1:-1, None, 2:] * (wide_state[1:-1, :, 2:] - center_state)
    neighbour_sum = neighbour_sum + wide_coupling[1:-1, None, :-2] * (wide_state[1:-1, :, :-2] - center_state)
    return stiffness * center_coupling[:, None, :] * neighbour_sum

def torque(magnet, effective):
    first_cross = jnp.cross(magnet, effective, axis=1)
    second_cross = jnp.cross(magnet, first_cross, axis=1)
    return -(first_cross + damping * second_cross) / (1.0 + damping * damping)

def demag_field(magnet):
    padded = jnp.pad(magnet, ((0, GRID), (0, 0), (0, GRID)))
    spectrum = jnp.fft.fft2(padded, axes=(0, 2))
    index_all = jnp.arange(2 * GRID, dtype=jnp.int32)
    tensor_first, tensor_second, tensor_cross, tensor_normal = spectral_tensor(index_all, index_all, 2 * GRID)
    first_out = tensor_first * spectrum[:, 0] + tensor_cross * spectrum[:, 1]
    second_out = tensor_cross * spectrum[:, 0] + tensor_second * spectrum[:, 1]
    third_out = tensor_normal * spectrum[:, 2]
    combined = jnp.stack([first_out, second_out, third_out], axis=1)
    result = jnp.fft.ifft2(combined, axes=(0, 2)) * float(2 * GRID * (2 * GRID))
    return jnp.real(result)[:GRID, :, :GRID].astype(jnp.float32)

def effective_fine(magnet, applied_field, padded_coupling):
    padded_state = jnp.pad(magnet, ((1, 1), (0, 0), (0, 0)))
    return exchange_field(padded_state, padded_coupling) + demag_field(magnet) + applied_field

def propagate_fine(magnet, applied_field, padded_coupling):
    for repeat in range(FINE):
        first_rate = torque(magnet, effective_fine(magnet, applied_field, padded_coupling))
        predicted = magnet + step_time * first_rate
        second_rate = torque(predicted, effective_fine(predicted, applied_field, padded_coupling))
        magnet = magnet + 0.5 * step_time * (first_rate + second_rate)
    return magnet

def propagate_coarse(magnet, applied_field, padded_coupling):
    padded_state = jnp.pad(magnet, ((1, 1), (0, 0), (0, 0)))
    local_demag = jnp.array([0.0, 0.0, -1.0], dtype=jnp.float32).reshape(1, 3, 1)
    effective = exchange_field(padded_state, padded_coupling) + applied_field + magnet * local_demag
    return magnet + FINE * step_time * torque(magnet, effective)

def coarse_sweep(differences, initial_state, applied_field, padded_coupling):
    current = initial_state
    starts = []
    coarse_ends = []
    slice_ends = []
    for slice_number in range(SLICES):
        predicted = propagate_coarse(current, applied_field, padded_coupling)
        advanced = predicted + differences[slice_number]
        starts.append(current)
        coarse_ends.append(predicted)
        slice_ends.append(advanced)
        current = advanced
    return (starts, coarse_ends, slice_ends)

def reference(initial_state, applied_field, coupling):
    padded_coupling = jnp.pad(coupling, ((1, 1), (0, 0)))
    differences = [jnp.zeros_like(initial_state) for slice_number in range(SLICES)]
    starts, coarse_ends, slice_ends = coarse_sweep(differences, initial_state, applied_field, padded_coupling)
    for iteration in range(ITERS):
        differences = [propagate_fine(starts[slice_number], applied_field, padded_coupling) - coarse_ends[slice_number] for slice_number in range(SLICES)]
        starts, coarse_ends, slice_ends = coarse_sweep(differences, initial_state, applied_field, padded_coupling)
    return jnp.stack(slice_ends, axis=0)
```

```python
import functools
import math

import jax
import jax.numpy as jnp
from jax import lax
from jax.experimental import pallas as pl
from jax.experimental.pallas import tpu as pltpu
from jax.sharding import Mesh
from jax.sharding import PartitionSpec as P

FINE = 2
VMEM_LIMIT = 32 * 1024 * 1024


step_time = 0.06
damping = 0.02
stiffness = 0.25
thickness = 8.0


def with_halo(x, sides, width):
    for axis, dim in sides:
        peers, length = (lax.axis_size(axis), x.shape[dim])
        up = [(i, (i + 1) % peers) for i in range(peers - 1)]
        down = [(j, i) for i, j in up]
        last = lax.slice_in_dim(x, length - width, length, axis=dim)
        initial = lax.slice_in_dim(x, 0, width, axis=dim)
        before = lax.ppermute(last, axis, up)
        after = lax.ppermute(initial, axis, down)
        x = jnp.concatenate([before, x, after], axis=dim)
    return x


def passed_along(block, axis, distance):
    devices = range(lax.axis_size(axis))
    route = [(i - distance, i) for i in devices if i - distance in devices]
    return lax.ppermute(block, axis, route)


def spectral_tensor(row_index, column_index, length):
    half_length = length // 2
    signed_rows = jnp.where(row_index < half_length, row_index, row_index - length).astype(
        jnp.float32
    )
    signed_columns = jnp.where(
        column_index < half_length, column_index, column_index - length
    ).astype(jnp.float32)
    wave_rows = 2.0 * math.pi / length * signed_rows[:, None]
    wave_columns = 2.0 * math.pi / length * signed_columns[None, :]
    squared = wave_rows * wave_rows + wave_columns * wave_columns
    nonzero = squared > 0.0
    safe_square = jnp.where(nonzero, squared, 1.0)
    scaled_wave = jnp.sqrt(safe_square) * thickness
    film_factor = jnp.where(nonzero, (1.0 - jnp.exp(-scaled_wave)) / scaled_wave, 1.0)
    in_plane = (1.0 - film_factor) / safe_square
    nyquist = (row_index[:, None] == half_length) | (column_index[None, :] == half_length)
    normalizer = -1.0 / (length * length)
    tensor_first = in_plane * wave_columns * wave_columns * normalizer
    tensor_second = in_plane * wave_rows * wave_rows * normalizer
    tensor_cross = jnp.where(nyquist, 0.0, in_plane * wave_columns * wave_rows) * normalizer
    tensor_normal = film_factor * normalizer
    return (tensor_first, tensor_second, tensor_cross, tensor_normal)


def exchange_field(padded_state, padded_coupling):
    center_state = padded_state[1:-1]
    center_coupling = padded_coupling[1:-1]
    wide_state = jnp.pad(padded_state, ((0, 0), (0, 0), (1, 1)))
    wide_coupling = jnp.pad(padded_coupling, ((0, 0), (1, 1)))
    neighbour_sum = padded_coupling[2:, None, :] * (padded_state[2:] - center_state)
    neighbour_sum = neighbour_sum + padded_coupling[:-2, None, :] * (
        padded_state[:-2] - center_state
    )
    neighbour_sum = neighbour_sum + wide_coupling[1:-1, None, 2:] * (
        wide_state[1:-1, :, 2:] - center_state
    )
    neighbour_sum = neighbour_sum + wide_coupling[1:-1, None, :-2] * (
        wide_state[1:-1, :, :-2] - center_state
    )
    return stiffness * center_coupling[:, None, :] * neighbour_sum


def torque(magnet, effective):
    first_cross = jnp.cross(magnet, effective, axis=1)
    second_cross = jnp.cross(magnet, first_cross, axis=1)
    return -(first_cross + damping * second_cross) / (1.0 + damping * damping)


def phase_table(row_count, column_count, period, direction):
    row_ids = lax.broadcasted_iota(jnp.int32, (row_count, column_count), 0)
    column_ids = lax.broadcasted_iota(jnp.int32, (row_count, column_count), 1)
    angles = (row_ids * column_ids % period).astype(jnp.float32) * (2.0 * math.pi / period)
    return (jnp.cos(angles), direction * jnp.sin(angles))


def joined_table(row_count, column_count, period, direction):
    table_cos, table_sin = phase_table(row_count, column_count, period, direction)
    return jnp.concatenate([table_cos, table_sin], axis=1)


def contract(pattern, left, right):
    return jnp.einsum(pattern, left, right, precision=lax.Precision.HIGHEST)


def complex_apply(pattern, real_part, imag_part, joined):
    half_width = joined.shape[-1] // 2
    real_both = contract(pattern, real_part, joined)
    imag_both = contract(pattern, imag_part, joined)
    return (
        real_both[..., :half_width] - imag_both[..., half_width:],
        real_both[..., half_width:] + imag_both[..., :half_width],
    )


def apply_tensor(real_part, imag_part, tensor):
    tensor_first, tensor_second, tensor_cross, tensor_normal = tensor

    def mix_components(values):
        return jnp.stack(
            [
                tensor_first * values[0] + tensor_cross * values[1],
                tensor_cross * values[0] + tensor_second * values[1],
                tensor_normal * values[2],
            ],
            axis=0,
        )

    return (mix_components(real_part), mix_components(imag_part))


def shards(initial_state, applied_field, coupling):
    row_count, component_count, grid_size = initial_state.shape
    length = 2 * grid_size
    space_count = lax.axis_size("space")
    space_index = lax.axis_index("space")
    slice_count = lax.axis_size("tm")
    slice_index = lax.axis_index("tm")
    is_first = slice_index == 0
    padded_coupling = with_halo(coupling, (("space", 0),), 1)
    index_all = jnp.arange(length, dtype=jnp.int32)
    local_demag = jnp.array([0.0, 0.0, -1.0], dtype=jnp.float32).reshape(1, 3, 1)
    forward_y = joined_table(grid_size, length, length, -1.0)
    inverse_y = joined_table(length, grid_size, length, 1.0)

    def transform_columns(real_part, imag_part):
        return complex_apply("yca,yk->cak", real_part, imag_part, forward_y)

    column_width = grid_size // space_count
    columns = space_index * column_width + jnp.arange(column_width, dtype=jnp.int32)
    tensor = tuple((part_table.T for part_table in spectral_tensor(index_all, columns, length)))
    edge_first, edge_second, edge_cross, edge_normal = spectral_tensor(
        index_all, jnp.array([0, grid_size], dtype=jnp.int32), length
    )
    anchor_diag = jnp.stack([edge_first[:, 0], edge_second[:, 0], edge_normal[:, 0]], axis=0)
    nyquist_diag = jnp.stack([edge_first[:, 1], edge_second[:, 1], edge_normal[:, 1]], axis=0)
    mean_diag = 0.5 * (anchor_diag + nyquist_diag)
    half_gap = 0.5 * (anchor_diag - nyquist_diag)
    is_anchor = (columns == 0)[None, :, None]
    column_ids = jnp.arange(grid_size, dtype=jnp.int32)
    is_lead = column_ids == 0
    lead_columns = is_lead[None, :, None]
    alternating = jnp.where(column_ids % 2 == 0, 1.0, -1.0).astype(jnp.float32)
    forward_x = joined_table(grid_size, grid_size, length, -1.0)
    inverse_x_cos, inverse_x_sin = phase_table(grid_size, grid_size, length, 1.0)

    def demag_field(magnet):
        both_parts = contract("rcx,xk->rck", magnet, forward_x)
        packed_real = both_parts[..., :grid_size]
        imag_part = both_parts[..., grid_size:]
        nyquist_column = jnp.einsum(
            "rcx,x->rc", magnet, alternating, precision=lax.Precision.HIGHEST
        )
        packed_imag = jnp.where(is_lead, nyquist_column[:, :, None], imag_part)
        real_part, imag_part = (
            lax.all_to_all(packed_real, "space", split_axis=2, concat_axis=0, tiled=True),
            lax.all_to_all(packed_imag, "space", split_axis=2, concat_axis=0, tiled=True),
        )
        real_part, imag_part = transform_columns(real_part, imag_part)
        out_real, out_imag = apply_tensor(real_part, imag_part, tensor)
        lead_real = real_part[:, 0, :]
        lead_imag = imag_part[:, 0, :]
        mirror_real = jnp.concatenate([lead_real[:, :1], lead_real[:, 1:][:, ::-1]], axis=1)
        mirror_imag = jnp.concatenate([lead_imag[:, :1], lead_imag[:, 1:][:, ::-1]], axis=1)
        fixed_real = mean_diag * lead_real + half_gap * mirror_real
        fixed_imag = mean_diag * lead_imag - half_gap * mirror_imag
        out_real = jnp.where(is_anchor, fixed_real[:, None, :], out_real)
        out_imag = jnp.where(is_anchor, fixed_imag[:, None, :], out_imag)
        out_real, out_imag = complex_apply("cak,ky->cay", out_real, out_imag, inverse_y)
        out_real, out_imag = (
            lax.all_to_all(out_real, "space", split_axis=2, concat_axis=1, tiled=True),
            lax.all_to_all(out_imag, "space", split_axis=2, concat_axis=1, tiled=True),
        )
        nyquist_part = jnp.transpose(out_imag[:, :1, :], (2, 0, 1))
        doubled_real = jnp.where(lead_columns, out_real, 2.0 * out_real)
        doubled_imag = jnp.where(lead_columns, 0.0, 2.0 * out_imag)
        result = contract("cxr,xo->rco", doubled_real, inverse_x_cos) - contract(
            "cxr,xo->rco", doubled_imag, inverse_x_sin
        )
        return result + nyquist_part * alternating

    def effective_fine(state_now):
        padded_state = with_halo(state_now, (("space", 0),), 1)
        return (
            exchange_field(padded_state, padded_coupling) + demag_field(state_now) + applied_field
        )

    def propagate_coarse(magnet):
        padded_state = with_halo(magnet, (("space", 0),), 1)
        effective = (
            exchange_field(padded_state, padded_coupling) + applied_field + magnet * local_demag
        )
        return magnet + FINE * step_time * torque(magnet, effective)

    def coarse_sweep(jump_term):

        def one_turn(turn_index, loop_state):
            start_state, coarse_end, slice_end = loop_state
            start_state = jnp.where(is_first, initial_state, passed_along(slice_end, "tm", 1))
            coarse_end = propagate_coarse(start_state)
            return (start_state, coarse_end, coarse_end + jump_term)

        coarse_end = propagate_coarse(initial_state)
        return lax.fori_loop(
            0, slice_count - 1, one_turn, (initial_state, coarse_end, coarse_end + jump_term)
        )

    start_state, coarse_end, slice_end = coarse_sweep(jnp.zeros_like(initial_state))
    magnet = start_state
    for repeat in range(FINE):
        first_rate = torque(magnet, effective_fine(magnet))
        predicted = magnet + step_time * first_rate
        second_rate = torque(predicted, effective_fine(predicted))
        magnet = magnet + 0.5 * step_time * (first_rate + second_rate)
    jump_term = magnet - coarse_end
    start_state, coarse_end, slice_end = coarse_sweep(jump_term)
    return slice_end[None]


def turn_tables(grid, product):
    angle = (product % (4 * grid)).astype(jnp.float32) * (math.pi / (2 * grid))
    return (jnp.cos(angle), jnp.sin(angle))


def addition_tables(grid, coarse, fine, sine):
    coarse_cos, coarse_sin = turn_tables(grid, coarse)
    fine_cos, fine_sin = turn_tables(grid, fine)
    lead = jnp.where(sine, coarse_sin, coarse_cos)
    side = jnp.where(sine, coarse_cos, -coarse_sin)
    return (lead, side, fine_cos, fine_sin)


def small_tables(rank, grid, peers, halo):
    width = grid // peers
    lane = jnp.arange(2 * grid, dtype=jnp.int32)
    peer = (lane // (2 * width)) ^ rank
    sine = (lane % (2 * width)) >= width
    wave = peer * width + lane % width
    wave = jnp.where(sine & (wave == 0), grid, wave)[None, :]
    sixteens = 16 * jnp.arange(grid // 16, dtype=jnp.int32)[:, None]
    ones = jnp.arange(16, dtype=jnp.int32)[:, None]
    row = addition_tables(
        grid, 2 * sixteens * wave, (2 * ones - (grid - 1)) * wave, sine[None, :]
    )

    base = jnp.where(rank < peers // 2, rank, peers - 1 - rank)
    spot = jnp.arange(grid // 2, dtype=jnp.int32)
    place = (2 * (((spot // width) ^ base) * width + spot % width) - (grid - 1))[None, :]
    column_cos = addition_tables(grid, sixteens * place, ones * place, False)
    column_sin = addition_tables(grid, sixteens * place, ones * place, True)
    edge = turn_tables(grid, grid * place)[1]

    number = jnp.arange(grid, dtype=jnp.int32)[None, :]
    number_sin = jnp.where(number == 0, grid, number)
    span = 16 * jnp.arange((grid // 2 + 2 * halo) // 16, dtype=jnp.int32)[:, None]
    start = 2 * (ones - halo) - (grid - 1)
    back_cos = addition_tables(grid, 2 * span * number, start * number, False)
    back_sin = addition_tables(grid, 2 * span * number_sin, start * number_sin, True)
    sign = jnp.where(rank < peers // 2, 1.0, -1.0).astype(jnp.float32)
    column_sin = (sign * column_sin[0], sign * column_sin[1]) + column_sin[2:]
    back_sin = (sign * back_sin[0], sign * back_sin[1]) + back_sin[2:]
    return row + column_cos + column_sin + back_cos + back_sin + (sign * edge,)


def tables_body(*refs):
    factors, outs = (refs[:21], refs[21:])
    edge_ref = factors[20]
    for number in range(5):
        lead_ref, side_ref, first_ref, second_ref = factors[4 * number : 4 * number + 4]
        first, second = (first_ref[...], second_ref[...])
        out_ref = outs[number]
        for block in range(lead_ref.shape[0]):
            values = lead_ref[block : block + 1] * first + side_ref[block : block + 1] * second
            if number == 2 and block == 0:
                top = lax.broadcasted_iota(jnp.int32, values.shape, 0) == 0
                values = jnp.where(top, edge_ref[...], values)
            high, low = split(values)
            out_ref[0, 16 * block : 16 * block + 16] = high
            out_ref[1, 16 * block : 16 * block + 16] = low


def weighted_tensor(rank, grid, width):
    own = rank * width + jnp.arange(width, dtype=jnp.int32)
    columns = jnp.concatenate([own, jnp.where(own == 0, grid, own)])
    rows_cos = jnp.arange(grid, dtype=jnp.int32)
    rows_sin = jnp.where(rows_cos == 0, grid, rows_cos)
    row_weight = jnp.where(rows_cos == 0, 1.0, 2.0)[:, None]
    column_weight = jnp.where(columns % grid == 0, 1.0, 2.0)[None, :]
    weight = (row_weight * column_weight).astype(jnp.float32)
    side = jnp.where(jnp.arange(2 * width) < width, 1.0, -1.0).astype(jnp.float32)
    c_first, c_second, c_cross, c_normal = spectral_tensor(rows_cos, columns, 2 * grid)
    s_first, s_second, _, s_normal = spectral_tensor(rows_sin, columns, 2 * grid)
    return jnp.stack(
        [
            c_first * weight,
            c_second * weight,
            c_normal * weight,
            s_first * weight,
            s_second * weight,
            s_normal * weight,
            c_cross * weight * side,
        ]
    )


def split(values):
    high = values.astype(jnp.bfloat16)
    low = (values - high.astype(jnp.float32)).astype(jnp.bfloat16)
    return (high, low)


def multiply(left, right, transposed=False):
    numbers = (((1,), (1 if transposed else 0,)), ((), ()))

    def one(a, b):
        return lax.dot_general(a, b, numbers, preferred_element_type=jnp.float32)

    return one(left[0], right[0]) + (one(left[0], right[1]) + one(left[1], right[0]))


def exchange_weights(coupling):
    rows, columns = coupling.shape
    place = lax.broadcasted_iota(jnp.int32, coupling.shape, 1)
    own = stiffness * coupling
    right = jnp.where(place < columns - 1, pltpu.roll(coupling, columns - 1, 1), 0.0)
    left = jnp.where(place > 0, pltpu.roll(coupling, 1, 1), 0.0)
    below = pltpu.roll(coupling, rows - 1, 0)
    above = pltpu.roll(coupling, 1, 0)
    return (own * right, own * left, own * below, own * above)


def exchange_of(part, weights):
    rows, columns = part.shape
    right, left, below, above = weights
    total = right * (pltpu.roll(part, columns - 1, 1) - part)
    total = total + left * (pltpu.roll(part, 1, 1) - part)
    total = total + below * (pltpu.roll(part, rows - 1, 0) - part)
    return total + above * (pltpu.roll(part, 1, 0) - part)


def cross(a, b):
    return (a[1] * b[2] - a[2] * b[1], a[2] * b[0] - a[0] * b[2], a[0] * b[1] - a[1] * b[0])


def torque_of(magnet, effective):
    first = cross(magnet, effective)
    second = cross(magnet, first)
    scale = -1.0 / (1.0 + damping * damping)
    return [scale * (a + damping * b) for a, b in zip(first, second)]


def coarse_step(magnet, applied, weights):
    effective = [exchange_of(part, weights) + field for part, field in zip(magnet, applied)]
    effective[2] = effective[2] - magnet[2]
    return [part + FINE * step_time * rate for part, rate in zip(magnet, torque_of(magnet, effective))]


def vmem_call(body, outs, name, scalars=0, scratch=(), cost=10**8):
    whole = pl.BlockSpec(memory_space=pltpu.VMEM)

    def call(*args):
        first = [pl.BlockSpec(memory_space=pltpu.SMEM)] * scalars
        return pl.pallas_call(
            body,
            out_shape=[
                out if isinstance(out, jax.ShapeDtypeStruct) else jax.ShapeDtypeStruct(out, jnp.float32)
                for out in outs
            ],
            in_specs=first + [whole] * (len(args) - scalars),
            out_specs=[whole] * len(outs),
            scratch_shapes=[pltpu.VMEM(shape, jnp.float32) for shape in scratch],
            compiler_params=pltpu.CompilerParams(vmem_limit_bytes=VMEM_LIMIT),
            cost_estimate=pl.CostEstimate(flops=cost, bytes_accessed=10**6, transcendentals=0),
            name=name,
        )(*args)

    return call


def pack_body(reach, state_ref, applied_ref, coupling_ref, top_ref, bottom_ref):
    rows = coupling_ref.shape[0]
    for ref, rng in ((top_ref, slice(0, reach)), (bottom_ref, slice(rows - reach, rows))):
        for c in range(3):
            ref[c * reach : (c + 1) * reach] = state_ref[c, rng]
            ref[(3 + c) * reach : (4 + c) * reach] = applied_ref[c, rng]
        ref[6 * reach : 7 * reach] = coupling_ref[rng]
        ref[7 * reach :] = jnp.zeros_like(ref[7 * reach :])


def pieces(values):
    high = values.astype(jnp.bfloat16)
    rest = values - high.astype(jnp.float32)
    middle = rest.astype(jnp.bfloat16)
    low = (rest - middle.astype(jnp.float32)).astype(jnp.bfloat16)
    return (high, middle, low)


def choose(selection, parts):
    first, second, third = (
        jnp.dot(selection, part, preferred_element_type=jnp.float32) for part in parts
    )
    return first + (second + third)


def start_body(
    reach, halo, slices, place_ref, state_ref, applied_ref, coupling_ref, before_ref, after_ref,
    first_ref, around_ref, wide_ref,
):
    turn, flipped = (place_ref[0], place_ref[1])
    rows = coupling_ref.shape[0]
    total = wide_ref.shape[1]
    margin = (total - rows) // 2

    def selection(count, base):
        row = lax.broadcasted_iota(jnp.int32, (total, count), 0)
        row = jnp.where(flipped == 1, total - 1 - row, row)
        column = lax.broadcasted_iota(jnp.int32, (total, count), 1)
        return (row, column, base)

    def matrix(chosen, low, high):
        row, column, base = chosen
        inside = (column >= low) & (column < high) & (row == column - low + base)
        return jnp.where(inside, 1.0, 0.0).astype(jnp.bfloat16)

    own = matrix(selection(rows, margin), 0, rows)
    before, after = (pieces(before_ref[...]), pieces(after_ref[...]))
    count = before_ref.shape[0]
    fields = [state_ref[c] for c in range(3)] + [applied_ref[c] for c in range(3)]
    fields.append(coupling_ref[...])
    for number, field in enumerate(fields):
        low, high = (number * reach, (number + 1) * reach)
        wide_ref[number] = (
            choose(own, pieces(field))
            + choose(matrix(selection(count, margin - reach), low, high), before)
            + choose(matrix(selection(count, margin + rows), low, high), after)
        )
    kept = slice(margin - halo, margin + rows + halo)
    for c in range(4):
        around_ref[c] = wide_ref[3 + c, kept]
    weights = exchange_weights(wide_ref[6])
    applied = [wide_ref[3 + c] for c in range(3)]
    magnet = [wide_ref[c] for c in range(3)]
    for number in range(slices):
        @pl.when(turn == number)
        def keep():
            for c in range(3):
                first_ref[c] = magnet[c][kept]

        if number < slices - 1:
            magnet = coarse_step(magnet, applied, weights)


def send_rows(magnet, halo, table, out_refs):
    rows = magnet[0].shape[0] - 2 * halo
    width = out_refs[0].shape[2]
    block = split(jnp.concatenate([part[halo : halo + rows] for part in magnet], axis=0))
    spectrum = multiply(block, table)
    for slot, out_ref in enumerate(out_refs):
        for c in range(3):
            out_ref[c] = spectrum[c * rows : (c + 1) * rows, slot * width : (slot + 1) * width]


def rows_body(halo, state_ref, table_ref, *out_refs):
    send_rows([state_ref[c] for c in range(3)], halo, (table_ref[0], table_ref[1]), out_refs)


def spectrum_body(peers, skip, base_ref, *refs):
    in_refs, refs = (refs[:peers], refs[peers:])
    tensor_ref, cos_ref, sin_ref, back_cos_ref, back_sin_ref = refs[:5]
    out_refs = refs[5 : 5 + peers]
    front_ref, back_ref = refs[5 + peers :]
    _, rows, width = in_refs[0].shape
    window = out_refs[0].shape[1]
    half = peers // 2

    def fold(sign):
        return jnp.concatenate(
            [
                jnp.concatenate(
                    [in_refs[p][c] + sign * in_refs[peers - 1 - p][c] for p in range(half)], axis=0
                )
                for c in range(3)
            ],
            axis=1,
        )

    even = multiply((cos_ref[0], cos_ref[1]), split(fold(1.0)))
    odd = multiply((sin_ref[0], sin_ref[1]), split(fold(-1.0)))
    even_x, even_y, even_z = (even[:, c * width : (c + 1) * width] for c in range(3))
    odd_x, odd_y, odd_z = (odd[:, c * width : (c + 1) * width] for c in range(3))
    mixed = tensor_ref[6]

    def turned(values):
        return mixed * pltpu.roll(values, width // 2, 1)

    even_out = jnp.concatenate(
        [
            tensor_ref[0] * even_x - turned(odd_y),
            tensor_ref[1] * even_y - turned(odd_x),
            tensor_ref[2] * even_z,
        ],
        axis=1,
    )
    odd_out = jnp.concatenate(
        [
            tensor_ref[3] * odd_x + turned(even_y),
            tensor_ref[4] * odd_y + turned(even_x),
            tensor_ref[5] * odd_z,
        ],
        axis=1,
    )
    even_rows = multiply((back_cos_ref[0], back_cos_ref[1]), split(even_out))
    odd_rows = multiply((back_sin_ref[0], back_sin_ref[1]), split(odd_out))
    kept = slice(skip, even_rows.shape[0] - skip)
    front_ref[...] = (even_rows + odd_rows)[kept]
    back_ref[...] = (even_rows - odd_rows)[kept]
    base = base_ref[0]
    for p in range(half):
        span = pl.ds(pl.multiple_of((base ^ p) * rows, 8), window)
        for c in range(3):
            out_refs[p][c] = front_ref[span, c * width : (c + 1) * width]
            out_refs[peers - 1 - p][c] = back_ref[span, c * width : (c + 1) * width]


def field_rates(in_refs, magnet, applied, coupling, table):
    rows = in_refs[0].shape[1]
    spectrum = jnp.concatenate(
        [jnp.concatenate([ref[c] for c in range(3)], axis=0) for ref in in_refs], axis=1
    )
    demag = multiply(split(spectrum), table, transposed=True)
    weights = exchange_weights(coupling)
    effective = [
        exchange_of(magnet[c], weights) + demag[c * rows : (c + 1) * rows] + applied[c]
        for c in range(3)
    ]
    return torque_of(magnet, effective)


def inner_rows(ref, number, rows):
    skip = (ref.shape[1] - rows) // 2
    return ref[number, skip : skip + rows]


def predict_body(peers, halo, *refs):
    in_refs, refs = (refs[:peers], refs[peers:])
    state_ref, around_ref, table_ref = refs[:3]
    send_refs, (predicted_ref, base_ref) = (refs[3 : 3 + peers], refs[3 + peers :])
    rows = in_refs[0].shape[1]
    table = (table_ref[0], table_ref[1])
    magnet = [inner_rows(state_ref, c, rows) for c in range(3)]
    around = [inner_rows(around_ref, c, rows) for c in range(4)]
    rates = field_rates(in_refs, magnet, around[:3], around[3], table)
    predicted = [part + step_time * rate for part, rate in zip(magnet, rates)]
    send_rows(predicted, halo, table, send_refs)
    for c in range(3):
        predicted_ref[c] = predicted[c]
        base_ref[c] = magnet[c] + 0.5 * step_time * rates[c]


def correct_body(peers, halo, *refs):
    in_refs, refs = (refs[:peers], refs[peers:])
    state_ref, base_ref, around_ref, table_ref = refs[:4]
    send_refs, following_ref = (refs[4 : 4 + peers], refs[4 + peers])
    rows = in_refs[0].shape[1]
    table = (table_ref[0], table_ref[1])
    magnet = [state_ref[c] for c in range(3)]
    around = [inner_rows(around_ref, c, rows) for c in range(4)]
    rates = field_rates(in_refs, magnet, around[:3], around[3], table)
    following = [base_ref[c] + 0.5 * step_time * rates[c] for c in range(3)]
    send_rows(following, halo, table, send_refs)
    for c in range(3):
        following_ref[c] = following[c]


def end_body(peers, share, number_ref, *refs):
    in_refs, refs = (refs[:peers], refs[peers:])
    state_ref, base_ref, around_ref, table_ref = refs[:4]
    out_refs, end_ref = (refs[4:-1], refs[-1])
    rows = in_refs[0].shape[1]
    magnet = [state_ref[c] for c in range(3)]
    around = [inner_rows(around_ref, c, rows) for c in range(4)]
    rates = field_rates(in_refs, magnet, around[:3], around[3], (table_ref[0], table_ref[1]))
    for c in range(3):
        end_ref[c] = base_ref[c] + 0.5 * step_time * rates[c]
    for t, out_ref in enumerate(out_refs):
        start = pl.multiple_of((number_ref[0] ^ t) * share, 8)
        for c in range(3):
            out_ref[c] = end_ref[c, pl.ds(start, out_ref.shape[1])]


def finish_body(slices, trim, turn_ref, *refs):
    in_refs, wide_ref = (refs[:slices], refs[slices])
    out_refs = refs[slices + 1 : 2 * slices + 1]
    fine_ref, end_ref = refs[2 * slices + 1 :]
    turn = turn_ref[0]
    rows = fine_ref.shape[2]
    share = rows - 2 * trim
    for t in range(slices):
        fine_ref[turn ^ t] = in_refs[t][...]
    margin = (wide_ref.shape[1] - slices * share) // 2
    start = pl.multiple_of(turn * share + margin - 8, 8)

    def strip(number):
        return wide_ref[number, pl.ds(start, share + 16)][8 - trim : 8 + share + trim]

    weights = exchange_weights(strip(6))
    applied = [strip(3 + c) for c in range(3)]
    first = [strip(c) for c in range(3)]
    magnet = first
    for number in range(slices):
        first = coarse_step(first, applied, weights)
        ahead = coarse_step(magnet, applied, weights) if number > 0 else first
        magnet = [ahead[c] + (fine_ref[number, c] - first[c]) for c in range(3)]
        for c in range(3):
            end_ref[number, c] = magnet[c][trim : trim + share]
    for t in range(slices):
        out_refs[t][...] = end_ref[turn ^ t]


def gather_body(slices, place_ref, *refs):
    in_refs, out_ref = (refs[:slices], refs[slices])
    turn, flipped = (place_ref[0], place_ref[1])
    share = in_refs[0].shape[1]
    row = lax.broadcasted_iota(jnp.int32, (share, share), 0)
    column = lax.broadcasted_iota(jnp.int32, (share, share), 1)
    row = jnp.where(flipped == 1, share - 1 - row, row)
    matrix = jnp.where(row == column, 1.0, 0.0).astype(jnp.bfloat16)
    for t in range(slices):
        strip = turn ^ t
        strip = jnp.where(flipped == 1, slices - 1 - strip, strip)
        span = pl.ds(pl.multiple_of(strip * share, 8), share)
        for c in range(3):
            out_ref[c, span] = choose(matrix, pieces(in_refs[t][c]))


def shards_by_block(initial_state, applied_field, coupling):
    rows, _, grid = initial_state.shape
    group = ("core", "z_low", "y")
    peers = 8
    slices = 4
    wide_halo, halo, reach = (8, 4, 10)
    width = grid // peers
    space = ("z_high", "z_low", "y")
    blocks = 8
    rank = lax.axis_index(group)
    turn = lax.axis_index(("x", "core"))
    half = lax.axis_index("z_high")
    place = jnp.stack([turn, half]).astype(jnp.int32)
    number = (2 * lax.axis_index("x") + half).astype(jnp.int32)[None]
    base = jnp.where(rank < peers // 2, rank, peers - 1 - rank).astype(jnp.int32)[None]

    state_in = jnp.transpose(initial_state, (1, 0, 2))
    applied_in = jnp.transpose(applied_field, (1, 0, 2))
    edge_shape = (-(-7 * reach // 8) * 8, grid)
    top, bottom = vmem_call(functools.partial(pack_body, reach), [edge_shape] * 2, "pack")(
        state_in, applied_in, coupling
    )
    before = lax.ppermute(bottom, space, [(i, i + 1) for i in range(blocks - 1)])
    after = lax.ppermute(top, space, [(i + 1, i) for i in range(blocks - 1)])

    def pair(*shape):
        return jax.ShapeDtypeStruct((2,) + shape, jnp.bfloat16)

    back_rows = grid // 2 + 2 * wide_halo
    row_table, *column_tables = vmem_call(
        tables_body,
        [pair(grid, 2 * grid)] + [pair(grid, grid // 2)] * 2 + [pair(back_rows, grid)] * 2,
        "tables",
    )(*small_tables(rank, grid, peers, wide_halo))
    tensor = weighted_tensor(rank, grid, width)

    window = rows + 2 * wide_halo
    state_shape = (3, window, grid)
    first, around, wide = vmem_call(
        functools.partial(start_body, reach, wide_halo, slices),
        [state_shape, (4, window, grid), (7, rows + 32, grid)],
        "start",
        scalars=1,
    )(place, state_in, applied_in, coupling, before, after)

    def trade(values):
        return lax.ppermute(values, ("core", "z_high"), [(0, 0), (1, 2), (2, 1), (3, 3)])

    def spread(slots):
        return [slots[0]] + [
            lax.ppermute(slots[k], group, [(i, i ^ k) for i in range(peers)])
            for k in range(1, peers)
        ]

    send_shapes = [(3, rows, 2 * width)] * peers

    def demag_blocks(slots, margin):
        span = rows + 2 * margin
        skip = wide_halo - margin
        return spread(
            vmem_call(
                functools.partial(spectrum_body, peers, skip),
                [(3, span, 2 * width)] * peers,
                "spectrum",
                scalars=1,
                scratch=[(back_rows - 2 * skip, 6 * width)] * 2,
                cost=10**9,
            )(base, *spread(slots), tensor, *column_tables)
        )

    state = trade(first)
    around = trade(around)
    sent = vmem_call(functools.partial(rows_body, wide_halo), send_shapes, "rows")(state, row_table)
    for repeat in range(FINE):
        last = repeat == FINE - 1
        margin = halo if last else wide_halo
        shape = (3, rows + 2 * margin, grid)
        *sent, predicted, start = vmem_call(
            functools.partial(predict_body, peers, margin), send_shapes + [shape] * 2, "predict", cost=10**9
        )(*demag_blocks(sent, margin), state, around, row_table)
        received = demag_blocks(sent, margin)
        if not last:
            *sent, state = vmem_call(
                functools.partial(correct_body, peers, margin), send_shapes + [shape], "correct", cost=10**9
            )(*received, predicted, start, around, row_table)
    share = rows // slices
    *strips, _ = vmem_call(
        functools.partial(end_body, peers, share),
        [(3, share + 2 * halo, grid)] * slices + [shape],
        "end",
        scalars=1,
    )(number, *received, predicted, start, around, row_table)

    def strip_route(t):
        route = []
        for i in range(8):
            x, core, z = (i // 4, i // 2 % 2, i % 2)
            route.append((i, 4 * (x ^ (t // 2)) + 2 * (z ^ (t % 2)) + core))
        return route

    strips = [
        lax.ppermute(strips[t], ("x", "core", "z_high"), strip_route(t)) for t in range(slices)
    ]
    ends = vmem_call(
        functools.partial(finish_body, slices, halo),
        [(3, share, grid)] * slices,
        "finish",
        scalars=1,
        scratch=[(slices, 3, share + 2 * halo, grid), (slices, 3, share, grid)],
    )(turn.astype(jnp.int32)[None], *strips, wide)
    ends = [ends[0]] + [
        lax.ppermute(ends[t], ("x", "core"), [(i, i ^ t) for i in range(slices)])
        for t in range(1, slices)
    ]
    (result,) = vmem_call(
        functools.partial(gather_body, slices), [(3, rows, grid)], "gather", scalars=1
    )(place, *ends)
    return jnp.transpose(result, (1, 0, 2))[None]


def fits_blocks(mesh):
    return mesh.shape["tm"] == 4 and mesh.shape["space"] == 8


def solution(mesh):
    if not fits_blocks(mesh):
        in_specs = (P("space", None, None), P("space", None, None), P("space", None))
        out_specs = P("tm", "space", None, None)
        return jax.shard_map(
            shards, mesh=mesh, in_specs=in_specs, out_specs=out_specs, check_vma=False
        )
    fine_mesh = Mesh(
        mesh.devices.reshape(2, 2, 2, 2, 2), ("x", "core", "z_high", "z_low", "y")
    )
    space = ("z_high", "z_low", "y")
    in_specs = (P(space, None, None), P(space, None, None), P(space, None))
    out_specs = P(("x", "core"), space, None, None)
    return jax.shard_map(
        shards_by_block, mesh=fine_mesh, in_specs=in_specs, out_specs=out_specs, check_vma=False
    )
```

```python
import functools
import math

import jax
import jax.numpy as jnp
from jax import lax
from jax.experimental import pallas as pl
from jax.experimental.pallas import tpu as pltpu
from jax.sharding import Mesh
from jax.sharding import PartitionSpec as P

FINE = 2
VMEM_LIMIT = 16 * 1024 * 1024


step_time = 0.06
damping = 0.02
stiffness = 0.25
thickness = 8.0


def with_halo(x, sides, width):
    for axis, dim in sides:
        peers, length = (lax.axis_size(axis), x.shape[dim])
        up = [(i, (i + 1) % peers) for i in range(peers - 1)]
        down = [(j, i) for i, j in up]
        last = lax.slice_in_dim(x, length - width, length, axis=dim)
        initial = lax.slice_in_dim(x, 0, width, axis=dim)
        before = lax.ppermute(last, axis, up)
        after = lax.ppermute(initial, axis, down)
        x = jnp.concatenate([before, x, after], axis=dim)
    return x


def passed_along(block, axis, distance):
    devices = range(lax.axis_size(axis))
    route = [(i - distance, i) for i in devices if i - distance in devices]
    return lax.ppermute(block, axis, route)


def spectral_tensor(row_index, column_index, length):
    half_length = length // 2
    signed_rows = jnp.where(row_index < half_length, row_index, row_index - length).astype(
        jnp.float32
    )
    signed_columns = jnp.where(
        column_index < half_length, column_index, column_index - length
    ).astype(jnp.float32)
    wave_rows = 2.0 * math.pi / length * signed_rows[:, None]
    wave_columns = 2.0 * math.pi / length * signed_columns[None, :]
    squared = wave_rows * wave_rows + wave_columns * wave_columns
    nonzero = squared > 0.0
    safe_square = jnp.where(nonzero, squared, 1.0)
    scaled_wave = jnp.sqrt(safe_square) * thickness
    film_factor = jnp.where(nonzero, (1.0 - jnp.exp(-scaled_wave)) / scaled_wave, 1.0)
    in_plane = (1.0 - film_factor) / safe_square
    nyquist = (row_index[:, None] == half_length) | (column_index[None, :] == half_length)
    normalizer = -1.0 / (length * length)
    tensor_first = in_plane * wave_columns * wave_columns * normalizer
    tensor_second = in_plane * wave_rows * wave_rows * normalizer
    tensor_cross = jnp.where(nyquist, 0.0, in_plane * wave_columns * wave_rows) * normalizer
    tensor_normal = film_factor * normalizer
    return (tensor_first, tensor_second, tensor_cross, tensor_normal)


def exchange_field(padded_state, padded_coupling):
    center_state = padded_state[1:-1]
    center_coupling = padded_coupling[1:-1]
    wide_state = jnp.pad(padded_state, ((0, 0), (0, 0), (1, 1)))
    wide_coupling = jnp.pad(padded_coupling, ((0, 0), (1, 1)))
    neighbour_sum = padded_coupling[2:, None, :] * (padded_state[2:] - center_state)
    neighbour_sum = neighbour_sum + padded_coupling[:-2, None, :] * (
        padded_state[:-2] - center_state
    )
    neighbour_sum = neighbour_sum + wide_coupling[1:-1, None, 2:] * (
        wide_state[1:-1, :, 2:] - center_state
    )
    neighbour_sum = neighbour_sum + wide_coupling[1:-1, None, :-2] * (
        wide_state[1:-1, :, :-2] - center_state
    )
    return stiffness * center_coupling[:, None, :] * neighbour_sum


def torque(magnet, effective):
    first_cross = jnp.cross(magnet, effective, axis=1)
    second_cross = jnp.cross(magnet, first_cross, axis=1)
    return -(first_cross + damping * second_cross) / (1.0 + damping * damping)


def phase_table(row_count, column_count, period, direction):
    row_ids = lax.broadcasted_iota(jnp.int32, (row_count, column_count), 0)
    column_ids = lax.broadcasted_iota(jnp.int32, (row_count, column_count), 1)
    angles = (row_ids * column_ids % period).astype(jnp.float32) * (2.0 * math.pi / period)
    return (jnp.cos(angles), direction * jnp.sin(angles))


def joined_table(row_count, column_count, period, direction):
    table_cos, table_sin = phase_table(row_count, column_count, period, direction)
    return jnp.concatenate([table_cos, table_sin], axis=1)


def contract(pattern, left, right):
    return jnp.einsum(pattern, left, right, precision=lax.Precision.HIGHEST)


def complex_apply(pattern, real_part, imag_part, joined):
    half_width = joined.shape[-1] // 2
    real_both = contract(pattern, real_part, joined)
    imag_both = contract(pattern, imag_part, joined)
    return (
        real_both[..., :half_width] - imag_both[..., half_width:],
        real_both[..., half_width:] + imag_both[..., :half_width],
    )


def apply_tensor(real_part, imag_part, tensor):
    tensor_first, tensor_second, tensor_cross, tensor_normal = tensor

    def mix_components(values):
        return jnp.stack(
            [
                tensor_first * values[0] + tensor_cross * values[1],
                tensor_cross * values[0] + tensor_second * values[1],
                tensor_normal * values[2],
            ],
            axis=0,
        )

    return (mix_components(real_part), mix_components(imag_part))


def shards(initial_state, applied_field, coupling):
    row_count, component_count, grid_size = initial_state.shape
    length = 2 * grid_size
    space_count = lax.axis_size("space")
    space_index = lax.axis_index("space")
    slice_count = lax.axis_size("tm")
    slice_index = lax.axis_index("tm")
    is_first = slice_index == 0
    padded_coupling = with_halo(coupling, (("space", 0),), 1)
    index_all = jnp.arange(length, dtype=jnp.int32)
    local_demag = jnp.array([0.0, 0.0, -1.0], dtype=jnp.float32).reshape(1, 3, 1)
    forward_y = joined_table(grid_size, length, length, -1.0)
    inverse_y = joined_table(length, grid_size, length, 1.0)

    def transform_columns(real_part, imag_part):
        return complex_apply("yca,yk->cak", real_part, imag_part, forward_y)

    column_width = grid_size // space_count
    columns = space_index * column_width + jnp.arange(column_width, dtype=jnp.int32)
    tensor = tuple((part_table.T for part_table in spectral_tensor(index_all, columns, length)))
    edge_first, edge_second, edge_cross, edge_normal = spectral_tensor(
        index_all, jnp.array([0, grid_size], dtype=jnp.int32), length
    )
    anchor_diag = jnp.stack([edge_first[:, 0], edge_second[:, 0], edge_normal[:, 0]], axis=0)
    nyquist_diag = jnp.stack([edge_first[:, 1], edge_second[:, 1], edge_normal[:, 1]], axis=0)
    mean_diag = 0.5 * (anchor_diag + nyquist_diag)
    half_gap = 0.5 * (anchor_diag - nyquist_diag)
    is_anchor = (columns == 0)[None, :, None]
    column_ids = jnp.arange(grid_size, dtype=jnp.int32)
    is_lead = column_ids == 0
    lead_columns = is_lead[None, :, None]
    alternating = jnp.where(column_ids % 2 == 0, 1.0, -1.0).astype(jnp.float32)
    forward_x = joined_table(grid_size, grid_size, length, -1.0)
    inverse_x_cos, inverse_x_sin = phase_table(grid_size, grid_size, length, 1.0)

    def demag_field(magnet):
        both_parts = contract("rcx,xk->rck", magnet, forward_x)
        packed_real = both_parts[..., :grid_size]
        imag_part = both_parts[..., grid_size:]
        nyquist_column = jnp.einsum(
            "rcx,x->rc", magnet, alternating, precision=lax.Precision.HIGHEST
        )
        packed_imag = jnp.where(is_lead, nyquist_column[:, :, None], imag_part)
        real_part, imag_part = (
            lax.all_to_all(packed_real, "space", split_axis=2, concat_axis=0, tiled=True),
            lax.all_to_all(packed_imag, "space", split_axis=2, concat_axis=0, tiled=True),
        )
        real_part, imag_part = transform_columns(real_part, imag_part)
        out_real, out_imag = apply_tensor(real_part, imag_part, tensor)
        lead_real = real_part[:, 0, :]
        lead_imag = imag_part[:, 0, :]
        mirror_real = jnp.concatenate([lead_real[:, :1], lead_real[:, 1:][:, ::-1]], axis=1)
        mirror_imag = jnp.concatenate([lead_imag[:, :1], lead_imag[:, 1:][:, ::-1]], axis=1)
        fixed_real = mean_diag * lead_real + half_gap * mirror_real
        fixed_imag = mean_diag * lead_imag - half_gap * mirror_imag
        out_real = jnp.where(is_anchor, fixed_real[:, None, :], out_real)
        out_imag = jnp.where(is_anchor, fixed_imag[:, None, :], out_imag)
        out_real, out_imag = complex_apply("cak,ky->cay", out_real, out_imag, inverse_y)
        out_real, out_imag = (
            lax.all_to_all(out_real, "space", split_axis=2, concat_axis=1, tiled=True),
            lax.all_to_all(out_imag, "space", split_axis=2, concat_axis=1, tiled=True),
        )
        nyquist_part = jnp.transpose(out_imag[:, :1, :], (2, 0, 1))
        doubled_real = jnp.where(lead_columns, out_real, 2.0 * out_real)
        doubled_imag = jnp.where(lead_columns, 0.0, 2.0 * out_imag)
        result = contract("cxr,xo->rco", doubled_real, inverse_x_cos) - contract(
            "cxr,xo->rco", doubled_imag, inverse_x_sin
        )
        return result + nyquist_part * alternating

    def effective_fine(state_now):
        padded_state = with_halo(state_now, (("space", 0),), 1)
        return (
            exchange_field(padded_state, padded_coupling) + demag_field(state_now) + applied_field
        )

    def propagate_coarse(magnet):
        padded_state = with_halo(magnet, (("space", 0),), 1)
        effective = (
            exchange_field(padded_state, padded_coupling) + applied_field + magnet * local_demag
        )
        return magnet + FINE * step_time * torque(magnet, effective)

    def coarse_sweep(jump_term):

        def one_turn(turn_index, loop_state):
            start_state, coarse_end, slice_end = loop_state
            start_state = jnp.where(is_first, initial_state, passed_along(slice_end, "tm", 1))
            coarse_end = propagate_coarse(start_state)
            return (start_state, coarse_end, coarse_end + jump_term)

        coarse_end = propagate_coarse(initial_state)
        return lax.fori_loop(
            0, slice_count - 1, one_turn, (initial_state, coarse_end, coarse_end + jump_term)
        )

    start_state, coarse_end, slice_end = coarse_sweep(jnp.zeros_like(initial_state))
    magnet = start_state
    for repeat in range(FINE):
        first_rate = torque(magnet, effective_fine(magnet))
        predicted = magnet + step_time * first_rate
        second_rate = torque(predicted, effective_fine(predicted))
        magnet = magnet + 0.5 * step_time * (first_rate + second_rate)
    jump_term = magnet - coarse_end
    start_state, coarse_end, slice_end = coarse_sweep(jump_term)
    return slice_end[None]


def turn_parts(grid, product):
    shifted = (product & (4 * grid - 1)) + grid // 2
    quarter = (shifted >> (grid.bit_length() - 1)) & 3
    rest = (shifted & (grid - 1)) - grid // 2
    angle = rest.astype(jnp.float32) * (math.pi / (2 * grid))
    square = angle * angle
    sine = -1.0 / 39916800.0
    for term in (1.0 / 362880.0, -1.0 / 5040.0, 1.0 / 120.0, -1.0 / 6.0, 1.0):
        sine = sine * square + term
    sine = sine * angle
    cosine = 1.0 / 479001600.0
    for term in (-1.0 / 3628800.0, 1.0 / 40320.0, -1.0 / 720.0, 1.0 / 24.0, -0.5, 1.0):
        cosine = cosine * square + term
    odd = (quarter & 1) == 1
    first = jnp.where(odd, sine, cosine)
    second = jnp.where(odd, cosine, sine)
    first = jnp.where((quarter == 1) | (quarter == 2), -first, first)
    second = jnp.where(quarter >= 2, -second, second)
    return (first, second)


def fill_table(grid, coarse, fine, sine, sign, out_ref, top=None):
    coarse_cos, coarse_sin = turn_parts(grid, coarse)
    fine_cos, fine_sin = turn_parts(grid, fine)
    lead = sign * jnp.where(sine, coarse_sin, coarse_cos)
    side = sign * jnp.where(sine, coarse_cos, -coarse_sin)
    for block in range(out_ref.shape[1] // 16):
        values = lead[block : block + 1] * fine_cos + side[block : block + 1] * fine_sin
        if top is not None and block == 0:
            first = lax.broadcasted_iota(jnp.int32, values.shape, 0) == 0
            values = jnp.where(first, top, values)
        high, low = split(values)
        out_ref[0, 16 * block : 16 * block + 16] = high
        out_ref[1, 16 * block : 16 * block + 16] = low


def tables_body(
    peers, halo, rank_ref, row_ref, cos_ref, sin_ref, back_cos_ref, back_sin_ref, tensor_ref
):
    rank = rank_ref[0]
    grid = row_ref.shape[1]
    width = grid // peers
    bits = width.bit_length() - 1
    late = rank >= peers // 2
    sign = jnp.where(late, -1.0, 1.0).astype(jnp.float32)
    base = jnp.where(late, peers - 1 - rank, rank)

    def iota(rows, columns, dim):
        return lax.broadcasted_iota(jnp.int32, (rows, columns), dim)

    lane = iota(grid // 16, 2 * grid, 1)
    sine = ((lane >> bits) & 1) == 1
    wave = ((lane >> (bits + 1)) ^ rank) * width + (lane & (width - 1))
    wave = jnp.where(sine & (wave == 0), grid, wave)
    sixteens = 32 * iota(grid // 16, 2 * grid, 0)
    ones = 2 * iota(16, 2 * grid, 0) - (grid - 1)
    fill_table(grid, sixteens * wave, ones * wave[:16], sine, 1.0, row_ref)

    half = grid // 2
    spot = iota(grid // 16, half, 1)
    place = 2 * (((spot >> bits) ^ base) * width + (spot & (width - 1))) - (grid - 1)
    sixteens = 16 * iota(grid // 16, half, 0) * place
    ones = iota(16, half, 0) * place[:16]
    edge = sign * turn_parts(grid, grid * place[:16])[1]
    fill_table(grid, sixteens, ones, False, 1.0, cos_ref)
    fill_table(grid, sixteens, ones, True, sign, sin_ref, top=edge)

    count = back_cos_ref.shape[1] // 16
    for out_ref, is_sine in ((back_cos_ref, False), (back_sin_ref, True)):
        number = iota(count, grid, 1)
        if is_sine:
            number = jnp.where(number == 0, grid, number)
        span = 32 * iota(count, grid, 0) * number
        start = (2 * (iota(16, grid, 0) - halo) - (grid - 1)) * number[:16]
        fill_table(grid, span, start, is_sine, sign if is_sine else 1.0, out_ref)

    def parts(row_number, column_number, weight):
        row_wave = (2.0 * math.pi / (2 * grid)) * signed(row_number)
        column_wave = (2.0 * math.pi / (2 * grid)) * signed(column_number)
        squared = row_wave * row_wave + column_wave * column_wave
        nonzero = squared > 0.0
        safe = jnp.where(nonzero, squared, 1.0)
        scaled = jnp.sqrt(safe) * thickness
        film = jnp.where(nonzero, (1.0 - jnp.exp(-scaled)) / scaled, 1.0)
        in_plane = (1.0 - film) / safe * weight
        edge = (row_number == grid) | (column_number == grid)
        return (
            in_plane * column_wave * column_wave,
            in_plane * row_wave * row_wave,
            film * weight,
            jnp.where(edge, 0.0, in_plane * column_wave * row_wave),
        )

    def signed(number):
        return jnp.where(number < grid, number, number - 2 * grid).astype(jnp.float32)

    columns = 2 * width
    for block in range(grid // 64):
        spots = slice(64 * block, 64 * block + 64)
        row_number = iota(64, columns, 0) + 64 * block
        lane = iota(64, columns, 1)
        is_sine = lane >= width
        column_number = rank * width + (lane & (width - 1))
        column_number = jnp.where(is_sine & (column_number == 0), grid, column_number)
        column_weight = jnp.where((column_number & (grid - 1)) == 0, 1.0, 2.0)
        weight = column_weight * jnp.where(row_number == 0, 1.0, 2.0) * (-0.25 / (grid * grid))
        found = parts(row_number, column_number, weight)
        for c in range(3):
            tensor_ref[c, spots] = found[c]
        tensor_ref[6, spots] = jnp.where(is_sine, -found[3], found[3])
        if block == 0:
            other = parts(jnp.where(row_number == 0, grid, row_number), column_number, weight)
            found = [jnp.where(row_number == 0, a, b) for a, b in zip(other, found)]
        for c in range(3):
            tensor_ref[3 + c, spots] = found[c]


def split(values):
    high = values.astype(jnp.bfloat16)
    low = (values - high.astype(jnp.float32)).astype(jnp.bfloat16)
    return (high, low)


def multiply(left, right, transposed=False):
    numbers = (((1,), (1 if transposed else 0,)), ((), ()))

    def one(a, b):
        return lax.dot_general(a, b, numbers, preferred_element_type=jnp.float32)

    return one(left[0], right[0]) + (one(left[0], right[1]) + one(left[1], right[0]))


def exchange_weights(coupling):
    rows, columns = coupling.shape
    place = lax.broadcasted_iota(jnp.int32, coupling.shape, 1)
    own = stiffness * coupling
    right = jnp.where(place < columns - 1, pltpu.roll(coupling, columns - 1, 1), 0.0)
    left = jnp.where(place > 0, pltpu.roll(coupling, 1, 1), 0.0)
    below = pltpu.roll(coupling, rows - 1, 0)
    above = pltpu.roll(coupling, 1, 0)
    return (own * right, own * left, own * below, own * above)


def exchange_of(part, weights):
    rows, columns = part.shape
    right, left, below, above = weights
    total = right * (pltpu.roll(part, columns - 1, 1) - part)
    total = total + left * (pltpu.roll(part, 1, 1) - part)
    total = total + below * (pltpu.roll(part, rows - 1, 0) - part)
    return total + above * (pltpu.roll(part, 1, 0) - part)


def cross(a, b):
    return (a[1] * b[2] - a[2] * b[1], a[2] * b[0] - a[0] * b[2], a[0] * b[1] - a[1] * b[0])


def torque_of(magnet, effective):
    first = cross(magnet, effective)
    second = cross(magnet, first)
    scale = -1.0 / (1.0 + damping * damping)
    return [scale * (a + damping * b) for a, b in zip(first, second)]


def coarse_step(magnet, applied, weights):
    effective = [exchange_of(part, weights) + field for part, field in zip(magnet, applied)]
    effective[2] = effective[2] - magnet[2]
    return [part + FINE * step_time * rate for part, rate in zip(magnet, torque_of(magnet, effective))]


def vmem_call(body, outs, name, scalars=0, scratch=(), cost=10**8):
    whole = pl.BlockSpec(memory_space=pltpu.VMEM)

    def call(*args):
        first = [pl.BlockSpec(memory_space=pltpu.SMEM)] * scalars
        return pl.pallas_call(
            body,
            out_shape=[
                out if isinstance(out, jax.ShapeDtypeStruct) else jax.ShapeDtypeStruct(out, jnp.float32)
                for out in outs
            ],
            in_specs=first + [whole] * (len(args) - scalars),
            out_specs=[whole] * len(outs),
            scratch_shapes=[pltpu.VMEM(shape, jnp.float32) for shape in scratch],
            compiler_params=pltpu.CompilerParams(vmem_limit_bytes=VMEM_LIMIT),
            cost_estimate=pl.CostEstimate(flops=cost, bytes_accessed=10**6, transcendentals=0),
            name=name,
        )(*args)

    return call


def pack_body(reach, state_ref, applied_ref, coupling_ref, top_ref, bottom_ref, *scratch):
    rows = coupling_ref.shape[0]
    span = scratch[-2].shape[1]
    buffers, sems = (scratch[:-1], scratch[-1])
    copies = []
    for side, start in enumerate((0, rows - span)):
        for number, ref in enumerate((state_ref, applied_ref)):
            copies.append((ref.at[:, pl.ds(start, span)], buffers[0].at[side, number]))
        copies.append((coupling_ref.at[pl.ds(start, span)], buffers[1].at[side]))
    copies = [pltpu.make_async_copy(*ends, sems.at[i]) for i, ends in enumerate(copies)]
    for copy in copies:
        copy.start()
    for copy in copies:
        copy.wait()
    for side, (ref, first) in enumerate(((top_ref, 0), (bottom_ref, span - reach))):
        kept = slice(first, first + reach)
        for c in range(6):
            ref[c * reach : (c + 1) * reach] = buffers[0][side, c // 3, c % 3][kept]
        ref[6 * reach : 7 * reach] = buffers[1][side][kept]
        ref[7 * reach :] = jnp.zeros_like(ref[7 * reach :])


def pack_edges(reach, state, applied, coupling):
    grid = coupling.shape[1]
    span = -(-reach // 8) * 8
    edge = jax.ShapeDtypeStruct((-(-7 * reach // 8) * 8, grid), jnp.float32)
    return pl.pallas_call(
        functools.partial(pack_body, reach),
        out_shape=[edge] * 2,
        in_specs=[pl.BlockSpec(memory_space=pltpu.HBM)] * 3,
        out_specs=[pl.BlockSpec(memory_space=pltpu.VMEM)] * 2,
        scratch_shapes=[
            pltpu.VMEM((2, 2, 3, span, grid), jnp.float32),
            pltpu.VMEM((2, span, grid), jnp.float32),
            pltpu.SemaphoreType.DMA((6,)),
        ],
        compiler_params=pltpu.CompilerParams(vmem_limit_bytes=VMEM_LIMIT),
        name="pack",
    )(state, applied, coupling)


def pieces(values):
    high = values.astype(jnp.bfloat16)
    rest = values - high.astype(jnp.float32)
    middle = rest.astype(jnp.bfloat16)
    low = (rest - middle.astype(jnp.float32)).astype(jnp.bfloat16)
    return (high, middle, low)


def choose(selection, parts):
    first, second, third = (
        jnp.dot(selection, part, preferred_element_type=jnp.float32) for part in parts
    )
    return first + (second + third)


def build_wide(flipped, reach, state_ref, applied_ref, coupling_ref, before_ref, after_ref, wide_ref):
    rows = coupling_ref.shape[0]
    count = before_ref.shape[0]
    total = wide_ref.shape[1]
    margin = (total - rows) // 2

    def matrix(fields, columns, base):
        row = lax.broadcasted_iota(jnp.int32, (fields * total, columns), 0)
        column = lax.broadcasted_iota(jnp.int32, (fields * total, columns), 1)
        field, row = (row // total, row % total)
        row = jnp.where(flipped == 1, total - 1 - row, row) - base
        size = reach if fields > 1 else columns
        inside = (row >= 0) & (row < size) & (column == field * size + row)
        return jnp.where(inside, 1.0, 0.0).astype(jnp.bfloat16)

    own = matrix(1, rows, margin)
    edges = choose(matrix(7, count, margin - reach), pieces(before_ref[...]))
    edges = edges + choose(matrix(7, count, margin + rows), pieces(after_ref[...]))
    fields = [state_ref[c] for c in range(3)] + [applied_ref[c] for c in range(3)]
    fields.append(coupling_ref[...])
    for number, field in enumerate(fields):
        wide_ref[number] = choose(own, pieces(field)) + edges[number * total : (number + 1) * total]


def wide_body(reach, flip_ref, *refs):
    build_wide(flip_ref[0], reach, *refs)


def start_body(reach, halo, slices, turn_ref, flip_ref, *refs):
    first_ref, around_ref, wide_ref = refs[5:]
    turn = turn_ref[0]
    build_wide(flip_ref[0], reach, *refs[:5], wide_ref)
    rows = first_ref.shape[1] - 2 * halo
    margin = (wide_ref.shape[1] - rows) // 2
    kept = slice(margin - halo, margin + rows + halo)
    for c in range(4):
        around_ref[c] = wide_ref[3 + c, kept]
    for c in range(3):
        first_ref[c] = wide_ref[c, kept]
    weights = exchange_weights(wide_ref[6])
    applied = [wide_ref[3 + c] for c in range(3)]
    for number in range(1, slices):
        @pl.when(turn >= number)
        def step():
            magnet = coarse_step([wide_ref[c] for c in range(3)], applied, weights)
            for c in range(3):
                wide_ref[c] = magnet[c]
                first_ref[c] = magnet[c][kept]


def send_rows(magnet, halo, table, out_refs):
    rows = magnet[0].shape[0] - 2 * halo
    width = out_refs[0].shape[2]
    block = split(jnp.concatenate([part[halo : halo + rows] for part in magnet], axis=0))
    spectrum = multiply(block, table)
    for slot, out_ref in enumerate(out_refs):
        for c in range(3):
            out_ref[c] = spectrum[c * rows : (c + 1) * rows, slot * width : (slot + 1) * width]


def rows_body(halo, state_ref, table_ref, *out_refs):
    send_rows([state_ref[c] for c in range(3)], halo, (table_ref[0], table_ref[1]), out_refs)


def spectrum_body(peers, skip, base_ref, *refs):
    in_refs, refs = (refs[:peers], refs[peers:])
    tensor_ref, cos_ref, sin_ref, back_cos_ref, back_sin_ref = refs[:5]
    out_refs = refs[5 : 5 + peers]
    front_ref, back_ref = refs[5 + peers :]
    _, rows, width = in_refs[0].shape
    window = out_refs[0].shape[1]
    half = peers // 2

    def fold(sign):
        return jnp.concatenate(
            [
                jnp.concatenate(
                    [in_refs[p][c] + sign * in_refs[peers - 1 - p][c] for p in range(half)], axis=0
                )
                for c in range(3)
            ],
            axis=1,
        )

    even = multiply((cos_ref[0], cos_ref[1]), split(fold(1.0)))
    odd = multiply((sin_ref[0], sin_ref[1]), split(fold(-1.0)))
    even_x, even_y, even_z = (even[:, c * width : (c + 1) * width] for c in range(3))
    odd_x, odd_y, odd_z = (odd[:, c * width : (c + 1) * width] for c in range(3))
    mixed = tensor_ref[6]

    def turned(values):
        return mixed * pltpu.roll(values, width // 2, 1)

    even_out = jnp.concatenate(
        [
            tensor_ref[0] * even_x - turned(odd_y),
            tensor_ref[1] * even_y - turned(odd_x),
            tensor_ref[2] * even_z,
        ],
        axis=1,
    )
    odd_out = jnp.concatenate(
        [
            tensor_ref[3] * odd_x + turned(even_y),
            tensor_ref[4] * odd_y + turned(even_x),
            tensor_ref[5] * odd_z,
        ],
        axis=1,
    )
    even_rows = multiply((back_cos_ref[0], back_cos_ref[1]), split(even_out))
    odd_rows = multiply((back_sin_ref[0], back_sin_ref[1]), split(odd_out))
    kept = slice(skip, even_rows.shape[0] - skip)
    front_ref[...] = (even_rows + odd_rows)[kept]
    back_ref[...] = (even_rows - odd_rows)[kept]
    base = base_ref[0]
    for p in range(half):
        span = pl.ds(pl.multiple_of((base ^ p) * rows, 8), window)
        for c in range(3):
            out_refs[p][c] = front_ref[span, c * width : (c + 1) * width]
            out_refs[peers - 1 - p][c] = back_ref[span, c * width : (c + 1) * width]


def field_rates(in_refs, magnet, applied, coupling, table):
    rows = in_refs[0].shape[1]
    spectrum = jnp.concatenate(
        [jnp.concatenate([ref[c] for c in range(3)], axis=0) for ref in in_refs], axis=1
    )
    demag = multiply(split(spectrum), table, transposed=True)
    weights = exchange_weights(coupling)
    effective = [
        exchange_of(magnet[c], weights) + demag[c * rows : (c + 1) * rows] + applied[c]
        for c in range(3)
    ]
    return torque_of(magnet, effective)


def inner_rows(ref, number, rows):
    skip = (ref.shape[1] - rows) // 2
    return ref[number, skip : skip + rows]


def predict_body(peers, halo, *refs):
    in_refs, refs = (refs[:peers], refs[peers:])
    state_ref, around_ref, table_ref = refs[:3]
    send_refs, (predicted_ref, base_ref) = (refs[3 : 3 + peers], refs[3 + peers :])
    rows = in_refs[0].shape[1]
    table = (table_ref[0], table_ref[1])
    magnet = [inner_rows(state_ref, c, rows) for c in range(3)]
    around = [inner_rows(around_ref, c, rows) for c in range(4)]
    rates = field_rates(in_refs, magnet, around[:3], around[3], table)
    predicted = [part + step_time * rate for part, rate in zip(magnet, rates)]
    send_rows(predicted, halo, table, send_refs)
    for c in range(3):
        predicted_ref[c] = predicted[c]
        base_ref[c] = magnet[c] + 0.5 * step_time * rates[c]


def correct_body(peers, halo, *refs):
    in_refs, refs = (refs[:peers], refs[peers:])
    state_ref, base_ref, around_ref, table_ref = refs[:4]
    send_refs, following_ref = (refs[4 : 4 + peers], refs[4 + peers])
    rows = in_refs[0].shape[1]
    table = (table_ref[0], table_ref[1])
    magnet = [state_ref[c] for c in range(3)]
    around = [inner_rows(around_ref, c, rows) for c in range(4)]
    rates = field_rates(in_refs, magnet, around[:3], around[3], table)
    following = [base_ref[c] + 0.5 * step_time * rates[c] for c in range(3)]
    send_rows(following, halo, table, send_refs)
    for c in range(3):
        following_ref[c] = following[c]


def end_body(peers, share, number_ref, *refs):
    in_refs, refs = (refs[:peers], refs[peers:])
    state_ref, base_ref, around_ref, table_ref = refs[:4]
    out_refs, end_ref = (refs[4:-1], refs[-1])
    rows = in_refs[0].shape[1]
    magnet = [state_ref[c] for c in range(3)]
    around = [inner_rows(around_ref, c, rows) for c in range(4)]
    rates = field_rates(in_refs, magnet, around[:3], around[3], (table_ref[0], table_ref[1]))
    for c in range(3):
        end_ref[c] = base_ref[c] + 0.5 * step_time * rates[c]
    for t, out_ref in enumerate(out_refs):
        start = pl.multiple_of((number_ref[0] ^ t) * share, 8)
        for c in range(3):
            out_ref[c] = end_ref[c, pl.ds(start, out_ref.shape[1])]


def finish_body(slices, trim, turn_ref, *refs):
    in_refs, wide_ref = (refs[:slices], refs[slices])
    out_refs = refs[slices + 1 : 2 * slices + 1]
    fine_ref, end_ref = refs[2 * slices + 1 :]
    turn = turn_ref[0]
    rows = fine_ref.shape[2]
    share = rows - 2 * trim
    for t in range(slices):
        fine_ref[turn ^ t] = in_refs[t][...]
    margin = (wide_ref.shape[1] - slices * share) // 2
    start = pl.multiple_of(turn * share + margin - 8, 8)

    def strip(number):
        return wide_ref[number, pl.ds(start, share + 16)][8 - trim : 8 + share + trim]

    weights = exchange_weights(strip(6))
    applied = [strip(3 + c) for c in range(3)]
    first = [strip(c) for c in range(3)]
    magnet = first
    for number in range(slices):
        first = coarse_step(first, applied, weights)
        ahead = coarse_step(magnet, applied, weights) if number > 0 else first
        magnet = [ahead[c] + (fine_ref[number, c] - first[c]) for c in range(3)]
        for c in range(3):
            end_ref[number, c] = magnet[c][trim : trim + share]
    for t in range(slices):
        out_refs[t][...] = end_ref[turn ^ t]


def gather_body(slices, turn_ref, flip_ref, *refs):
    in_refs, out_ref = (refs[:slices], refs[slices])
    turn, flipped = (turn_ref[0], flip_ref[0])
    share = in_refs[0].shape[1]
    row = lax.broadcasted_iota(jnp.int32, (share, share), 0)
    column = lax.broadcasted_iota(jnp.int32, (share, share), 1)
    row = jnp.where(flipped == 1, share - 1 - row, row)
    matrix = jnp.where(row == column, 1.0, 0.0).astype(jnp.bfloat16)
    for t in range(slices):
        strip = turn ^ t
        strip = jnp.where(flipped == 1, slices - 1 - strip, strip)
        span = pl.ds(pl.multiple_of(strip * share, 8), share)
        for c in range(3):
            out_ref[c, span] = choose(matrix, pieces(in_refs[t][c]))


def shards_by_block(initial_state, applied_field, coupling):
    rows, _, grid = initial_state.shape
    group = ("core", "z_low", "y")
    peers = 8
    slices = 4
    wide_halo, halo, reach = (8, 4, 10)
    width = grid // peers
    space = ("z_high", "z_low", "y")
    blocks = 8
    def scalar(value):
        return value.astype(jnp.int32).reshape(1)

    rank = lax.axis_index(group)
    half = lax.axis_index("z_high")
    turn = lax.axis_index(("x", "core"))
    number = 2 * lax.axis_index("x") + half
    base = jnp.where(rank < peers // 2, rank, peers - 1 - rank)
    scalars = (rank, half, lax.axis_index("core"), turn, number, base)
    rank, native_flip, fine_flip, turn, number, base = lax.optimization_barrier(
        tuple(value.astype(jnp.int32).reshape(1) for value in scalars)
    )

    state_in = jnp.transpose(initial_state, (1, 0, 2))
    applied_in = jnp.transpose(applied_field, (1, 0, 2))
    top, bottom = pack_edges(reach, state_in, applied_in, coupling)

    def trade(values):
        return lax.ppermute(values, ("core", "z_high"), [(0, 0), (1, 2), (2, 1), (3, 3)])

    def edge_route(step):
        route = []
        for core in range(2):
            for block in range(blocks):
                following = block + step
                if 0 <= following < blocks:
                    target = (following // 4, core, following % 4)
                    route.append((8 * core + block, 8 * target[0] + 4 * target[1] + target[2]))
        return route

    everywhere = ("core",) + space
    before = lax.ppermute(bottom, everywhere, edge_route(1))
    after = lax.ppermute(top, everywhere, edge_route(-1))
    own = (trade(state_in), trade(applied_in), trade(coupling))

    def pair(*shape):
        return jax.ShapeDtypeStruct((2,) + shape, jnp.bfloat16)

    back_rows = grid // 2 + 2 * wide_halo
    row_table, *column_tables, tensor = vmem_call(
        functools.partial(tables_body, peers, wide_halo),
        [pair(grid, 2 * grid)]
        + [pair(grid, grid // 2)] * 2
        + [pair(back_rows, grid)] * 2
        + [(7, grid, 2 * width)],
        "tables",
        scalars=1,
    )(rank)

    window = rows + 2 * wide_halo
    state_shape = (3, window, grid)
    wide_shape = (7, rows + 32, grid)
    state, around = vmem_call(
        functools.partial(start_body, reach, wide_halo, slices),
        [state_shape, (4, window, grid)],
        "start",
        scalars=2,
        scratch=[wide_shape],
    )(number, fine_flip, *own, before, after)

    def spread(slots):
        return [slots[0]] + [
            lax.ppermute(slots[k], group, [(i, i ^ k) for i in range(peers)])
            for k in range(1, peers)
        ]

    send_shapes = [(3, rows, 2 * width)] * peers

    def demag_blocks(slots, margin):
        span = rows + 2 * margin
        skip = wide_halo - margin
        return spread(
            vmem_call(
                functools.partial(spectrum_body, peers, skip),
                [(3, span, 2 * width)] * peers,
                "spectrum",
                scalars=1,
                scratch=[(back_rows - 2 * skip, 6 * width)] * 2,
                cost=10**9,
            )(base, *spread(slots), tensor, *column_tables)
        )

    sent = vmem_call(functools.partial(rows_body, wide_halo), send_shapes, "rows")(state, row_table)
    for repeat in range(FINE):
        last = repeat == FINE - 1
        margin = halo if last else wide_halo
        shape = (3, rows + 2 * margin, grid)
        *sent, predicted, start = vmem_call(
            functools.partial(predict_body, peers, margin), send_shapes + [shape] * 2, "predict", cost=10**9
        )(*demag_blocks(sent, margin), state, around, row_table)
        received = demag_blocks(sent, margin)
        if not last:
            *sent, state = vmem_call(
                functools.partial(correct_body, peers, margin), send_shapes + [shape], "correct", cost=10**9
            )(*received, predicted, start, around, row_table)
    share = rows // slices
    top, bottom, _ = lax.optimization_barrier((top, bottom, state))
    (wide,) = vmem_call(functools.partial(wide_body, reach), [wide_shape], "wide", scalars=1)(
        native_flip,
        state_in,
        applied_in,
        coupling,
        lax.ppermute(bottom, space, [(i, i + 1) for i in range(blocks - 1)]),
        lax.ppermute(top, space, [(i + 1, i) for i in range(blocks - 1)]),
    )
    *strips, _ = vmem_call(
        functools.partial(end_body, peers, share),
        [(3, share + 2 * halo, grid)] * slices + [shape],
        "end",
        scalars=1,
    )(number, *received, predicted, start, around, row_table)

    def strip_route(t):
        route = []
        for i in range(8):
            x, core, z = (i // 4, i // 2 % 2, i % 2)
            route.append((i, 4 * (x ^ (t // 2)) + 2 * (z ^ (t % 2)) + core))
        return route

    strips = [
        lax.ppermute(strips[t], ("x", "core", "z_high"), strip_route(t)) for t in range(slices)
    ]
    ends = vmem_call(
        functools.partial(finish_body, slices, halo),
        [(3, share, grid)] * slices,
        "finish",
        scalars=1,
        scratch=[(slices, 3, share + 2 * halo, grid), (slices, 3, share, grid)],
    )(turn, *strips, wide)
    ends = [ends[0]] + [
        lax.ppermute(ends[t], ("x", "core"), [(i, i ^ t) for i in range(slices)])
        for t in range(1, slices)
    ]
    (result,) = vmem_call(
        functools.partial(gather_body, slices), [(3, rows, grid)], "gather", scalars=2
    )(turn, native_flip, *ends)
    return jnp.transpose(result, (1, 0, 2))[None]


def fits_blocks(mesh):
    return mesh.shape["tm"] == 4 and mesh.shape["space"] == 8


def solution(mesh):
    if not fits_blocks(mesh):
        in_specs = (P("space", None, None), P("space", None, None), P("space", None))
        out_specs = P("tm", "space", None, None)
        return jax.shard_map(
            shards, mesh=mesh, in_specs=in_specs, out_specs=out_specs, check_vma=False
        )
    fine_mesh = Mesh(
        mesh.devices.reshape(2, 2, 2, 2, 2), ("x", "core", "z_high", "z_low", "y")
    )
    space = ("z_high", "z_low", "y")
    in_specs = (P(space, None, None), P(space, None, None), P(space, None))
    out_specs = P(("x", "core"), space, None, None)
    return jax.shard_map(
        shards_by_block, mesh=fine_mesh, in_specs=in_specs, out_specs=out_specs, check_vma=False
    )
```

```python
import functools
import math

import jax
import jax.numpy as jnp
from jax import lax
from jax.experimental import pallas as pl
from jax.experimental.pallas import tpu as pltpu
from jax.sharding import Mesh
from jax.sharding import PartitionSpec as P

FINE = 2
VMEM_LIMIT = 16 * 1024 * 1024


step_time = 0.06
damping = 0.02
stiffness = 0.25
thickness = 8.0


def with_halo(x, sides, width):
    for axis, dim in sides:
        peers, length = (lax.axis_size(axis), x.shape[dim])
        up = [(i, (i + 1) % peers) for i in range(peers - 1)]
        down = [(j, i) for i, j in up]
        last = lax.slice_in_dim(x, length - width, length, axis=dim)
        initial = lax.slice_in_dim(x, 0, width, axis=dim)
        before = lax.ppermute(last, axis, up)
        after = lax.ppermute(initial, axis, down)
        x = jnp.concatenate([before, x, after], axis=dim)
    return x


def passed_along(block, axis, distance):
    devices = range(lax.axis_size(axis))
    route = [(i - distance, i) for i in devices if i - distance in devices]
    return lax.ppermute(block, axis, route)


def spectral_tensor(row_index, column_index, length):
    half_length = length // 2
    signed_rows = jnp.where(row_index < half_length, row_index, row_index - length).astype(
        jnp.float32
    )
    signed_columns = jnp.where(
        column_index < half_length, column_index, column_index - length
    ).astype(jnp.float32)
    wave_rows = 2.0 * math.pi / length * signed_rows[:, None]
    wave_columns = 2.0 * math.pi / length * signed_columns[None, :]
    squared = wave_rows * wave_rows + wave_columns * wave_columns
    nonzero = squared > 0.0
    safe_square = jnp.where(nonzero, squared, 1.0)
    scaled_wave = jnp.sqrt(safe_square) * thickness
    film_factor = jnp.where(nonzero, (1.0 - jnp.exp(-scaled_wave)) / scaled_wave, 1.0)
    in_plane = (1.0 - film_factor) / safe_square
    nyquist = (row_index[:, None] == half_length) | (column_index[None, :] == half_length)
    normalizer = -1.0 / (length * length)
    tensor_first = in_plane * wave_columns * wave_columns * normalizer
    tensor_second = in_plane * wave_rows * wave_rows * normalizer
    tensor_cross = jnp.where(nyquist, 0.0, in_plane * wave_columns * wave_rows) * normalizer
    tensor_normal = film_factor * normalizer
    return (tensor_first, tensor_second, tensor_cross, tensor_normal)


def exchange_field(padded_state, padded_coupling):
    center_state = padded_state[1:-1]
    center_coupling = padded_coupling[1:-1]
    wide_state = jnp.pad(padded_state, ((0, 0), (0, 0), (1, 1)))
    wide_coupling = jnp.pad(padded_coupling, ((0, 0), (1, 1)))
    neighbour_sum = padded_coupling[2:, None, :] * (padded_state[2:] - center_state)
    neighbour_sum = neighbour_sum + padded_coupling[:-2, None, :] * (
        padded_state[:-2] - center_state
    )
    neighbour_sum = neighbour_sum + wide_coupling[1:-1, None, 2:] * (
        wide_state[1:-1, :, 2:] - center_state
    )
    neighbour_sum = neighbour_sum + wide_coupling[1:-1, None, :-2] * (
        wide_state[1:-1, :, :-2] - center_state
    )
    return stiffness * center_coupling[:, None, :] * neighbour_sum


def torque(magnet, effective):
    first_cross = jnp.cross(magnet, effective, axis=1)
    second_cross = jnp.cross(magnet, first_cross, axis=1)
    return -(first_cross + damping * second_cross) / (1.0 + damping * damping)


def phase_table(row_count, column_count, period, direction):
    row_ids = lax.broadcasted_iota(jnp.int32, (row_count, column_count), 0)
    column_ids = lax.broadcasted_iota(jnp.int32, (row_count, column_count), 1)
    angles = (row_ids * column_ids % period).astype(jnp.float32) * (2.0 * math.pi / period)
    return (jnp.cos(angles), direction * jnp.sin(angles))


def joined_table(row_count, column_count, period, direction):
    table_cos, table_sin = phase_table(row_count, column_count, period, direction)
    return jnp.concatenate([table_cos, table_sin], axis=1)


def contract(pattern, left, right):
    return jnp.einsum(pattern, left, right, precision=lax.Precision.HIGHEST)


def complex_apply(pattern, real_part, imag_part, joined):
    half_width = joined.shape[-1] // 2
    real_both = contract(pattern, real_part, joined)
    imag_both = contract(pattern, imag_part, joined)
    return (
        real_both[..., :half_width] - imag_both[..., half_width:],
        real_both[..., half_width:] + imag_both[..., :half_width],
    )


def apply_tensor(real_part, imag_part, tensor):
    tensor_first, tensor_second, tensor_cross, tensor_normal = tensor

    def mix_components(values):
        return jnp.stack(
            [
                tensor_first * values[0] + tensor_cross * values[1],
                tensor_cross * values[0] + tensor_second * values[1],
                tensor_normal * values[2],
            ],
            axis=0,
        )

    return (mix_components(real_part), mix_components(imag_part))


def shards(initial_state, applied_field, coupling):
    row_count, component_count, grid_size = initial_state.shape
    length = 2 * grid_size
    space_count = lax.axis_size("space")
    space_index = lax.axis_index("space")
    slice_count = lax.axis_size("tm")
    slice_index = lax.axis_index("tm")
    is_first = slice_index == 0
    padded_coupling = with_halo(coupling, (("space", 0),), 1)
    index_all = jnp.arange(length, dtype=jnp.int32)
    local_demag = jnp.array([0.0, 0.0, -1.0], dtype=jnp.float32).reshape(1, 3, 1)
    forward_y = joined_table(grid_size, length, length, -1.0)
    inverse_y = joined_table(length, grid_size, length, 1.0)

    def transform_columns(real_part, imag_part):
        return complex_apply("yca,yk->cak", real_part, imag_part, forward_y)

    column_width = grid_size // space_count
    columns = space_index * column_width + jnp.arange(column_width, dtype=jnp.int32)
    tensor = tuple((part_table.T for part_table in spectral_tensor(index_all, columns, length)))
    edge_first, edge_second, edge_cross, edge_normal = spectral_tensor(
        index_all, jnp.array([0, grid_size], dtype=jnp.int32), length
    )
    anchor_diag = jnp.stack([edge_first[:, 0], edge_second[:, 0], edge_normal[:, 0]], axis=0)
    nyquist_diag = jnp.stack([edge_first[:, 1], edge_second[:, 1], edge_normal[:, 1]], axis=0)
    mean_diag = 0.5 * (anchor_diag + nyquist_diag)
    half_gap = 0.5 * (anchor_diag - nyquist_diag)
    is_anchor = (columns == 0)[None, :, None]
    column_ids = jnp.arange(grid_size, dtype=jnp.int32)
    is_lead = column_ids == 0
    lead_columns = is_lead[None, :, None]
    alternating = jnp.where(column_ids % 2 == 0, 1.0, -1.0).astype(jnp.float32)
    forward_x = joined_table(grid_size, grid_size, length, -1.0)
    inverse_x_cos, inverse_x_sin = phase_table(grid_size, grid_size, length, 1.0)

    def demag_field(magnet):
        both_parts = contract("rcx,xk->rck", magnet, forward_x)
        packed_real = both_parts[..., :grid_size]
        imag_part = both_parts[..., grid_size:]
        nyquist_column = jnp.einsum(
            "rcx,x->rc", magnet, alternating, precision=lax.Precision.HIGHEST
        )
        packed_imag = jnp.where(is_lead, nyquist_column[:, :, None], imag_part)
        real_part, imag_part = (
            lax.all_to_all(packed_real, "space", split_axis=2, concat_axis=0, tiled=True),
            lax.all_to_all(packed_imag, "space", split_axis=2, concat_axis=0, tiled=True),
        )
        real_part, imag_part = transform_columns(real_part, imag_part)
        out_real, out_imag = apply_tensor(real_part, imag_part, tensor)
        lead_real = real_part[:, 0, :]
        lead_imag = imag_part[:, 0, :]
        mirror_real = jnp.concatenate([lead_real[:, :1], lead_real[:, 1:][:, ::-1]], axis=1)
        mirror_imag = jnp.concatenate([lead_imag[:, :1], lead_imag[:, 1:][:, ::-1]], axis=1)
        fixed_real = mean_diag * lead_real + half_gap * mirror_real
        fixed_imag = mean_diag * lead_imag - half_gap * mirror_imag
        out_real = jnp.where(is_anchor, fixed_real[:, None, :], out_real)
        out_imag = jnp.where(is_anchor, fixed_imag[:, None, :], out_imag)
        out_real, out_imag = complex_apply("cak,ky->cay", out_real, out_imag, inverse_y)
        out_real, out_imag = (
            lax.all_to_all(out_real, "space", split_axis=2, concat_axis=1, tiled=True),
            lax.all_to_all(out_imag, "space", split_axis=2, concat_axis=1, tiled=True),
        )
        nyquist_part = jnp.transpose(out_imag[:, :1, :], (2, 0, 1))
        doubled_real = jnp.where(lead_columns, out_real, 2.0 * out_real)
        doubled_imag = jnp.where(lead_columns, 0.0, 2.0 * out_imag)
        result = contract("cxr,xo->rco", doubled_real, inverse_x_cos) - contract(
            "cxr,xo->rco", doubled_imag, inverse_x_sin
        )
        return result + nyquist_part * alternating

    def effective_fine(state_now):
        padded_state = with_halo(state_now, (("space", 0),), 1)
        return (
            exchange_field(padded_state, padded_coupling) + demag_field(state_now) + applied_field
        )

    def propagate_coarse(magnet):
        padded_state = with_halo(magnet, (("space", 0),), 1)
        effective = (
            exchange_field(padded_state, padded_coupling) + applied_field + magnet * local_demag
        )
        return magnet + FINE * step_time * torque(magnet, effective)

    def coarse_sweep(jump_term):

        def one_turn(turn_index, loop_state):
            start_state, coarse_end, slice_end = loop_state
            start_state = jnp.where(is_first, initial_state, passed_along(slice_end, "tm", 1))
            coarse_end = propagate_coarse(start_state)
            return (start_state, coarse_end, coarse_end + jump_term)

        coarse_end = propagate_coarse(initial_state)
        return lax.fori_loop(
            0, slice_count - 1, one_turn, (initial_state, coarse_end, coarse_end + jump_term)
        )

    start_state, coarse_end, slice_end = coarse_sweep(jnp.zeros_like(initial_state))
    magnet = start_state
    for repeat in range(FINE):
        first_rate = torque(magnet, effective_fine(magnet))
        predicted = magnet + step_time * first_rate
        second_rate = torque(predicted, effective_fine(predicted))
        magnet = magnet + 0.5 * step_time * (first_rate + second_rate)
    jump_term = magnet - coarse_end
    start_state, coarse_end, slice_end = coarse_sweep(jump_term)
    return slice_end[None]


def turn_parts(grid, product):
    shifted = (product & (4 * grid - 1)) + grid // 2
    quarter = (shifted >> (grid.bit_length() - 1)) & 3
    rest = (shifted & (grid - 1)) - grid // 2
    angle = rest.astype(jnp.float32) * (math.pi / (2 * grid))
    square = angle * angle
    sine = -1.0 / 39916800.0
    for term in (1.0 / 362880.0, -1.0 / 5040.0, 1.0 / 120.0, -1.0 / 6.0, 1.0):
        sine = sine * square + term
    sine = sine * angle
    cosine = 1.0 / 479001600.0
    for term in (-1.0 / 3628800.0, 1.0 / 40320.0, -1.0 / 720.0, 1.0 / 24.0, -0.5, 1.0):
        cosine = cosine * square + term
    odd = (quarter & 1) == 1
    first = jnp.where(odd, sine, cosine)
    second = jnp.where(odd, cosine, sine)
    first = jnp.where((quarter == 1) | (quarter == 2), -first, first)
    second = jnp.where(quarter >= 2, -second, second)
    return (first, second)


def fill_table(grid, coarse, fine, sine, sign, out_ref, top=None):
    coarse_cos, coarse_sin = turn_parts(grid, coarse)
    fine_cos, fine_sin = turn_parts(grid, fine)
    lead = sign * jnp.where(sine, coarse_sin, coarse_cos)
    side = sign * jnp.where(sine, coarse_cos, -coarse_sin)
    for block in range(out_ref.shape[1] // 16):
        values = lead[block : block + 1] * fine_cos + side[block : block + 1] * fine_sin
        if top is not None and block == 0:
            first = lax.broadcasted_iota(jnp.int32, values.shape, 0) == 0
            values = jnp.where(first, top, values)
        high, low = split(values)
        out_ref[0, 16 * block : 16 * block + 16] = high
        out_ref[1, 16 * block : 16 * block + 16] = low


def tables_body(
    peers, halo, rank_ref, row_ref, cos_ref, sin_ref, back_cos_ref, back_sin_ref, tensor_ref
):
    rank = rank_ref[0]
    grid = row_ref.shape[1]
    width = grid // peers
    bits = width.bit_length() - 1
    late = rank >= peers // 2
    sign = jnp.where(late, -1.0, 1.0).astype(jnp.float32)
    base = jnp.where(late, peers - 1 - rank, rank)

    def iota(rows, columns, dim):
        return lax.broadcasted_iota(jnp.int32, (rows, columns), dim)

    lane = iota(grid // 16, 2 * grid, 1)
    sine = ((lane >> bits) & 1) == 1
    wave = ((lane >> (bits + 1)) ^ rank) * width + (lane & (width - 1))
    wave = jnp.where(sine & (wave == 0), grid, wave)
    sixteens = 32 * iota(grid // 16, 2 * grid, 0)
    ones = 2 * iota(16, 2 * grid, 0) - (grid - 1)
    fill_table(grid, sixteens * wave, ones * wave[:16], sine, 1.0, row_ref)

    half = grid // 2
    spot = iota(grid // 16, half, 1)
    place = 2 * (((spot >> bits) ^ base) * width + (spot & (width - 1))) - (grid - 1)
    sixteens = 16 * iota(grid // 16, half, 0) * place
    ones = iota(16, half, 0) * place[:16]
    edge = sign * turn_parts(grid, grid * place[:16])[1]
    fill_table(grid, sixteens, ones, False, 1.0, cos_ref)
    fill_table(grid, sixteens, ones, True, sign, sin_ref, top=edge)

    count = back_cos_ref.shape[1] // 16
    for out_ref, is_sine in ((back_cos_ref, False), (back_sin_ref, True)):
        number = iota(count, grid, 1)
        if is_sine:
            number = jnp.where(number == 0, grid, number)
        span = 32 * iota(count, grid, 0) * number
        start = (2 * (iota(16, grid, 0) - halo) - (grid - 1)) * number[:16]
        fill_table(grid, span, start, is_sine, sign if is_sine else 1.0, out_ref)

    def parts(row_number, column_number, weight):
        row_wave = (2.0 * math.pi / (2 * grid)) * signed(row_number)
        column_wave = (2.0 * math.pi / (2 * grid)) * signed(column_number)
        squared = row_wave * row_wave + column_wave * column_wave
        nonzero = squared > 0.0
        safe = jnp.where(nonzero, squared, 1.0)
        scaled = jnp.sqrt(safe) * thickness
        film = jnp.where(nonzero, (1.0 - jnp.exp(-scaled)) / scaled, 1.0)
        in_plane = (1.0 - film) / safe * weight
        edge = (row_number == grid) | (column_number == grid)
        return (
            in_plane * column_wave * column_wave,
            in_plane * row_wave * row_wave,
            film * weight,
            jnp.where(edge, 0.0, in_plane * column_wave * row_wave),
        )

    def signed(number):
        return jnp.where(number < grid, number, number - 2 * grid).astype(jnp.float32)

    columns = 2 * width
    for block in range(grid // 64):
        spots = slice(64 * block, 64 * block + 64)
        row_number = iota(64, columns, 0) + 64 * block
        lane = iota(64, columns, 1)
        is_sine = lane >= width
        column_number = rank * width + (lane & (width - 1))
        column_number = jnp.where(is_sine & (column_number == 0), grid, column_number)
        column_weight = jnp.where((column_number & (grid - 1)) == 0, 1.0, 2.0)
        weight = column_weight * jnp.where(row_number == 0, 1.0, 2.0) * (-0.25 / (grid * grid))
        found = parts(row_number, column_number, weight)
        for c in range(3):
            tensor_ref[c, spots] = found[c]
        tensor_ref[6, spots] = jnp.where(is_sine, -found[3], found[3])
        if block == 0:
            other = parts(jnp.where(row_number == 0, grid, row_number), column_number, weight)
            found = [jnp.where(row_number == 0, a, b) for a, b in zip(other, found)]
        for c in range(3):
            tensor_ref[3 + c, spots] = found[c]


def split(values):
    high = values.astype(jnp.bfloat16)
    low = (values - high.astype(jnp.float32)).astype(jnp.bfloat16)
    return (high, low)


def multiply(left, right, transposed=False):
    numbers = (((1,), (1 if transposed else 0,)), ((), ()))

    def one(a, b):
        return lax.dot_general(a, b, numbers, preferred_element_type=jnp.float32)

    return one(left[0], right[0]) + (one(left[0], right[1]) + one(left[1], right[0]))


def exchange_weights(coupling):
    rows, columns = coupling.shape
    place = lax.broadcasted_iota(jnp.int32, coupling.shape, 1)
    own = stiffness * coupling
    right = jnp.where(place < columns - 1, pltpu.roll(coupling, columns - 1, 1), 0.0)
    left = jnp.where(place > 0, pltpu.roll(coupling, 1, 1), 0.0)
    below = pltpu.roll(coupling, rows - 1, 0)
    above = pltpu.roll(coupling, 1, 0)
    return (own * right, own * left, own * below, own * above)


def exchange_of(part, weights):
    rows, columns = part.shape
    right, left, below, above = weights
    total = right * (pltpu.roll(part, columns - 1, 1) - part)
    total = total + left * (pltpu.roll(part, 1, 1) - part)
    total = total + below * (pltpu.roll(part, rows - 1, 0) - part)
    return total + above * (pltpu.roll(part, 1, 0) - part)


def cross(a, b):
    return (a[1] * b[2] - a[2] * b[1], a[2] * b[0] - a[0] * b[2], a[0] * b[1] - a[1] * b[0])


def torque_of(magnet, effective):
    first = cross(magnet, effective)
    second = cross(magnet, first)
    scale = -1.0 / (1.0 + damping * damping)
    return [scale * (a + damping * b) for a, b in zip(first, second)]


def coarse_step(magnet, applied, weights):
    effective = [exchange_of(part, weights) + field for part, field in zip(magnet, applied)]
    effective[2] = effective[2] - magnet[2]
    return [part + FINE * step_time * rate for part, rate in zip(magnet, torque_of(magnet, effective))]


def vmem_call(body, outs, name, scalars=0, scratch=(), cost=10**8):
    whole = pl.BlockSpec(memory_space=pltpu.VMEM)

    def call(*args):
        first = [pl.BlockSpec(memory_space=pltpu.SMEM)] * scalars
        return pl.pallas_call(
            body,
            out_shape=[
                out if isinstance(out, jax.ShapeDtypeStruct) else jax.ShapeDtypeStruct(out, jnp.float32)
                for out in outs
            ],
            in_specs=first + [whole] * (len(args) - scalars),
            out_specs=[whole] * len(outs),
            scratch_shapes=[pltpu.VMEM(shape, jnp.float32) for shape in scratch],
            compiler_params=pltpu.CompilerParams(vmem_limit_bytes=VMEM_LIMIT),
            cost_estimate=pl.CostEstimate(flops=cost, bytes_accessed=10**6, transcendentals=0),
            name=name,
        )(*args)

    return call


def pack_body(reach, state_ref, applied_ref, coupling_ref, own_ref, top_ref, bottom_ref):
    rows = coupling_ref.shape[0]
    for c in range(3):
        own_ref[c] = state_ref[c]
        own_ref[3 + c] = applied_ref[c]
    own_ref[6] = coupling_ref[...]
    for ref, first in ((top_ref, 0), (bottom_ref, rows - reach)):
        for c in range(7):
            ref[c * reach : (c + 1) * reach] = own_ref[c, first : first + reach]
        if 7 * reach < ref.shape[0]:
            ref[7 * reach :] = jnp.zeros_like(ref[7 * reach :])


def pieces(values):
    high = values.astype(jnp.bfloat16)
    rest = values - high.astype(jnp.float32)
    middle = rest.astype(jnp.bfloat16)
    low = (rest - middle.astype(jnp.float32)).astype(jnp.bfloat16)
    return (high, middle, low)


def choose(selection, parts):
    first, second, third = (
        jnp.dot(selection, part, preferred_element_type=jnp.float32) for part in parts
    )
    return first + (second + third)


def build_wide(flipped, reach, state_ref, applied_ref, coupling_ref, before, after, wide_ref):
    rows = coupling_ref.shape[0]
    count = before.shape[0]
    total = wide_ref.shape[1]
    margin = (total - rows) // 2

    def matrix(fields, columns, base):
        row = lax.broadcasted_iota(jnp.int32, (fields * total, columns), 0)
        column = lax.broadcasted_iota(jnp.int32, (fields * total, columns), 1)
        field, row = (row // total, row % total)
        row = jnp.where(flipped == 1, total - 1 - row, row) - base
        size = reach if fields > 1 else columns
        inside = (row >= 0) & (row < size) & (column == field * size + row)
        return jnp.where(inside, 1.0, 0.0).astype(jnp.bfloat16)

    own = matrix(1, rows, margin)
    edges = choose(matrix(7, count, margin - reach), pieces(before))
    edges = edges + choose(matrix(7, count, margin + rows), pieces(after))
    fields = [state_ref[c] for c in range(3)] + [applied_ref[c] for c in range(3)]
    fields.append(coupling_ref[...])
    for number, field in enumerate(fields):
        wide_ref[number] = choose(own, pieces(field)) + edges[number * total : (number + 1) * total]


def wide_body(reach, flip_ref, fine_flip_ref, own_ref, *refs):
    edge_refs, wide_ref = (refs[:4], refs[4])
    kept = flip_ref[0] == fine_flip_ref[0]
    before, after = (
        jnp.where(kept, edge_refs[i][...], edge_refs[2 + i][...]) for i in range(2)
    )
    fields = (own_ref.at[0:3], own_ref.at[3:6], own_ref.at[6])
    build_wide(flip_ref[0], reach, *fields, before, after, wide_ref)


def start_body(reach, slices, turn_ref, flip_ref, *refs):
    first_ref, around_ref, wide_ref = refs[5:]
    turn = turn_ref[0]
    build_wide(flip_ref[0], reach, *refs[:3], refs[3][...], refs[4][...], wide_ref)
    rows = first_ref.shape[1]
    margin = (wide_ref.shape[1] - rows) // 2
    kept = slice(margin, margin + rows)
    weights = exchange_weights(wide_ref[6])
    applied = [wide_ref[3 + c] for c in range(3)]
    for number, values in enumerate(applied + list(weights)):
        around_ref[number] = values[kept]
    for c in range(3):
        first_ref[c] = wide_ref[c, kept]
    for number in range(1, slices):
        @pl.when(turn >= number)
        def step():
            magnet = coarse_step([wide_ref[c] for c in range(3)], applied, weights)
            for c in range(3):
                wide_ref[c] = magnet[c]
                first_ref[c] = magnet[c][kept]


def first_is_end(rank):
    return (rank & 1) == jnp.where(rank >= 4, 1, 0)


def send_rows(magnet, rank, table, out_refs):
    rows, grid = magnet[0].shape
    width = out_refs[0].shape[1]
    block = split(jnp.concatenate(magnet, axis=0))
    spectrum = multiply(block, table)
    at_end = first_is_end(rank)
    for slot, out_ref in enumerate(out_refs):
        out_ref[: 3 * rows] = spectrum[:, slot * width : (slot + 1) * width]
        if out_ref.shape[0] > 3 * rows:
            which = at_end if slot == 1 else jnp.logical_not(at_end)
            place = 3 * rows
            for part in magnet:
                edge = jnp.where(which, part[rows - 1 :], part[:1])
                for start in range(0, grid, width):
                    out_ref[place : place + 1] = edge[:, start : start + width]
                    place += 1
            rest = out_ref.shape[0] - place
            out_ref[place:] = jnp.zeros((rest, width), jnp.float32)


def edge_rows(rank, near_ref, far_ref, middle_ref, rows):
    width = near_ref.shape[1]
    count = rows * 3
    at_end = first_is_end(rank)
    outer = (rank == 0) | (rank == 7)
    central = (rank == 3) | (rank == 4)
    grid = 4 * width
    pairs = []
    for c in range(3):
        near, far, middle = (
            jnp.concatenate(
                [
                    ref[count + c * (grid // width) + j : count + c * (grid // width) + j + 1]
                    for j in range(grid // width)
                ],
                axis=1,
            )
            for ref in (near_ref, far_ref, middle_ref)
        )
        other = jnp.where(central, middle, far)
        start = jnp.where(at_end, jnp.where(outer, jnp.zeros_like(far), far), near)
        pairs.append((start, jnp.where(at_end, near, other)))
    return pairs


def rows_body(rank_ref, state_ref, table_ref, *out_refs):
    send_rows([state_ref[c] for c in range(3)], rank_ref[0], (table_ref[0], table_ref[1]), out_refs)


def spectrum_body(peers, rows, base_ref, *refs):
    in_refs, refs = (refs[:peers], refs[peers:])
    tensor_ref, cos_ref, sin_ref, back_cos_ref, back_sin_ref = refs[:5]
    out_refs = refs[5 : 5 + peers]
    front_ref, back_ref = refs[5 + peers :]
    width = in_refs[0].shape[1]
    half = peers // 2

    def part(slot, c):
        return in_refs[slot][c * rows : (c + 1) * rows]

    def fold(sign):
        return jnp.concatenate(
            [
                jnp.concatenate(
                    [part(p, c) + sign * part(peers - 1 - p, c) for p in range(half)], axis=0
                )
                for c in range(3)
            ],
            axis=1,
        )

    even = multiply((cos_ref[0], cos_ref[1]), split(fold(1.0)))
    odd = multiply((sin_ref[0], sin_ref[1]), split(fold(-1.0)))
    even_x, even_y, even_z = (even[:, c * width : (c + 1) * width] for c in range(3))
    odd_x, odd_y, odd_z = (odd[:, c * width : (c + 1) * width] for c in range(3))
    mixed = tensor_ref[6]

    def turned(values):
        return mixed * pltpu.roll(values, width // 2, 1)

    even_out = jnp.concatenate(
        [
            tensor_ref[0] * even_x - turned(odd_y),
            tensor_ref[1] * even_y - turned(odd_x),
            tensor_ref[2] * even_z,
        ],
        axis=1,
    )
    odd_out = jnp.concatenate(
        [
            tensor_ref[3] * odd_x + turned(even_y),
            tensor_ref[4] * odd_y + turned(even_x),
            tensor_ref[5] * odd_z,
        ],
        axis=1,
    )
    even_rows = multiply((back_cos_ref[0], back_cos_ref[1]), split(even_out))
    odd_rows = multiply((back_sin_ref[0], back_sin_ref[1]), split(odd_out))
    front_ref[...] = even_rows + odd_rows
    back_ref[...] = even_rows - odd_rows
    base = base_ref[0]
    for p in range(half):
        span = pl.ds(pl.multiple_of((base ^ p) * rows, 8), rows)
        for c in range(3):
            kept = slice(c * rows, (c + 1) * rows)
            out_refs[p][kept] = front_ref[span, c * width : (c + 1) * width]
            out_refs[peers - 1 - p][kept] = back_ref[span, c * width : (c + 1) * width]


def exchange_inside(part, weights, start, end):
    rows, columns = part.shape
    right, left, below, above = weights
    row = lax.broadcasted_iota(jnp.int32, part.shape, 0)
    following = jnp.where(row == rows - 1, end, pltpu.roll(part, rows - 1, 0))
    preceding = jnp.where(row == 0, start, pltpu.roll(part, 1, 0))
    total = right * (pltpu.roll(part, columns - 1, 1) - part)
    total = total + left * (pltpu.roll(part, 1, 1) - part)
    total = total + below * (following - part)
    return total + above * (preceding - part)


def field_rates(rank, in_refs, edge_refs, magnet, around_ref, table):
    rows = magnet[0].shape[0]
    spectrum = jnp.concatenate([ref[...] for ref in in_refs], axis=1)
    demag = multiply(split(spectrum), table, transposed=True)
    edges = edge_rows(rank, *edge_refs, rows)
    weights = [around_ref[3 + c] for c in range(4)]
    effective = [
        exchange_inside(magnet[c], weights, *edges[c])
        + demag[c * rows : (c + 1) * rows]
        + around_ref[c]
        for c in range(3)
    ]
    return torque_of(magnet, effective)


def predict_body(peers, rank_ref, *refs):
    in_refs, edge_refs, refs = (refs[:peers], refs[peers : peers + 3], refs[peers + 3 :])
    state_ref, around_ref, table_ref = refs[:3]
    send_refs, (predicted_ref, base_ref) = (refs[3 : 3 + peers], refs[3 + peers :])
    rank = rank_ref[0]
    table = (table_ref[0], table_ref[1])
    magnet = [state_ref[c] for c in range(3)]
    rates = field_rates(rank, in_refs, edge_refs, magnet, around_ref, table)
    predicted = [part + step_time * rate for part, rate in zip(magnet, rates)]
    send_rows(predicted, rank, table, send_refs)
    for c in range(3):
        predicted_ref[c] = predicted[c]
        base_ref[c] = magnet[c] + 0.5 * step_time * rates[c]


def correct_body(peers, rank_ref, *refs):
    in_refs, edge_refs, refs = (refs[:peers], refs[peers : peers + 3], refs[peers + 3 :])
    state_ref, base_ref, around_ref, table_ref = refs[:4]
    send_refs, following_ref = (refs[4 : 4 + peers], refs[4 + peers])
    rank = rank_ref[0]
    table = (table_ref[0], table_ref[1])
    magnet = [state_ref[c] for c in range(3)]
    rates = field_rates(rank, in_refs, edge_refs, magnet, around_ref, table)
    following = [base_ref[c] + 0.5 * step_time * rates[c] for c in range(3)]
    send_rows(following, rank, table, send_refs)
    for c in range(3):
        following_ref[c] = following[c]


def end_body(peers, share, trim, slices, rank_ref, number_ref, *refs):
    in_refs, edge_refs, refs = (refs[:peers], refs[peers : peers + 3], refs[peers + 3 :])
    state_ref, base_ref, around_ref, table_ref = refs[:4]
    strip_refs, margin_refs, end_ref = (refs[4 : 4 + slices], refs[4 + slices : -1], refs[-1])
    rank, number = (rank_ref[0], number_ref[0])
    magnet = [state_ref[c] for c in range(3)]
    rows = magnet[0].shape[0]
    table = (table_ref[0], table_ref[1])
    rates = field_rates(rank, in_refs, edge_refs, magnet, around_ref, table)
    blank = jnp.zeros((trim, magnet[0].shape[1]), jnp.float32)
    for c in range(3):
        end_ref[c, :trim] = blank
        end_ref[c, trim + rows :] = blank
        end_ref[c, trim : trim + rows] = base_ref[c] + 0.5 * step_time * rates[c]
    central = (rank == 3) | (rank == 4)
    for t in range(slices):
        start = pl.multiple_of((number ^ t) * share, 8)
        ending = number == t
        for c in range(3):
            strip_refs[t][c] = end_ref[c, pl.ds(start, strip_refs[t].shape[1])]
            for i in range(trim):
                head = end_ref[c, trim + i : trim + i + 1]
                tail = end_ref[c, rows + i : rows + i + 1]
                mirrored = end_ref[c, trim + rows - 1 - i : trim + rows - i]
                tail = jnp.where(central, mirrored, tail)
                margin_refs[t][c * trim + i : c * trim + i + 1] = jnp.where(ending, tail, head)
        margin_refs[t][3 * trim :] = jnp.zeros_like(margin_refs[t][3 * trim :])


def finish_body(slices, trim, turn_ref, block_ref, *refs):
    in_refs, margin_refs, refs = (refs[:slices], refs[slices : 2 * slices], refs[2 * slices :])
    wide_ref, out_refs = (refs[0], refs[1 : slices + 1])
    fine_ref, edge_ref, end_ref = refs[slices + 1 :]
    turn, block = (turn_ref[0], block_ref[0])
    rows = fine_ref.shape[2]
    share = rows - 2 * trim
    central = (block == 3) | (block == 4)
    straight = (turn == 0) | central
    for t in range(slices):
        fine_ref[turn ^ t] = in_refs[t][...]
        edge_ref[jnp.where(straight, t, t ^ 3)] = margin_refs[t][...]
    row = lax.broadcasted_iota(jnp.int32, (rows, fine_ref.shape[3]), 0)
    patched = ((turn == 0) & (row < trim)) | ((turn == slices - 1) & (row >= rows - trim))
    blank = jnp.zeros((share, fine_ref.shape[3]), jnp.float32)

    def fine(number, c):
        edge = edge_ref[number, c * trim : (c + 1) * trim]
        return jnp.where(patched, jnp.concatenate([edge, blank, edge], axis=0), fine_ref[number, c])

    margin = (wide_ref.shape[1] - slices * share) // 2
    start = pl.multiple_of(turn * share + margin - 8, 8)

    def strip(number):
        return wide_ref[number, pl.ds(start, share + 16)][8 - trim : 8 + share + trim]

    weights = exchange_weights(strip(6))
    applied = [strip(3 + c) for c in range(3)]
    first = [strip(c) for c in range(3)]
    magnet = first
    for number in range(slices):
        first = coarse_step(first, applied, weights)
        ahead = coarse_step(magnet, applied, weights) if number > 0 else first
        magnet = [ahead[c] + (fine(number, c) - first[c]) for c in range(3)]
        for c in range(3):
            end_ref[number, c] = magnet[c][trim : trim + share]
    for t in range(slices):
        out_refs[t][...] = end_ref[turn ^ t]


def gather_body(slices, turn_ref, flip_ref, *refs):
    in_refs, out_ref = (refs[:slices], refs[slices])
    turn, flipped = (turn_ref[0], flip_ref[0])
    share = in_refs[0].shape[1]
    row = lax.broadcasted_iota(jnp.int32, (share, share), 0)
    column = lax.broadcasted_iota(jnp.int32, (share, share), 1)
    row = jnp.where(flipped == 1, share - 1 - row, row)
    matrix = jnp.where(row == column, 1.0, 0.0).astype(jnp.bfloat16)
    for t in range(slices):
        strip = turn ^ t
        strip = jnp.where(flipped == 1, slices - 1 - strip, strip)
        span = pl.ds(pl.multiple_of(strip * share, 8), share)
        for c in range(3):
            out_ref[c, span] = choose(matrix, pieces(in_refs[t][c]))


def shards_by_block(initial_state, applied_field, coupling):
    rows, _, grid = initial_state.shape
    group = ("core", "z_low", "y")
    peers = 8
    slices = 4
    margin, trim, reach = (8, 4, 4)
    width = grid // peers
    space = ("z_high", "z_low", "y")
    blocks = 8
    def scalar(value):
        return value.astype(jnp.int32).reshape(1)

    rank = lax.axis_index(group)
    half = lax.axis_index("z_high")
    turn = lax.axis_index(("x", "core"))
    number = 2 * lax.axis_index("x") + half
    base = jnp.where(rank < peers // 2, rank, peers - 1 - rank)
    scalars = (rank, half, lax.axis_index("core"), turn, number, base, lax.axis_index(space))
    rank, native_flip, fine_flip, turn, number, base, block = lax.optimization_barrier(
        tuple(value.astype(jnp.int32).reshape(1) for value in scalars)
    )

    state_in = jnp.transpose(initial_state, (1, 0, 2))
    applied_in = jnp.transpose(applied_field, (1, 0, 2))
    edge_shape = (-(-7 * reach // 8) * 8, grid)
    native, top, bottom = vmem_call(
        functools.partial(pack_body, reach), [(7, rows, grid), edge_shape, edge_shape], "pack"
    )(state_in, applied_in, coupling)

    def trade(values):
        return lax.ppermute(values, ("core", "z_high"), [(0, 0), (1, 2), (2, 1), (3, 3)])

    def edge_route(step):
        route = []
        for core in range(2):
            for block in range(blocks):
                following = block + step
                if 0 <= following < blocks:
                    target = (following // 4, core, following % 4)
                    route.append((8 * core + block, 8 * target[0] + 4 * target[1] + target[2]))
        return route

    everywhere = ("core",) + space
    before = lax.ppermute(bottom, everywhere, edge_route(1))
    after = lax.ppermute(top, everywhere, edge_route(-1))
    own = (trade(state_in), trade(applied_in), trade(coupling))

    def pair(*shape):
        return jax.ShapeDtypeStruct((2,) + shape, jnp.bfloat16)

    back_rows = grid // 2
    row_table, *column_tables, tensor = vmem_call(
        functools.partial(tables_body, peers, 0),
        [pair(grid, 2 * grid)]
        + [pair(grid, grid // 2)] * 2
        + [pair(back_rows, grid)] * 2
        + [(7, grid, 2 * width)],
        "tables",
        scalars=1,
    )(rank)

    state_shape = (3, rows, grid)
    wide_shape = (7, rows + 2 * margin, grid)
    state, around = vmem_call(
        functools.partial(start_body, reach, slices),
        [state_shape, (7, rows, grid)],
        "start",
        scalars=2,
        scratch=[wide_shape],
    )(number, fine_flip, *own, before, after)
    def spread(slots):
        return [slots[0]] + [
            lax.ppermute(slots[k], group, [(i, i ^ k) for i in range(peers)])
            for k in range(1, peers)
        ]

    lanes = 2 * width
    extra = -(-3 * grid // lanes // 8) * 8
    near, far, middle = (1, 3, 7)
    send_shapes = [
        (3 * rows + (extra if slot in (near, far, middle) else 0), lanes) for slot in range(peers)
    ]

    def demag_blocks(received):
        return received, vmem_call(
            functools.partial(spectrum_body, peers, rows),
            [(3 * rows, lanes)] * peers,
            "spectrum",
            scalars=1,
            scratch=[(back_rows, 3 * lanes)] * 2,
            cost=10**9,
        )(base, *received, tensor, *column_tables)

    def complete(received, blocks_back):
        return spread(blocks_back) + [received[slot] for slot in (near, far, middle)]

    sent = vmem_call(rows_body, send_shapes, "rows", scalars=1)(rank, state, row_table)
    for repeat in range(FINE):
        received = spread(sent)
        received = complete(*demag_blocks(received))
        *sent, predicted, start = vmem_call(
            functools.partial(predict_body, peers), send_shapes + [state_shape] * 2, "predict", scalars=1, cost=10**9
        )(rank, *received, state, around, row_table)
        received = complete(*demag_blocks(spread(sent)))
        if repeat < FINE - 1:
            *sent, state = vmem_call(
                functools.partial(correct_body, peers), send_shapes + [state_shape], "correct", scalars=1, cost=10**9
            )(rank, *received, predicted, start, around, row_table)
    swap = [(0, 1), (1, 0)]
    (wide,) = vmem_call(functools.partial(wide_body, reach), [wide_shape], "wide", scalars=2)(
        native_flip,
        fine_flip,
        native,
        before,
        after,
        lax.ppermute(before, "core", swap),
        lax.ppermute(after, "core", swap),
    )
    share = rows // slices
    strip_shape = (3, share + 2 * trim, grid)
    margin_shape = (-(-3 * trim // 8) * 8, grid)
    ending = vmem_call(
        functools.partial(end_body, peers, share, trim, slices),
        [strip_shape] * slices + [margin_shape] * slices,
        "end",
        scalars=2,
        scratch=[(3, rows + 2 * trim, grid)],
    )(rank, number, *received, predicted, start, around, row_table)
    strips, margins = (ending[:slices], ending[slices:])

    def margin_route(t):
        route = []
        for s in range(blocks):
            if s in (3, 4):
                beyond = (7 - s, slices - 1)
            else:
                beyond = (s + 1 if s < 4 else s - 1, 0)
            ahead = s - 1 if s < 4 else s + 1
            for n, (block_to, strip) in ((t, beyond), (t ^ 3, (ahead, slices - 1))):
                if 0 <= block_to < blocks:
                    source = 16 * (n // 2) + 8 * (s // 4) + 4 * (n % 2) + s % 4
                    route.append((source, 8 * strip + block_to))
        return route

    def strip_route(t):
        route = []
        for i in range(8):
            x, core, z = (i // 4, i // 2 % 2, i % 2)
            route.append((i, 4 * (x ^ (t // 2)) + 2 * (z ^ (t % 2)) + core))
        return route

    strips = [
        lax.ppermute(strips[t], ("x", "core", "z_high"), strip_route(t)) for t in range(slices)
    ]
    margins = [
        lax.ppermute(margins[t], ("x",) + everywhere, margin_route(t)) for t in range(slices)
    ]
    ends = vmem_call(
        functools.partial(finish_body, slices, trim),
        [(3, share, grid)] * slices,
        "finish",
        scalars=2,
        scratch=[
            (slices,) + strip_shape,
            (slices,) + margin_shape,
            (slices, 3, share, grid),
        ],
    )(turn, block, *strips, *margins, wide)
    ends = [ends[0]] + [
        lax.ppermute(ends[t], ("x", "core"), [(i, i ^ t) for i in range(slices)])
        for t in range(1, slices)
    ]
    (result,) = vmem_call(
        functools.partial(gather_body, slices), [(3, rows, grid)], "gather", scalars=2
    )(turn, native_flip, *ends)
    return jnp.transpose(result, (1, 0, 2))[None]


def fits_blocks(mesh):
    return mesh.shape["tm"] == 4 and mesh.shape["space"] == 8


def solution(mesh):
    if not fits_blocks(mesh):
        in_specs = (P("space", None, None), P("space", None, None), P("space", None))
        out_specs = P("tm", "space", None, None)
        return jax.shard_map(
            shards, mesh=mesh, in_specs=in_specs, out_specs=out_specs, check_vma=False
        )
    fine_mesh = Mesh(
        mesh.devices.reshape(2, 2, 2, 2, 2), ("x", "core", "z_high", "z_low", "y")
    )
    space = ("z_high", "z_low", "y")
    in_specs = (P(space, None, None), P(space, None, None), P(space, None))
    out_specs = P(("x", "core"), space, None, None)
    return jax.shard_map(
        shards_by_block, mesh=fine_mesh, in_specs=in_specs, out_specs=out_specs, check_vma=False
    )
```

```python
import functools
import math

import jax
import jax.numpy as jnp
from jax import lax
from jax.experimental import pallas as pl
from jax.experimental.pallas import tpu as pltpu
from jax.sharding import Mesh
from jax.sharding import PartitionSpec as P

FINE = 2
VMEM_LIMIT = 16 * 1024 * 1024


step_time = 0.06
damping = 0.02
stiffness = 0.25
thickness = 8.0


def with_halo(x, sides, width):
    for axis, dim in sides:
        peers, length = (lax.axis_size(axis), x.shape[dim])
        up = [(i, (i + 1) % peers) for i in range(peers - 1)]
        down = [(j, i) for i, j in up]
        last = lax.slice_in_dim(x, length - width, length, axis=dim)
        initial = lax.slice_in_dim(x, 0, width, axis=dim)
        before = lax.ppermute(last, axis, up)
        after = lax.ppermute(initial, axis, down)
        x = jnp.concatenate([before, x, after], axis=dim)
    return x


def passed_along(block, axis, distance):
    devices = range(lax.axis_size(axis))
    route = [(i - distance, i) for i in devices if i - distance in devices]
    return lax.ppermute(block, axis, route)


def spectral_tensor(row_index, column_index, length):
    half_length = length // 2
    signed_rows = jnp.where(row_index < half_length, row_index, row_index - length).astype(
        jnp.float32
    )
    signed_columns = jnp.where(
        column_index < half_length, column_index, column_index - length
    ).astype(jnp.float32)
    wave_rows = 2.0 * math.pi / length * signed_rows[:, None]
    wave_columns = 2.0 * math.pi / length * signed_columns[None, :]
    squared = wave_rows * wave_rows + wave_columns * wave_columns
    nonzero = squared > 0.0
    safe_square = jnp.where(nonzero, squared, 1.0)
    scaled_wave = jnp.sqrt(safe_square) * thickness
    film_factor = jnp.where(nonzero, (1.0 - jnp.exp(-scaled_wave)) / scaled_wave, 1.0)
    in_plane = (1.0 - film_factor) / safe_square
    nyquist = (row_index[:, None] == half_length) | (column_index[None, :] == half_length)
    normalizer = -1.0 / (length * length)
    tensor_first = in_plane * wave_columns * wave_columns * normalizer
    tensor_second = in_plane * wave_rows * wave_rows * normalizer
    tensor_cross = jnp.where(nyquist, 0.0, in_plane * wave_columns * wave_rows) * normalizer
    tensor_normal = film_factor * normalizer
    return (tensor_first, tensor_second, tensor_cross, tensor_normal)


def exchange_field(padded_state, padded_coupling):
    center_state = padded_state[1:-1]
    center_coupling = padded_coupling[1:-1]
    wide_state = jnp.pad(padded_state, ((0, 0), (0, 0), (1, 1)))
    wide_coupling = jnp.pad(padded_coupling, ((0, 0), (1, 1)))
    neighbour_sum = padded_coupling[2:, None, :] * (padded_state[2:] - center_state)
    neighbour_sum = neighbour_sum + padded_coupling[:-2, None, :] * (
        padded_state[:-2] - center_state
    )
    neighbour_sum = neighbour_sum + wide_coupling[1:-1, None, 2:] * (
        wide_state[1:-1, :, 2:] - center_state
    )
    neighbour_sum = neighbour_sum + wide_coupling[1:-1, None, :-2] * (
        wide_state[1:-1, :, :-2] - center_state
    )
    return stiffness * center_coupling[:, None, :] * neighbour_sum


def torque(magnet, effective):
    first_cross = jnp.cross(magnet, effective, axis=1)
    second_cross = jnp.cross(magnet, first_cross, axis=1)
    return -(first_cross + damping * second_cross) / (1.0 + damping * damping)


def phase_table(row_count, column_count, period, direction):
    row_ids = lax.broadcasted_iota(jnp.int32, (row_count, column_count), 0)
    column_ids = lax.broadcasted_iota(jnp.int32, (row_count, column_count), 1)
    angles = (row_ids * column_ids % period).astype(jnp.float32) * (2.0 * math.pi / period)
    return (jnp.cos(angles), direction * jnp.sin(angles))


def joined_table(row_count, column_count, period, direction):
    table_cos, table_sin = phase_table(row_count, column_count, period, direction)
    return jnp.concatenate([table_cos, table_sin], axis=1)


def contract(pattern, left, right):
    return jnp.einsum(pattern, left, right, precision=lax.Precision.HIGHEST)


def complex_apply(pattern, real_part, imag_part, joined):
    half_width = joined.shape[-1] // 2
    real_both = contract(pattern, real_part, joined)
    imag_both = contract(pattern, imag_part, joined)
    return (
        real_both[..., :half_width] - imag_both[..., half_width:],
        real_both[..., half_width:] + imag_both[..., :half_width],
    )


def apply_tensor(real_part, imag_part, tensor):
    tensor_first, tensor_second, tensor_cross, tensor_normal = tensor

    def mix_components(values):
        return jnp.stack(
            [
                tensor_first * values[0] + tensor_cross * values[1],
                tensor_cross * values[0] + tensor_second * values[1],
                tensor_normal * values[2],
            ],
            axis=0,
        )

    return (mix_components(real_part), mix_components(imag_part))


def shards(initial_state, applied_field, coupling):
    row_count, component_count, grid_size = initial_state.shape
    length = 2 * grid_size
    space_count = lax.axis_size("space")
    space_index = lax.axis_index("space")
    slice_count = lax.axis_size("tm")
    slice_index = lax.axis_index("tm")
    is_first = slice_index == 0
    padded_coupling = with_halo(coupling, (("space", 0),), 1)
    index_all = jnp.arange(length, dtype=jnp.int32)
    local_demag = jnp.array([0.0, 0.0, -1.0], dtype=jnp.float32).reshape(1, 3, 1)
    forward_y = joined_table(grid_size, length, length, -1.0)
    inverse_y = joined_table(length, grid_size, length, 1.0)

    def transform_columns(real_part, imag_part):
        return complex_apply("yca,yk->cak", real_part, imag_part, forward_y)

    column_width = grid_size // space_count
    columns = space_index * column_width + jnp.arange(column_width, dtype=jnp.int32)
    tensor = tuple((part_table.T for part_table in spectral_tensor(index_all, columns, length)))
    edge_first, edge_second, edge_cross, edge_normal = spectral_tensor(
        index_all, jnp.array([0, grid_size], dtype=jnp.int32), length
    )
    anchor_diag = jnp.stack([edge_first[:, 0], edge_second[:, 0], edge_normal[:, 0]], axis=0)
    nyquist_diag = jnp.stack([edge_first[:, 1], edge_second[:, 1], edge_normal[:, 1]], axis=0)
    mean_diag = 0.5 * (anchor_diag + nyquist_diag)
    half_gap = 0.5 * (anchor_diag - nyquist_diag)
    is_anchor = (columns == 0)[None, :, None]
    column_ids = jnp.arange(grid_size, dtype=jnp.int32)
    is_lead = column_ids == 0
    lead_columns = is_lead[None, :, None]
    alternating = jnp.where(column_ids % 2 == 0, 1.0, -1.0).astype(jnp.float32)
    forward_x = joined_table(grid_size, grid_size, length, -1.0)
    inverse_x_cos, inverse_x_sin = phase_table(grid_size, grid_size, length, 1.0)

    def demag_field(magnet):
        both_parts = contract("rcx,xk->rck", magnet, forward_x)
        packed_real = both_parts[..., :grid_size]
        imag_part = both_parts[..., grid_size:]
        nyquist_column = jnp.einsum(
            "rcx,x->rc", magnet, alternating, precision=lax.Precision.HIGHEST
        )
        packed_imag = jnp.where(is_lead, nyquist_column[:, :, None], imag_part)
        real_part, imag_part = (
            lax.all_to_all(packed_real, "space", split_axis=2, concat_axis=0, tiled=True),
            lax.all_to_all(packed_imag, "space", split_axis=2, concat_axis=0, tiled=True),
        )
        real_part, imag_part = transform_columns(real_part, imag_part)
        out_real, out_imag = apply_tensor(real_part, imag_part, tensor)
        lead_real = real_part[:, 0, :]
        lead_imag = imag_part[:, 0, :]
        mirror_real = jnp.concatenate([lead_real[:, :1], lead_real[:, 1:][:, ::-1]], axis=1)
        mirror_imag = jnp.concatenate([lead_imag[:, :1], lead_imag[:, 1:][:, ::-1]], axis=1)
        fixed_real = mean_diag * lead_real + half_gap * mirror_real
        fixed_imag = mean_diag * lead_imag - half_gap * mirror_imag
        out_real = jnp.where(is_anchor, fixed_real[:, None, :], out_real)
        out_imag = jnp.where(is_anchor, fixed_imag[:, None, :], out_imag)
        out_real, out_imag = complex_apply("cak,ky->cay", out_real, out_imag, inverse_y)
        out_real, out_imag = (
            lax.all_to_all(out_real, "space", split_axis=2, concat_axis=1, tiled=True),
            lax.all_to_all(out_imag, "space", split_axis=2, concat_axis=1, tiled=True),
        )
        nyquist_part = jnp.transpose(out_imag[:, :1, :], (2, 0, 1))
        doubled_real = jnp.where(lead_columns, out_real, 2.0 * out_real)
        doubled_imag = jnp.where(lead_columns, 0.0, 2.0 * out_imag)
        result = contract("cxr,xo->rco", doubled_real, inverse_x_cos) - contract(
            "cxr,xo->rco", doubled_imag, inverse_x_sin
        )
        return result + nyquist_part * alternating

    def effective_fine(state_now):
        padded_state = with_halo(state_now, (("space", 0),), 1)
        return (
            exchange_field(padded_state, padded_coupling) + demag_field(state_now) + applied_field
        )

    def propagate_coarse(magnet):
        padded_state = with_halo(magnet, (("space", 0),), 1)
        effective = (
            exchange_field(padded_state, padded_coupling) + applied_field + magnet * local_demag
        )
        return magnet + FINE * step_time * torque(magnet, effective)

    def coarse_sweep(jump_term):

        def one_turn(turn_index, loop_state):
            start_state, coarse_end, slice_end = loop_state
            start_state = jnp.where(is_first, initial_state, passed_along(slice_end, "tm", 1))
            coarse_end = propagate_coarse(start_state)
            return (start_state, coarse_end, coarse_end + jump_term)

        coarse_end = propagate_coarse(initial_state)
        return lax.fori_loop(
            0, slice_count - 1, one_turn, (initial_state, coarse_end, coarse_end + jump_term)
        )

    start_state, coarse_end, slice_end = coarse_sweep(jnp.zeros_like(initial_state))
    magnet = start_state
    for repeat in range(FINE):
        first_rate = torque(magnet, effective_fine(magnet))
        predicted = magnet + step_time * first_rate
        second_rate = torque(predicted, effective_fine(predicted))
        magnet = magnet + 0.5 * step_time * (first_rate + second_rate)
    jump_term = magnet - coarse_end
    start_state, coarse_end, slice_end = coarse_sweep(jump_term)
    return slice_end[None]


def turn_parts(grid, product):
    shifted = (product & (4 * grid - 1)) + grid // 2
    quarter = (shifted >> (grid.bit_length() - 1)) & 3
    rest = (shifted & (grid - 1)) - grid // 2
    angle = rest.astype(jnp.float32) * (math.pi / (2 * grid))
    square = angle * angle
    sine = -1.0 / 39916800.0
    for term in (1.0 / 362880.0, -1.0 / 5040.0, 1.0 / 120.0, -1.0 / 6.0, 1.0):
        sine = sine * square + term
    sine = sine * angle
    cosine = 1.0 / 479001600.0
    for term in (-1.0 / 3628800.0, 1.0 / 40320.0, -1.0 / 720.0, 1.0 / 24.0, -0.5, 1.0):
        cosine = cosine * square + term
    odd = (quarter & 1) == 1
    first = jnp.where(odd, sine, cosine)
    second = jnp.where(odd, cosine, sine)
    first = jnp.where((quarter == 1) | (quarter == 2), -first, first)
    second = jnp.where(quarter >= 2, -second, second)
    return (first, second)


def fill_table(grid, coarse, fine, sine, sign, out_ref, top=None):
    coarse_cos, coarse_sin = turn_parts(grid, coarse)
    fine_cos, fine_sin = turn_parts(grid, fine)
    lead = sign * jnp.where(sine, coarse_sin, coarse_cos)
    side = sign * jnp.where(sine, coarse_cos, -coarse_sin)
    for block in range(out_ref.shape[1] // 16):
        values = lead[block : block + 1] * fine_cos + side[block : block + 1] * fine_sin
        if top is not None and block == 0:
            first = lax.broadcasted_iota(jnp.int32, values.shape, 0) == 0
            values = jnp.where(first, top, values)
        high, low = split(values)
        out_ref[0, 16 * block : 16 * block + 16] = high
        out_ref[1, 16 * block : 16 * block + 16] = low


def tables_body(
    peers, halo, rank_ref, row_ref, cos_ref, sin_ref, back_cos_ref, back_sin_ref, tensor_ref
):
    rank = rank_ref[0]
    grid = row_ref.shape[1]
    width = grid // peers
    bits = width.bit_length() - 1
    late = rank >= peers // 2
    sign = jnp.where(late, -1.0, 1.0).astype(jnp.float32)
    base = jnp.where(late, peers - 1 - rank, rank)

    def iota(rows, columns, dim):
        return lax.broadcasted_iota(jnp.int32, (rows, columns), dim)

    lane = iota(grid // 16, 2 * grid, 1)
    sine = ((lane >> bits) & 1) == 1
    wave = ((lane >> (bits + 1)) ^ rank) * width + (lane & (width - 1))
    wave = jnp.where(sine & (wave == 0), grid, wave)
    sixteens = 32 * iota(grid // 16, 2 * grid, 0)
    ones = 2 * iota(16, 2 * grid, 0) - (grid - 1)
    fill_table(grid, sixteens * wave, ones * wave[:16], sine, 1.0, row_ref)

    half = grid // 2
    spot = iota(grid // 16, half, 1)
    place = 2 * (((spot >> bits) ^ base) * width + (spot & (width - 1))) - (grid - 1)
    sixteens = 16 * iota(grid // 16, half, 0) * place
    ones = iota(16, half, 0) * place[:16]
    edge = sign * turn_parts(grid, grid * place[:16])[1]
    fill_table(grid, sixteens, ones, False, 1.0, cos_ref)
    fill_table(grid, sixteens, ones, True, sign, sin_ref, top=edge)

    count = back_cos_ref.shape[1] // 16
    for out_ref, is_sine in ((back_cos_ref, False), (back_sin_ref, True)):
        number = iota(count, grid, 1)
        if is_sine:
            number = jnp.where(number == 0, grid, number)
        span = 32 * iota(count, grid, 0) * number
        start = (2 * (iota(16, grid, 0) - halo) - (grid - 1)) * number[:16]
        fill_table(grid, span, start, is_sine, sign if is_sine else 1.0, out_ref)

    def parts(row_number, column_number, weight):
        row_wave = (2.0 * math.pi / (2 * grid)) * signed(row_number)
        column_wave = (2.0 * math.pi / (2 * grid)) * signed(column_number)
        squared = row_wave * row_wave + column_wave * column_wave
        nonzero = squared > 0.0
        safe = jnp.where(nonzero, squared, 1.0)
        scaled = jnp.sqrt(safe) * thickness
        film = jnp.where(nonzero, (1.0 - jnp.exp(-scaled)) / scaled, 1.0)
        in_plane = (1.0 - film) / safe * weight
        edge = (row_number == grid) | (column_number == grid)
        return (
            in_plane * column_wave * column_wave,
            in_plane * row_wave * row_wave,
            film * weight,
            jnp.where(edge, 0.0, in_plane * column_wave * row_wave),
        )

    def signed(number):
        return jnp.where(number < grid, number, number - 2 * grid).astype(jnp.float32)

    columns = 2 * width
    for block in range(grid // 64):
        spots = slice(64 * block, 64 * block + 64)
        row_number = iota(64, columns, 0) + 64 * block
        lane = iota(64, columns, 1)
        is_sine = lane >= width
        column_number = rank * width + (lane & (width - 1))
        column_number = jnp.where(is_sine & (column_number == 0), grid, column_number)
        column_weight = jnp.where((column_number & (grid - 1)) == 0, 1.0, 2.0)
        weight = column_weight * jnp.where(row_number == 0, 1.0, 2.0) * (-0.25 / (grid * grid))
        found = parts(row_number, column_number, weight)
        for c in range(3):
            tensor_ref[c, spots] = found[c]
        tensor_ref[6, spots] = jnp.where(is_sine, -found[3], found[3])
        if block == 0:
            other = parts(jnp.where(row_number == 0, grid, row_number), column_number, weight)
            found = [jnp.where(row_number == 0, a, b) for a, b in zip(other, found)]
        for c in range(3):
            tensor_ref[3 + c, spots] = found[c]


def split(values):
    high = values.astype(jnp.bfloat16)
    low = (values - high.astype(jnp.float32)).astype(jnp.bfloat16)
    return (high, low)


def multiply_rows(left, table, transposed=False):
    numbers = (((1,), (1 if transposed else 0,)), ((), ()))

    def one(a, b):
        return lax.dot_general(a, b, numbers, preferred_element_type=jnp.float32)

    rows = left[0].shape[0]
    both = one(jnp.concatenate(left, axis=0), table[0])
    return both[:rows] + (both[rows:] + one(left[0], table[1]))


def multiply(table, right):
    columns = right[0].shape[1]
    both = jnp.dot(table[0], jnp.concatenate(right, axis=1), preferred_element_type=jnp.float32)
    rest = jnp.dot(table[1], right[0], preferred_element_type=jnp.float32)
    return both[:, :columns] + (both[:, columns:] + rest)


def exchange_weights(coupling):
    rows, columns = coupling.shape
    place = lax.broadcasted_iota(jnp.int32, coupling.shape, 1)
    own = stiffness * coupling
    right = jnp.where(place < columns - 1, pltpu.roll(coupling, columns - 1, 1), 0.0)
    left = jnp.where(place > 0, pltpu.roll(coupling, 1, 1), 0.0)
    below = pltpu.roll(coupling, rows - 1, 0)
    above = pltpu.roll(coupling, 1, 0)
    return (own * right, own * left, own * below, own * above)


def exchange_of(part, weights):
    rows, columns = part.shape
    right, left, below, above = weights
    total = right * (pltpu.roll(part, columns - 1, 1) - part)
    total = total + left * (pltpu.roll(part, 1, 1) - part)
    total = total + below * (pltpu.roll(part, rows - 1, 0) - part)
    return total + above * (pltpu.roll(part, 1, 0) - part)


def cross(a, b):
    return (a[1] * b[2] - a[2] * b[1], a[2] * b[0] - a[0] * b[2], a[0] * b[1] - a[1] * b[0])


def torque_of(magnet, effective):
    first = cross(magnet, effective)
    second = cross(magnet, first)
    scale = -1.0 / (1.0 + damping * damping)
    return [scale * (a + damping * b) for a, b in zip(first, second)]


def coarse_step(magnet, applied, weights):
    effective = [exchange_of(part, weights) + field for part, field in zip(magnet, applied)]
    effective[2] = effective[2] - magnet[2]
    return [part + FINE * step_time * rate for part, rate in zip(magnet, torque_of(magnet, effective))]


def vmem_call(body, outs, name, scalars=0, scratch=(), cost=10**8):
    whole = pl.BlockSpec(memory_space=pltpu.VMEM)

    def call(*args):
        first = [pl.BlockSpec(memory_space=pltpu.SMEM)] * scalars
        return pl.pallas_call(
            body,
            out_shape=[
                out if isinstance(out, jax.ShapeDtypeStruct) else jax.ShapeDtypeStruct(out, jnp.float32)
                for out in outs
            ],
            in_specs=first + [whole] * (len(args) - scalars),
            out_specs=[whole] * len(outs),
            scratch_shapes=[pltpu.VMEM(shape, jnp.float32) for shape in scratch],
            compiler_params=pltpu.CompilerParams(vmem_limit_bytes=VMEM_LIMIT),
            cost_estimate=pl.CostEstimate(flops=cost, bytes_accessed=10**6, transcendentals=0),
            name=name,
        )(*args)

    return call


def pack_body(reach, state_ref, applied_ref, coupling_ref, own_ref, top_ref, bottom_ref):
    rows = coupling_ref.shape[0]
    for c in range(3):
        own_ref[c] = state_ref[c]
        own_ref[3 + c] = applied_ref[c]
    own_ref[6] = coupling_ref[...]
    for ref, first in ((top_ref, 0), (bottom_ref, rows - reach)):
        for c in range(7):
            ref[c * reach : (c + 1) * reach] = own_ref[c, first : first + reach]
        if 7 * reach < ref.shape[0]:
            ref[7 * reach :] = jnp.zeros_like(ref[7 * reach :])


def pieces(values):
    high = values.astype(jnp.bfloat16)
    rest = values - high.astype(jnp.float32)
    middle = rest.astype(jnp.bfloat16)
    low = (rest - middle.astype(jnp.float32)).astype(jnp.bfloat16)
    return (high, middle, low)


def choose(selection, parts):
    first, second, third = (
        jnp.dot(selection, part, preferred_element_type=jnp.float32) for part in parts
    )
    return first + (second + third)


def build_wide(flipped, reach, state_ref, applied_ref, coupling_ref, before, after, wide_ref):
    rows = coupling_ref.shape[0]
    count = before.shape[0]
    total = wide_ref.shape[1]
    margin = (total - rows) // 2

    def matrix(fields, columns, base):
        row = lax.broadcasted_iota(jnp.int32, (fields * total, columns), 0)
        column = lax.broadcasted_iota(jnp.int32, (fields * total, columns), 1)
        field, row = (row // total, row % total)
        row = jnp.where(flipped == 1, total - 1 - row, row) - base
        size = reach if fields > 1 else columns
        inside = (row >= 0) & (row < size) & (column == field * size + row)
        return jnp.where(inside, 1.0, 0.0).astype(jnp.bfloat16)

    own = matrix(1, rows, margin)
    edges = choose(matrix(7, count, margin - reach), pieces(before))
    edges = edges + choose(matrix(7, count, margin + rows), pieces(after))
    fields = [state_ref[c] for c in range(3)] + [applied_ref[c] for c in range(3)]
    fields.append(coupling_ref[...])
    for number, field in enumerate(fields):
        wide_ref[number] = choose(own, pieces(field)) + edges[number * total : (number + 1) * total]


def sweep_body(reach, trim, flip_ref, fine_flip_ref, turn_ref, own_ref, *refs):
    edge_refs, (ends_ref, strip_ref, wide_ref) = (refs[:4], refs[4:])
    kept = flip_ref[0] == fine_flip_ref[0]
    before, after = (
        jnp.where(kept, edge_refs[i][...], edge_refs[2 + i][...]) for i in range(2)
    )
    fields = (own_ref.at[0:3], own_ref.at[3:6], own_ref.at[6])
    build_wide(flip_ref[0], reach, *fields, before, after, wide_ref)
    slices, _, rows, _ = ends_ref.shape
    share = rows - 2 * trim
    margin = (wide_ref.shape[1] - slices * share) // 2
    start = pl.multiple_of(turn_ref[0] * share + margin - 8, 8)

    def strip(number):
        return wide_ref[number, pl.ds(start, share + 16)][8 - trim : 8 + share + trim]

    applied = [strip(3 + c) for c in range(3)]
    weights = exchange_weights(strip(6))
    for number, values in enumerate(applied + list(weights)):
        strip_ref[number] = values
    first = [strip(c) for c in range(3)]
    for number in range(slices):
        first = coarse_step(first, applied, weights)
        for c in range(3):
            ends_ref[number, c] = first[c]


def start_body(reach, slices, turn_ref, flip_ref, rank_ref, *refs):
    table_ref, refs = (refs[5], refs[:5] + refs[6:])
    send_refs, (first_ref, around_ref, wide_ref) = (refs[5:-3], refs[-3:])
    turn = turn_ref[0]
    build_wide(flip_ref[0], reach, *refs[:3], refs[3][...], refs[4][...], wide_ref)
    rows = first_ref.shape[1]
    margin = (wide_ref.shape[1] - rows) // 2
    kept = slice(margin, margin + rows)
    weights = exchange_weights(wide_ref[6])
    applied = [wide_ref[3 + c] for c in range(3)]
    for number, values in enumerate(applied + list(weights)):
        around_ref[number] = values[kept]
    for c in range(3):
        first_ref[c] = wide_ref[c, kept]
    for number in range(1, slices):
        @pl.when(turn >= number)
        def step():
            magnet = coarse_step([wide_ref[c] for c in range(3)], applied, weights)
            for c in range(3):
                wide_ref[c] = magnet[c]
                first_ref[c] = magnet[c][kept]
    send_rows([first_ref[c] for c in range(3)], rank_ref[0], (table_ref[0], table_ref[1]), send_refs)


def first_is_end(rank):
    return (rank & 1) == jnp.where(rank >= 4, 1, 0)


def send_rows(magnet, rank, table, out_refs):
    rows, grid = magnet[0].shape
    width = out_refs[0].shape[1]
    block = split(jnp.concatenate(magnet, axis=0))
    spectrum = multiply_rows(block, table)
    at_end = first_is_end(rank)
    for slot, out_ref in enumerate(out_refs):
        out_ref[: 3 * rows] = spectrum[:, slot * width : (slot + 1) * width]
        if out_ref.shape[0] > 3 * rows:
            which = at_end if slot == 1 else jnp.logical_not(at_end)
            place = 3 * rows
            for part in magnet:
                edge = jnp.where(which, part[rows - 1 :], part[:1])
                for start in range(0, grid, width):
                    out_ref[place : place + 1] = edge[:, start : start + width]
                    place += 1
            rest = out_ref.shape[0] - place
            out_ref[place:] = jnp.zeros((rest, width), jnp.float32)


def edge_rows(rank, near_ref, far_ref, middle_ref, rows):
    width = near_ref.shape[1]
    count = rows * 3
    at_end = first_is_end(rank)
    outer = (rank == 0) | (rank == 7)
    central = (rank == 3) | (rank == 4)
    grid = 4 * width
    pairs = []
    for c in range(3):
        near, far, middle = (
            jnp.concatenate(
                [
                    ref[count + c * (grid // width) + j : count + c * (grid // width) + j + 1]
                    for j in range(grid // width)
                ],
                axis=1,
            )
            for ref in (near_ref, far_ref, middle_ref)
        )
        other = jnp.where(central, middle, far)
        start = jnp.where(at_end, jnp.where(outer, jnp.zeros_like(far), far), near)
        pairs.append((start, jnp.where(at_end, near, other)))
    return pairs


def spectrum_body(peers, rows, base_ref, *refs):
    in_refs, refs = (refs[:peers], refs[peers:])
    tensor_ref, cos_ref, sin_ref, back_cos_ref, back_sin_ref = refs[:5]
    out_refs = refs[5 : 5 + peers]
    front_ref, back_ref = refs[5 + peers :]
    width = in_refs[0].shape[1]
    half = peers // 2

    def part(slot, c):
        return in_refs[slot][c * rows : (c + 1) * rows]

    def fold(sign):
        return jnp.concatenate(
            [
                jnp.concatenate(
                    [part(p, c) + sign * part(peers - 1 - p, c) for p in range(half)], axis=0
                )
                for c in range(3)
            ],
            axis=1,
        )

    even = multiply((cos_ref[0], cos_ref[1]), split(fold(1.0)))
    odd = multiply((sin_ref[0], sin_ref[1]), split(fold(-1.0)))
    even_x, even_y, even_z = (even[:, c * width : (c + 1) * width] for c in range(3))
    odd_x, odd_y, odd_z = (odd[:, c * width : (c + 1) * width] for c in range(3))
    mixed = tensor_ref[6]

    def turned(values):
        return mixed * pltpu.roll(values, width // 2, 1)

    even_out = jnp.concatenate(
        [
            tensor_ref[0] * even_x - turned(odd_y),
            tensor_ref[1] * even_y - turned(odd_x),
            tensor_ref[2] * even_z,
        ],
        axis=1,
    )
    odd_out = jnp.concatenate(
        [
            tensor_ref[3] * odd_x + turned(even_y),
            tensor_ref[4] * odd_y + turned(even_x),
            tensor_ref[5] * odd_z,
        ],
        axis=1,
    )
    even_rows = multiply((back_cos_ref[0], back_cos_ref[1]), split(even_out))
    odd_rows = multiply((back_sin_ref[0], back_sin_ref[1]), split(odd_out))
    front_ref[...] = even_rows + odd_rows
    back_ref[...] = even_rows - odd_rows
    base = base_ref[0]
    for p in range(half):
        span = pl.ds(pl.multiple_of((base ^ p) * rows, 8), rows)
        for c in range(3):
            kept = slice(c * rows, (c + 1) * rows)
            out_refs[p][kept] = front_ref[span, c * width : (c + 1) * width]
            out_refs[peers - 1 - p][kept] = back_ref[span, c * width : (c + 1) * width]


def exchange_inside(part, weights, start, end):
    rows, columns = part.shape
    right, left, below, above = weights
    row = lax.broadcasted_iota(jnp.int32, part.shape, 0)
    following = jnp.where(row == rows - 1, end, pltpu.roll(part, rows - 1, 0))
    preceding = jnp.where(row == 0, start, pltpu.roll(part, 1, 0))
    total = right * (pltpu.roll(part, columns - 1, 1) - part)
    total = total + left * (pltpu.roll(part, 1, 1) - part)
    total = total + below * (following - part)
    return total + above * (preceding - part)


def field_rates(rank, in_refs, edge_refs, magnet, around_ref, table):
    rows = magnet[0].shape[0]
    spectrum = jnp.concatenate([ref[...] for ref in in_refs], axis=1)
    demag = multiply_rows(split(spectrum), table, transposed=True)
    edges = edge_rows(rank, *edge_refs, rows)
    weights = [around_ref[3 + c] for c in range(4)]
    effective = [
        exchange_inside(magnet[c], weights, *edges[c])
        + demag[c * rows : (c + 1) * rows]
        + around_ref[c]
        for c in range(3)
    ]
    return torque_of(magnet, effective)


def predict_body(peers, rank_ref, *refs):
    in_refs, edge_refs, refs = (refs[:peers], refs[peers : peers + 3], refs[peers + 3 :])
    state_ref, around_ref, table_ref = refs[:3]
    send_refs, (predicted_ref, base_ref) = (refs[3 : 3 + peers], refs[3 + peers :])
    rank = rank_ref[0]
    table = (table_ref[0], table_ref[1])
    magnet = [state_ref[c] for c in range(3)]
    rates = field_rates(rank, in_refs, edge_refs, magnet, around_ref, table)
    predicted = [part + step_time * rate for part, rate in zip(magnet, rates)]
    send_rows(predicted, rank, table, send_refs)
    for c in range(3):
        predicted_ref[c] = predicted[c]
        base_ref[c] = magnet[c] + 0.5 * step_time * rates[c]


def correct_body(peers, rank_ref, *refs):
    in_refs, edge_refs, refs = (refs[:peers], refs[peers : peers + 3], refs[peers + 3 :])
    state_ref, base_ref, around_ref, table_ref = refs[:4]
    send_refs, following_ref = (refs[4 : 4 + peers], refs[4 + peers])
    rank = rank_ref[0]
    table = (table_ref[0], table_ref[1])
    magnet = [state_ref[c] for c in range(3)]
    rates = field_rates(rank, in_refs, edge_refs, magnet, around_ref, table)
    following = [base_ref[c] + 0.5 * step_time * rates[c] for c in range(3)]
    send_rows(following, rank, table, send_refs)
    for c in range(3):
        following_ref[c] = following[c]


def end_body(peers, share, trim, slices, rank_ref, number_ref, *refs):
    in_refs, edge_refs, refs = (refs[:peers], refs[peers : peers + 3], refs[peers + 3 :])
    state_ref, base_ref, around_ref, table_ref = refs[:4]
    strip_refs, margin_refs, end_ref = (refs[4 : 4 + slices], refs[4 + slices : -1], refs[-1])
    rank, number = (rank_ref[0], number_ref[0])
    magnet = [state_ref[c] for c in range(3)]
    rows = magnet[0].shape[0]
    table = (table_ref[0], table_ref[1])
    rates = field_rates(rank, in_refs, edge_refs, magnet, around_ref, table)
    blank = jnp.zeros((trim, magnet[0].shape[1]), jnp.float32)
    for c in range(3):
        end_ref[c, :trim] = blank
        end_ref[c, trim + rows :] = blank
        end_ref[c, trim : trim + rows] = base_ref[c] + 0.5 * step_time * rates[c]
    central = (rank == 3) | (rank == 4)
    for t in range(slices):
        start = pl.multiple_of((number ^ t) * share, 8)
        ending = number == t
        for c in range(3):
            strip_refs[t][c] = end_ref[c, pl.ds(start, strip_refs[t].shape[1])]
            for i in range(trim):
                head = end_ref[c, trim + i : trim + i + 1]
                tail = end_ref[c, rows + i : rows + i + 1]
                mirrored = end_ref[c, trim + rows - 1 - i : trim + rows - i]
                tail = jnp.where(central, mirrored, tail)
                margin_refs[t][c * trim + i : c * trim + i + 1] = jnp.where(ending, tail, head)
        margin_refs[t][3 * trim :] = jnp.zeros_like(margin_refs[t][3 * trim :])


def finish_body(slices, trim, turn_ref, block_ref, *refs):
    in_refs, margin_refs, refs = (refs[:slices], refs[slices : 2 * slices], refs[2 * slices :])
    coarse_ref, strip_ref, out_refs = (refs[0], refs[1], refs[2 : slices + 2])
    fine_ref, edge_ref, end_ref = refs[slices + 2 :]
    turn, block = (turn_ref[0], block_ref[0])
    rows = fine_ref.shape[2]
    share = rows - 2 * trim
    central = (block == 3) | (block == 4)
    straight = (turn == 0) | central
    for t in range(slices):
        fine_ref[turn ^ t] = in_refs[t][...]
        edge_ref[jnp.where(straight, t, t ^ 3)] = margin_refs[t][...]
    row = lax.broadcasted_iota(jnp.int32, (rows, fine_ref.shape[3]), 0)
    patched = ((turn == 0) & (row < trim)) | ((turn == slices - 1) & (row >= rows - trim))
    blank = jnp.zeros((share, fine_ref.shape[3]), jnp.float32)

    def fine(number, c):
        edge = edge_ref[number, c * trim : (c + 1) * trim]
        return jnp.where(patched, jnp.concatenate([edge, blank, edge], axis=0), fine_ref[number, c])

    applied = [strip_ref[c] for c in range(3)]
    weights = [strip_ref[3 + c] for c in range(4)]
    magnet = []
    for number in range(slices):
        first = [coarse_ref[number, c] for c in range(3)]
        ahead = coarse_step(magnet, applied, weights) if number > 0 else first
        magnet = [ahead[c] + (fine(number, c) - first[c]) for c in range(3)]
        for c in range(3):
            end_ref[number, c] = magnet[c][trim : trim + share]
    for t in range(slices):
        out_refs[t][...] = end_ref[turn ^ t]


def gather_body(slices, turn_ref, flip_ref, *refs):
    in_refs, out_ref = (refs[:slices], refs[slices])
    turn, flipped = (turn_ref[0], flip_ref[0])
    share = in_refs[0].shape[1]
    row = lax.broadcasted_iota(jnp.int32, (share, share), 0)
    column = lax.broadcasted_iota(jnp.int32, (share, share), 1)
    row = jnp.where(flipped == 1, share - 1 - row, row)
    matrix = jnp.where(row == column, 1.0, 0.0).astype(jnp.bfloat16)
    for t in range(slices):
        strip = turn ^ t
        strip = jnp.where(flipped == 1, slices - 1 - strip, strip)
        span = pl.ds(pl.multiple_of(strip * share, 8), share)
        for c in range(3):
            out_ref[c, span] = choose(matrix, pieces(in_refs[t][c]))


def shards_by_block(initial_state, applied_field, coupling):
    rows, _, grid = initial_state.shape
    group = ("core", "z_low", "y")
    peers = 8
    slices = 4
    margin, trim, reach = (8, 4, 4)
    width = grid // peers
    space = ("z_high", "z_low", "y")
    blocks = 8
    def scalar(value):
        return value.astype(jnp.int32).reshape(1)

    rank = lax.axis_index(group)
    half = lax.axis_index("z_high")
    turn = lax.axis_index(("x", "core"))
    number = 2 * lax.axis_index("x") + half
    base = jnp.where(rank < peers // 2, rank, peers - 1 - rank)
    scalars = (rank, half, lax.axis_index("core"), turn, number, base, lax.axis_index(space))
    rank, native_flip, fine_flip, turn, number, base, block = lax.optimization_barrier(
        tuple(value.astype(jnp.int32).reshape(1) for value in scalars)
    )

    state_in = jnp.transpose(initial_state, (1, 0, 2))
    applied_in = jnp.transpose(applied_field, (1, 0, 2))
    edge_shape = (-(-7 * reach // 8) * 8, grid)
    native, top, bottom = vmem_call(
        functools.partial(pack_body, reach), [(7, rows, grid), edge_shape, edge_shape], "pack"
    )(state_in, applied_in, coupling)

    def trade(values):
        return lax.ppermute(values, ("core", "z_high"), [(0, 0), (1, 2), (2, 1), (3, 3)])

    def edge_route(step):
        route = []
        for core in range(2):
            for block in range(blocks):
                following = block + step
                if 0 <= following < blocks:
                    target = (following // 4, core, following % 4)
                    route.append((8 * core + block, 8 * target[0] + 4 * target[1] + target[2]))
        return route

    everywhere = ("core",) + space
    before = lax.ppermute(bottom, everywhere, edge_route(1))
    after = lax.ppermute(top, everywhere, edge_route(-1))
    own = (trade(state_in), trade(applied_in), trade(coupling))

    def pair(*shape):
        return jax.ShapeDtypeStruct((2,) + shape, jnp.bfloat16)

    back_rows = grid // 2
    row_table, *column_tables, tensor = vmem_call(
        functools.partial(tables_body, peers, 0),
        [pair(grid, 2 * grid)]
        + [pair(grid, grid // 2)] * 2
        + [pair(back_rows, grid)] * 2
        + [(7, grid, 2 * width)],
        "tables",
        scalars=1,
    )(rank)

    state_shape = (3, rows, grid)
    wide_shape = (7, rows + 2 * margin, grid)
    lanes = 2 * width
    extra = -(-3 * grid // lanes // 8) * 8
    near, far, middle = (1, 3, 7)
    send_shapes = [
        (3 * rows + (extra if slot in (near, far, middle) else 0), lanes) for slot in range(peers)
    ]
    *sent, state, around = vmem_call(
        functools.partial(start_body, reach, slices),
        send_shapes + [state_shape, (7, rows, grid)],
        "start",
        scalars=3,
        scratch=[wide_shape],
    )(number, fine_flip, rank, *own, before, after, row_table)

    def spread(slots):
        return [slots[0]] + [
            lax.ppermute(slots[k], group, [(i, i ^ k) for i in range(peers)])
            for k in range(1, peers)
        ]

    def demag_blocks(received):
        return received, vmem_call(
            functools.partial(spectrum_body, peers, rows),
            [(3 * rows, lanes)] * peers,
            "spectrum",
            scalars=1,
            scratch=[(back_rows, 3 * lanes)] * 2,
            cost=10**9,
        )(base, *received, tensor, *column_tables)

    def complete(received, blocks_back):
        return spread(blocks_back) + [received[slot] for slot in (near, far, middle)]

    share = rows // slices
    strip_shape = (3, share + 2 * trim, grid)
    swap = [(0, 1), (1, 0)]
    coarse_ends, strip = vmem_call(
        functools.partial(sweep_body, reach, trim),
        [(slices,) + strip_shape, (7,) + strip_shape[1:]],
        "sweep",
        scalars=3,
        scratch=[wide_shape],
    )(
        native_flip,
        fine_flip,
        turn,
        native,
        before,
        after,
        lax.ppermute(before, "core", swap),
        lax.ppermute(after, "core", swap),
    )
    for repeat in range(FINE):
        received = spread(sent)
        received = complete(*demag_blocks(received))
        if repeat == 0:
            received[4], coarse_ends = lax.optimization_barrier((received[4], coarse_ends))
        *sent, predicted, start = vmem_call(
            functools.partial(predict_body, peers), send_shapes + [state_shape] * 2, "predict", scalars=1, cost=10**9
        )(rank, *received, state, around, row_table)
        received = complete(*demag_blocks(spread(sent)))
        if repeat < FINE - 1:
            *sent, state = vmem_call(
                functools.partial(correct_body, peers), send_shapes + [state_shape], "correct", scalars=1, cost=10**9
            )(rank, *received, predicted, start, around, row_table)
    swap = [(0, 1), (1, 0)]
    margin_shape = (-(-3 * trim // 8) * 8, grid)
    ending = vmem_call(
        functools.partial(end_body, peers, share, trim, slices),
        [strip_shape] * slices + [margin_shape] * slices,
        "end",
        scalars=2,
        scratch=[(3, rows + 2 * trim, grid)],
    )(rank, number, *received, predicted, start, around, row_table)
    strips, margins = (ending[:slices], ending[slices:])

    def margin_route(t):
        route = []
        for s in range(blocks):
            if s in (3, 4):
                beyond = (7 - s, slices - 1)
            else:
                beyond = (s + 1 if s < 4 else s - 1, 0)
            ahead = s - 1 if s < 4 else s + 1
            for n, (block_to, strip) in ((t, beyond), (t ^ 3, (ahead, slices - 1))):
                if 0 <= block_to < blocks:
                    source = 16 * (n // 2) + 8 * (s // 4) + 4 * (n % 2) + s % 4
                    route.append((source, 8 * strip + block_to))
        return route

    def strip_route(t):
        route = []
        for i in range(8):
            x, core, z = (i // 4, i // 2 % 2, i % 2)
            route.append((i, 4 * (x ^ (t // 2)) + 2 * (z ^ (t % 2)) + core))
        return route

    strips = [
        lax.ppermute(strips[t], ("x", "core", "z_high"), strip_route(t)) for t in range(slices)
    ]
    margins = [
        lax.ppermute(margins[t], ("x",) + everywhere, margin_route(t)) for t in range(slices)
    ]
    ends = vmem_call(
        functools.partial(finish_body, slices, trim),
        [(3, share, grid)] * slices,
        "finish",
        scalars=2,
        scratch=[
            (slices,) + strip_shape,
            (slices,) + margin_shape,
            (slices, 3, share, grid),
        ],
    )(turn, block, *strips, *margins, coarse_ends, strip)
    ends = [ends[0]] + [
        lax.ppermute(ends[t], ("x", "core"), [(i, i ^ t) for i in range(slices)])
        for t in range(1, slices)
    ]
    (result,) = vmem_call(
        functools.partial(gather_body, slices), [(3, rows, grid)], "gather", scalars=2
    )(turn, native_flip, *ends)
    return jnp.transpose(result, (1, 0, 2))[None]


def fits_blocks(mesh):
    return mesh.shape["tm"] == 4 and mesh.shape["space"] == 8


def solution(mesh):
    if not fits_blocks(mesh):
        in_specs = (P("space", None, None), P("space", None, None), P("space", None))
        out_specs = P("tm", "space", None, None)
        return jax.shard_map(
            shards, mesh=mesh, in_specs=in_specs, out_specs=out_specs, check_vma=False
        )
    fine_mesh = Mesh(
        mesh.devices.reshape(2, 2, 2, 2, 2), ("x", "core", "z_high", "z_low", "y")
    )
    space = ("z_high", "z_low", "y")
    in_specs = (P(space, None, None), P(space, None, None), P(space, None))
    out_specs = P(("x", "core"), space, None, None)
    return jax.shard_map(
        shards_by_block, mesh=fine_mesh, in_specs=in_specs, out_specs=out_specs, check_vma=False
    )
```

```python
import functools
import math

import jax
import jax.numpy as jnp
from jax import lax
from jax.experimental import pallas as pl
from jax.experimental.pallas import tpu as pltpu
from jax.sharding import Mesh
from jax.sharding import PartitionSpec as P

FINE = 2
VMEM_LIMIT = 16 * 1024 * 1024


step_time = 0.06
damping = 0.02
stiffness = 0.25
thickness = 8.0


def with_halo(x, sides, width):
    for axis, dim in sides:
        peers, length = (lax.axis_size(axis), x.shape[dim])
        up = [(i, (i + 1) % peers) for i in range(peers - 1)]
        down = [(j, i) for i, j in up]
        last = lax.slice_in_dim(x, length - width, length, axis=dim)
        initial = lax.slice_in_dim(x, 0, width, axis=dim)
        before = lax.ppermute(last, axis, up)
        after = lax.ppermute(initial, axis, down)
        x = jnp.concatenate([before, x, after], axis=dim)
    return x


def passed_along(block, axis, distance):
    devices = range(lax.axis_size(axis))
    route = [(i - distance, i) for i in devices if i - distance in devices]
    return lax.ppermute(block, axis, route)


def spectral_tensor(row_index, column_index, length):
    half_length = length // 2
    signed_rows = jnp.where(row_index < half_length, row_index, row_index - length).astype(
        jnp.float32
    )
    signed_columns = jnp.where(
        column_index < half_length, column_index, column_index - length
    ).astype(jnp.float32)
    wave_rows = 2.0 * math.pi / length * signed_rows[:, None]
    wave_columns = 2.0 * math.pi / length * signed_columns[None, :]
    squared = wave_rows * wave_rows + wave_columns * wave_columns
    nonzero = squared > 0.0
    safe_square = jnp.where(nonzero, squared, 1.0)
    scaled_wave = jnp.sqrt(safe_square) * thickness
    film_factor = jnp.where(nonzero, (1.0 - jnp.exp(-scaled_wave)) / scaled_wave, 1.0)
    in_plane = (1.0 - film_factor) / safe_square
    nyquist = (row_index[:, None] == half_length) | (column_index[None, :] == half_length)
    normalizer = -1.0 / (length * length)
    tensor_first = in_plane * wave_columns * wave_columns * normalizer
    tensor_second = in_plane * wave_rows * wave_rows * normalizer
    tensor_cross = jnp.where(nyquist, 0.0, in_plane * wave_columns * wave_rows) * normalizer
    tensor_normal = film_factor * normalizer
    return (tensor_first, tensor_second, tensor_cross, tensor_normal)


def exchange_field(padded_state, padded_coupling):
    center_state = padded_state[1:-1]
    center_coupling = padded_coupling[1:-1]
    wide_state = jnp.pad(padded_state, ((0, 0), (0, 0), (1, 1)))
    wide_coupling = jnp.pad(padded_coupling, ((0, 0), (1, 1)))
    neighbour_sum = padded_coupling[2:, None, :] * (padded_state[2:] - center_state)
    neighbour_sum = neighbour_sum + padded_coupling[:-2, None, :] * (
        padded_state[:-2] - center_state
    )
    neighbour_sum = neighbour_sum + wide_coupling[1:-1, None, 2:] * (
        wide_state[1:-1, :, 2:] - center_state
    )
    neighbour_sum = neighbour_sum + wide_coupling[1:-1, None, :-2] * (
        wide_state[1:-1, :, :-2] - center_state
    )
    return stiffness * center_coupling[:, None, :] * neighbour_sum


def torque(magnet, effective):
    first_cross = jnp.cross(magnet, effective, axis=1)
    second_cross = jnp.cross(magnet, first_cross, axis=1)
    return -(first_cross + damping * second_cross) / (1.0 + damping * damping)


def phase_table(row_count, column_count, period, direction):
    row_ids = lax.broadcasted_iota(jnp.int32, (row_count, column_count), 0)
    column_ids = lax.broadcasted_iota(jnp.int32, (row_count, column_count), 1)
    angles = (row_ids * column_ids % period).astype(jnp.float32) * (2.0 * math.pi / period)
    return (jnp.cos(angles), direction * jnp.sin(angles))


def joined_table(row_count, column_count, period, direction):
    table_cos, table_sin = phase_table(row_count, column_count, period, direction)
    return jnp.concatenate([table_cos, table_sin], axis=1)


def contract(pattern, left, right):
    return jnp.einsum(pattern, left, right, precision=lax.Precision.HIGHEST)


def complex_apply(pattern, real_part, imag_part, joined):
    half_width = joined.shape[-1] // 2
    real_both = contract(pattern, real_part, joined)
    imag_both = contract(pattern, imag_part, joined)
    return (
        real_both[..., :half_width] - imag_both[..., half_width:],
        real_both[..., half_width:] + imag_both[..., :half_width],
    )


def apply_tensor(real_part, imag_part, tensor):
    tensor_first, tensor_second, tensor_cross, tensor_normal = tensor

    def mix_components(values):
        return jnp.stack(
            [
                tensor_first * values[0] + tensor_cross * values[1],
                tensor_cross * values[0] + tensor_second * values[1],
                tensor_normal * values[2],
            ],
            axis=0,
        )

    return (mix_components(real_part), mix_components(imag_part))


def shards(initial_state, applied_field, coupling):
    row_count, component_count, grid_size = initial_state.shape
    length = 2 * grid_size
    space_count = lax.axis_size("space")
    space_index = lax.axis_index("space")
    slice_count = lax.axis_size("tm")
    slice_index = lax.axis_index("tm")
    is_first = slice_index == 0
    padded_coupling = with_halo(coupling, (("space", 0),), 1)
    index_all = jnp.arange(length, dtype=jnp.int32)
    local_demag = jnp.array([0.0, 0.0, -1.0], dtype=jnp.float32).reshape(1, 3, 1)
    forward_y = joined_table(grid_size, length, length, -1.0)
    inverse_y = joined_table(length, grid_size, length, 1.0)

    def transform_columns(real_part, imag_part):
        return complex_apply("yca,yk->cak", real_part, imag_part, forward_y)

    column_width = grid_size // space_count
    columns = space_index * column_width + jnp.arange(column_width, dtype=jnp.int32)
    tensor = tuple((part_table.T for part_table in spectral_tensor(index_all, columns, length)))
    edge_first, edge_second, edge_cross, edge_normal = spectral_tensor(
        index_all, jnp.array([0, grid_size], dtype=jnp.int32), length
    )
    anchor_diag = jnp.stack([edge_first[:, 0], edge_second[:, 0], edge_normal[:, 0]], axis=0)
    nyquist_diag = jnp.stack([edge_first[:, 1], edge_second[:, 1], edge_normal[:, 1]], axis=0)
    mean_diag = 0.5 * (anchor_diag + nyquist_diag)
    half_gap = 0.5 * (anchor_diag - nyquist_diag)
    is_anchor = (columns == 0)[None, :, None]
    column_ids = jnp.arange(grid_size, dtype=jnp.int32)
    is_lead = column_ids == 0
    lead_columns = is_lead[None, :, None]
    alternating = jnp.where(column_ids % 2 == 0, 1.0, -1.0).astype(jnp.float32)
    forward_x = joined_table(grid_size, grid_size, length, -1.0)
    inverse_x_cos, inverse_x_sin = phase_table(grid_size, grid_size, length, 1.0)

    def demag_field(magnet):
        both_parts = contract("rcx,xk->rck", magnet, forward_x)
        packed_real = both_parts[..., :grid_size]
        imag_part = both_parts[..., grid_size:]
        nyquist_column = jnp.einsum(
            "rcx,x->rc", magnet, alternating, precision=lax.Precision.HIGHEST
        )
        packed_imag = jnp.where(is_lead, nyquist_column[:, :, None], imag_part)
        real_part, imag_part = (
            lax.all_to_all(packed_real, "space", split_axis=2, concat_axis=0, tiled=True),
            lax.all_to_all(packed_imag, "space", split_axis=2, concat_axis=0, tiled=True),
        )
        real_part, imag_part = transform_columns(real_part, imag_part)
        out_real, out_imag = apply_tensor(real_part, imag_part, tensor)
        lead_real = real_part[:, 0, :]
        lead_imag = imag_part[:, 0, :]
        mirror_real = jnp.concatenate([lead_real[:, :1], lead_real[:, 1:][:, ::-1]], axis=1)
        mirror_imag = jnp.concatenate([lead_imag[:, :1], lead_imag[:, 1:][:, ::-1]], axis=1)
        fixed_real = mean_diag * lead_real + half_gap * mirror_real
        fixed_imag = mean_diag * lead_imag - half_gap * mirror_imag
        out_real = jnp.where(is_anchor, fixed_real[:, None, :], out_real)
        out_imag = jnp.where(is_anchor, fixed_imag[:, None, :], out_imag)
        out_real, out_imag = complex_apply("cak,ky->cay", out_real, out_imag, inverse_y)
        out_real, out_imag = (
            lax.all_to_all(out_real, "space", split_axis=2, concat_axis=1, tiled=True),
            lax.all_to_all(out_imag, "space", split_axis=2, concat_axis=1, tiled=True),
        )
        nyquist_part = jnp.transpose(out_imag[:, :1, :], (2, 0, 1))
        doubled_real = jnp.where(lead_columns, out_real, 2.0 * out_real)
        doubled_imag = jnp.where(lead_columns, 0.0, 2.0 * out_imag)
        result = contract("cxr,xo->rco", doubled_real, inverse_x_cos) - contract(
            "cxr,xo->rco", doubled_imag, inverse_x_sin
        )
        return result + nyquist_part * alternating

    def effective_fine(state_now):
        padded_state = with_halo(state_now, (("space", 0),), 1)
        return (
            exchange_field(padded_state, padded_coupling) + demag_field(state_now) + applied_field
        )

    def propagate_coarse(magnet):
        padded_state = with_halo(magnet, (("space", 0),), 1)
        effective = (
            exchange_field(padded_state, padded_coupling) + applied_field + magnet * local_demag
        )
        return magnet + FINE * step_time * torque(magnet, effective)

    def coarse_sweep(jump_term):

        def one_turn(turn_index, loop_state):
            start_state, coarse_end, slice_end = loop_state
            start_state = jnp.where(is_first, initial_state, passed_along(slice_end, "tm", 1))
            coarse_end = propagate_coarse(start_state)
            return (start_state, coarse_end, coarse_end + jump_term)

        coarse_end = propagate_coarse(initial_state)
        return lax.fori_loop(
            0, slice_count - 1, one_turn, (initial_state, coarse_end, coarse_end + jump_term)
        )

    start_state, coarse_end, slice_end = coarse_sweep(jnp.zeros_like(initial_state))
    magnet = start_state
    for repeat in range(FINE):
        first_rate = torque(magnet, effective_fine(magnet))
        predicted = magnet + step_time * first_rate
        second_rate = torque(predicted, effective_fine(predicted))
        magnet = magnet + 0.5 * step_time * (first_rate + second_rate)
    jump_term = magnet - coarse_end
    start_state, coarse_end, slice_end = coarse_sweep(jump_term)
    return slice_end[None]


def turn_parts(grid, product):
    shifted = (product & (4 * grid - 1)) + grid // 2
    quarter = (shifted >> (grid.bit_length() - 1)) & 3
    rest = (shifted & (grid - 1)) - grid // 2
    angle = rest.astype(jnp.float32) * (math.pi / (2 * grid))
    square = angle * angle
    sine = -1.0 / 39916800.0
    for term in (1.0 / 362880.0, -1.0 / 5040.0, 1.0 / 120.0, -1.0 / 6.0, 1.0):
        sine = sine * square + term
    sine = sine * angle
    cosine = 1.0 / 479001600.0
    for term in (-1.0 / 3628800.0, 1.0 / 40320.0, -1.0 / 720.0, 1.0 / 24.0, -0.5, 1.0):
        cosine = cosine * square + term
    odd = (quarter & 1) == 1
    first = jnp.where(odd, sine, cosine)
    second = jnp.where(odd, cosine, sine)
    first = jnp.where((quarter == 1) | (quarter == 2), -first, first)
    second = jnp.where(quarter >= 2, -second, second)
    return (first, second)


def fill_table(grid, coarse, fine, sine, sign, out_ref, top=None):
    coarse_cos, coarse_sin = turn_parts(grid, coarse)
    fine_cos, fine_sin = turn_parts(grid, fine)
    lead = sign * jnp.where(sine, coarse_sin, coarse_cos)
    side = sign * jnp.where(sine, coarse_cos, -coarse_sin)
    for block in range(out_ref.shape[1] // 16):
        values = lead[block : block + 1] * fine_cos + side[block : block + 1] * fine_sin
        if top is not None and block == 0:
            first = lax.broadcasted_iota(jnp.int32, values.shape, 0) == 0
            values = jnp.where(first, top, values)
        high, low = split(values)
        out_ref[0, 16 * block : 16 * block + 16] = high
        out_ref[1, 16 * block : 16 * block + 16] = low


def tables_body(
    peers, halo, rank_ref, row_ref, cos_ref, sin_ref, back_cos_ref, back_sin_ref, tensor_ref
):
    rank = rank_ref[0]
    grid = row_ref.shape[1]
    width = grid // peers
    bits = width.bit_length() - 1
    late = rank >= peers // 2
    sign = jnp.where(late, -1.0, 1.0).astype(jnp.float32)
    base = jnp.where(late, peers - 1 - rank, rank)

    def iota(rows, columns, dim):
        return lax.broadcasted_iota(jnp.int32, (rows, columns), dim)

    lane = iota(grid // 16, 2 * grid, 1)
    sine = ((lane >> bits) & 1) == 1
    wave = ((lane >> (bits + 1)) ^ rank) * width + (lane & (width - 1))
    wave = jnp.where(sine & (wave == 0), grid, wave)
    sixteens = 32 * iota(grid // 16, 2 * grid, 0)
    ones = 2 * iota(16, 2 * grid, 0) - (grid - 1)
    fill_table(grid, sixteens * wave, ones * wave[:16], sine, 1.0, row_ref)

    half = grid // 2
    spot = iota(grid // 16, half, 1)
    place = 2 * (((spot >> bits) ^ base) * width + (spot & (width - 1))) - (grid - 1)
    sixteens = 16 * iota(grid // 16, half, 0) * place
    ones = iota(16, half, 0) * place[:16]
    edge = sign * turn_parts(grid, grid * place[:16])[1]
    fill_table(grid, sixteens, ones, False, 1.0, cos_ref)
    fill_table(grid, sixteens, ones, True, sign, sin_ref, top=edge)

    count = back_cos_ref.shape[1] // 16
    for out_ref, is_sine in ((back_cos_ref, False), (back_sin_ref, True)):
        number = iota(count, grid, 1)
        if is_sine:
            number = jnp.where(number == 0, grid, number)
        span = 32 * iota(count, grid, 0) * number
        start = (2 * (iota(16, grid, 0) - halo) - (grid - 1)) * number[:16]
        fill_table(grid, span, start, is_sine, sign if is_sine else 1.0, out_ref)

    def parts(row_number, column_number, weight):
        row_wave = (2.0 * math.pi / (2 * grid)) * signed(row_number)
        column_wave = (2.0 * math.pi / (2 * grid)) * signed(column_number)
        squared = row_wave * row_wave + column_wave * column_wave
        nonzero = squared > 0.0
        safe = jnp.where(nonzero, squared, 1.0)
        scaled = jnp.sqrt(safe) * thickness
        film = jnp.where(nonzero, (1.0 - jnp.exp(-scaled)) / scaled, 1.0)
        in_plane = (1.0 - film) / safe * weight
        edge = (row_number == grid) | (column_number == grid)
        return (
            in_plane * column_wave * column_wave,
            in_plane * row_wave * row_wave,
            film * weight,
            jnp.where(edge, 0.0, in_plane * column_wave * row_wave),
        )

    def signed(number):
        return jnp.where(number < grid, number, number - 2 * grid).astype(jnp.float32)

    columns = 2 * width
    for block in range(grid // 64):
        spots = slice(64 * block, 64 * block + 64)
        row_number = iota(64, columns, 0) + 64 * block
        lane = iota(64, columns, 1)
        is_sine = lane >= width
        column_number = rank * width + (lane & (width - 1))
        column_number = jnp.where(is_sine & (column_number == 0), grid, column_number)
        column_weight = jnp.where((column_number & (grid - 1)) == 0, 1.0, 2.0)
        weight = column_weight * jnp.where(row_number == 0, 1.0, 2.0) * (-0.25 / (grid * grid))
        found = parts(row_number, column_number, weight)
        for c in range(3):
            tensor_ref[c, spots] = found[c]
        tensor_ref[6, spots] = jnp.where(is_sine, -found[3], found[3])
        if block == 0:
            other = parts(jnp.where(row_number == 0, grid, row_number), column_number, weight)
            found = [jnp.where(row_number == 0, a, b) for a, b in zip(other, found)]
        for c in range(3):
            tensor_ref[3 + c, spots] = found[c]


def split(values):
    high = values.astype(jnp.bfloat16)
    low = (values - high.astype(jnp.float32)).astype(jnp.bfloat16)
    return (high, low)


def multiply_rows(left, table, transposed=False):
    numbers = (((1,), (1 if transposed else 0,)), ((), ()))

    def one(a, b):
        return lax.dot_general(a, b, numbers, preferred_element_type=jnp.float32)

    rows = left[0].shape[0]
    both = one(jnp.concatenate(left, axis=0), table[0])
    return both[:rows] + (both[rows:] + one(left[0], table[1]))


def multiply(table, right):
    columns = right[0].shape[1]
    both = jnp.dot(table[0], jnp.concatenate(right, axis=1), preferred_element_type=jnp.float32)
    rest = jnp.dot(table[1], right[0], preferred_element_type=jnp.float32)
    return both[:, :columns] + (both[:, columns:] + rest)


def exchange_weights(coupling):
    rows, columns = coupling.shape
    place = lax.broadcasted_iota(jnp.int32, coupling.shape, 1)
    own = stiffness * coupling
    right = jnp.where(place < columns - 1, pltpu.roll(coupling, columns - 1, 1), 0.0)
    left = jnp.where(place > 0, pltpu.roll(coupling, 1, 1), 0.0)
    below = pltpu.roll(coupling, rows - 1, 0)
    above = pltpu.roll(coupling, 1, 0)
    return (own * right, own * left, own * below, own * above)


def exchange_of(part, weights):
    rows, columns = part.shape
    right, left, below, above = weights
    total = right * (pltpu.roll(part, columns - 1, 1) - part)
    total = total + left * (pltpu.roll(part, 1, 1) - part)
    total = total + below * (pltpu.roll(part, rows - 1, 0) - part)
    return total + above * (pltpu.roll(part, 1, 0) - part)


def cross(a, b):
    return (a[1] * b[2] - a[2] * b[1], a[2] * b[0] - a[0] * b[2], a[0] * b[1] - a[1] * b[0])


def torque_of(magnet, effective):
    first = cross(magnet, effective)
    second = cross(magnet, first)
    scale = -1.0 / (1.0 + damping * damping)
    return [scale * (a + damping * b) for a, b in zip(first, second)]


def coarse_step(magnet, applied, weights):
    effective = [exchange_of(part, weights) + field for part, field in zip(magnet, applied)]
    effective[2] = effective[2] - magnet[2]
    return [part + FINE * step_time * rate for part, rate in zip(magnet, torque_of(magnet, effective))]


def vmem_call(body, outs, name, scalars=0, scratch=(), cost=10**8):
    whole = pl.BlockSpec(memory_space=pltpu.VMEM)

    def call(*args):
        first = [pl.BlockSpec(memory_space=pltpu.SMEM)] * scalars
        return pl.pallas_call(
            body,
            out_shape=[
                out if isinstance(out, jax.ShapeDtypeStruct) else jax.ShapeDtypeStruct(out, jnp.float32)
                for out in outs
            ],
            in_specs=first + [whole] * (len(args) - scalars),
            out_specs=[whole] * len(outs),
            scratch_shapes=[pltpu.VMEM(shape, jnp.float32) for shape in scratch],
            compiler_params=pltpu.CompilerParams(vmem_limit_bytes=VMEM_LIMIT),
            cost_estimate=pl.CostEstimate(flops=cost, bytes_accessed=10**6, transcendentals=0),
            name=name,
        )(*args)

    return call


def pack_body(reach, state_ref, applied_ref, coupling_ref, own_ref, top_ref, bottom_ref):
    rows = coupling_ref.shape[0]
    for c in range(3):
        own_ref[c] = state_ref[c]
        own_ref[3 + c] = applied_ref[c]
    own_ref[6] = coupling_ref[...]
    for ref, first in ((top_ref, 0), (bottom_ref, rows - reach)):
        for c in range(7):
            ref[c * reach : (c + 1) * reach] = own_ref[c, first : first + reach]
        if 7 * reach < ref.shape[0]:
            ref[7 * reach :] = jnp.zeros_like(ref[7 * reach :])


def pieces(values):
    high = values.astype(jnp.bfloat16)
    rest = values - high.astype(jnp.float32)
    middle = rest.astype(jnp.bfloat16)
    low = (rest - middle.astype(jnp.float32)).astype(jnp.bfloat16)
    return (high, middle, low)


def choose(selection, parts):
    first, second, third = (
        jnp.dot(selection, part, preferred_element_type=jnp.float32) for part in parts
    )
    return first + (second + third)


def build_wide(flipped, reach, state_ref, applied_ref, coupling_ref, before, after, wide_ref):
    rows = coupling_ref.shape[0]
    count = before.shape[0]
    total = wide_ref.shape[1]
    margin = (total - rows) // 2

    def edge_matrix(base):
        row = lax.broadcasted_iota(jnp.int32, (7 * 2 * margin, count), 0)
        column = lax.broadcasted_iota(jnp.int32, (7 * 2 * margin, count), 1)
        field, row = (row // (2 * margin), row % (2 * margin))
        row = jnp.where(row < margin, row, row + rows)
        row = jnp.where(flipped == 1, total - 1 - row, row) - base
        inside = (row >= 0) & (row < reach) & (column == field * reach + row)
        return jnp.where(inside, 1.0, 0.0).astype(jnp.bfloat16)

    row = lax.broadcasted_iota(jnp.int32, (rows, rows), 0)
    column = lax.broadcasted_iota(jnp.int32, (rows, rows), 1)
    row = jnp.where(flipped == 1, rows - 1 - row, row)
    own = jnp.where(row == column, 1.0, 0.0).astype(jnp.bfloat16)
    edges = choose(edge_matrix(margin - reach), pieces(before))
    edges = edges + choose(edge_matrix(margin + rows), pieces(after))
    fields = [state_ref[c] for c in range(3)] + [applied_ref[c] for c in range(3)]
    fields.append(coupling_ref[...])
    for number, field in enumerate(fields):
        place = 2 * margin * number
        wide_ref[number, :margin] = edges[place : place + margin]
        wide_ref[number, margin : margin + rows] = choose(own, pieces(field))
        wide_ref[number, margin + rows :] = edges[place + margin : place + 2 * margin]


def sweep_body(reach, trim, flip_ref, fine_flip_ref, turn_ref, own_ref, *refs):
    own_pair_ref, other_pair_ref, ends_ref, strip_ref, wide_ref = refs
    kept = flip_ref[0] == fine_flip_ref[0]
    before, after = (
        jnp.where(kept, own_pair_ref[i], other_pair_ref[i]) for i in range(2)
    )
    fields = (own_ref.at[0:3], own_ref.at[3:6], own_ref.at[6])
    build_wide(flip_ref[0], reach, *fields, before, after, wide_ref)
    slices, _, rows, _ = ends_ref.shape
    share = rows - 2 * trim
    margin = (wide_ref.shape[1] - slices * share) // 2
    start = pl.multiple_of(turn_ref[0] * share + margin - 8, 8)

    def strip(number):
        return wide_ref[number, pl.ds(start, share + 16)][8 - trim : 8 + share + trim]

    applied = [strip(3 + c) for c in range(3)]
    weights = exchange_weights(strip(6))
    for number, values in enumerate(applied + list(weights)):
        strip_ref[number] = values
    first = [strip(c) for c in range(3)]
    for number in range(slices):
        first = coarse_step(first, applied, weights)
        for c in range(3):
            ends_ref[number, c] = first[c]


def start_body(reach, slices, turn_ref, flip_ref, rank_ref, *refs):
    table_ref, refs = (refs[5], refs[:5] + refs[6:])
    send_refs, (first_ref, around_ref, pair_ref, wide_ref) = (refs[5:-4], refs[-4:])
    pair_ref[0] = refs[3][...]
    pair_ref[1] = refs[4][...]
    turn = turn_ref[0]
    build_wide(flip_ref[0], reach, *refs[:3], refs[3][...], refs[4][...], wide_ref)
    rows = first_ref.shape[1]
    margin = (wide_ref.shape[1] - rows) // 2
    kept = slice(margin, margin + rows)
    weights = exchange_weights(wide_ref[6])
    applied = [wide_ref[3 + c] for c in range(3)]
    for number, values in enumerate(applied + list(weights)):
        around_ref[number] = values[kept]
    for c in range(3):
        first_ref[c] = wide_ref[c, kept]
    for number in range(1, slices):
        @pl.when(turn >= number)
        def step():
            magnet = coarse_step([wide_ref[c] for c in range(3)], applied, weights)
            for c in range(3):
                wide_ref[c] = magnet[c]
                first_ref[c] = magnet[c][kept]
    send_rows([first_ref[c] for c in range(3)], rank_ref[0], (table_ref[0], table_ref[1]), send_refs)


def first_is_end(rank):
    return (rank & 1) == jnp.where(rank >= 4, 1, 0)


def send_rows(magnet, rank, table, out_refs):
    rows, grid = magnet[0].shape
    width = out_refs[0].shape[1]
    block = split(jnp.concatenate(magnet, axis=0))
    spectrum = multiply_rows(block, table)
    at_end = first_is_end(rank)
    for slot, out_ref in enumerate(out_refs):
        out_ref[: 3 * rows] = spectrum[:, slot * width : (slot + 1) * width]
        if out_ref.shape[0] > 3 * rows:
            which = at_end if slot == 1 else jnp.logical_not(at_end)
            place = 3 * rows
            for part in magnet:
                edge = jnp.where(which, part[rows - 1 :], part[:1])
                for start in range(0, grid, width):
                    out_ref[place : place + 1] = edge[:, start : start + width]
                    place += 1
            rest = out_ref.shape[0] - place
            out_ref[place:] = jnp.zeros((rest, width), jnp.float32)


def edge_rows(rank, near_ref, far_ref, middle_ref, rows):
    width = near_ref.shape[1]
    count = rows * 3
    at_end = first_is_end(rank)
    outer = (rank == 0) | (rank == 7)
    central = (rank == 3) | (rank == 4)
    grid = 4 * width
    pairs = []
    for c in range(3):
        near, far, middle = (
            jnp.concatenate(
                [
                    ref[count + c * (grid // width) + j : count + c * (grid // width) + j + 1]
                    for j in range(grid // width)
                ],
                axis=1,
            )
            for ref in (near_ref, far_ref, middle_ref)
        )
        other = jnp.where(central, middle, far)
        start = jnp.where(at_end, jnp.where(outer, jnp.zeros_like(far), far), near)
        pairs.append((start, jnp.where(at_end, near, other)))
    return pairs


def spectrum_body(peers, rows, base_ref, *refs):
    in_refs, refs = (refs[:peers], refs[peers:])
    tensor_ref, cos_ref, sin_ref, back_cos_ref, back_sin_ref = refs[:5]
    out_refs = refs[5 : 5 + peers]
    front_ref, back_ref = refs[5 + peers :]
    width = in_refs[0].shape[1]
    half = peers // 2

    def part(slot, c):
        return in_refs[slot][c * rows : (c + 1) * rows]

    def fold(sign):
        return jnp.concatenate(
            [
                jnp.concatenate(
                    [part(p, c) + sign * part(peers - 1 - p, c) for p in range(half)], axis=0
                )
                for c in range(3)
            ],
            axis=1,
        )

    even = multiply((cos_ref[0], cos_ref[1]), split(fold(1.0)))
    odd = multiply((sin_ref[0], sin_ref[1]), split(fold(-1.0)))
    even_x, even_y, even_z = (even[:, c * width : (c + 1) * width] for c in range(3))
    odd_x, odd_y, odd_z = (odd[:, c * width : (c + 1) * width] for c in range(3))
    mixed = tensor_ref[6]

    def turned(values):
        return mixed * pltpu.roll(values, width // 2, 1)

    even_out = jnp.concatenate(
        [
            tensor_ref[0] * even_x - turned(odd_y),
            tensor_ref[1] * even_y - turned(odd_x),
            tensor_ref[2] * even_z,
        ],
        axis=1,
    )
    odd_out = jnp.concatenate(
        [
            tensor_ref[3] * odd_x + turned(even_y),
            tensor_ref[4] * odd_y + turned(even_x),
            tensor_ref[5] * odd_z,
        ],
        axis=1,
    )
    even_rows = multiply((back_cos_ref[0], back_cos_ref[1]), split(even_out))
    odd_rows = multiply((back_sin_ref[0], back_sin_ref[1]), split(odd_out))
    front_ref[...] = even_rows + odd_rows
    back_ref[...] = even_rows - odd_rows
    base = base_ref[0]
    for p in range(half):
        span = pl.ds(pl.multiple_of((base ^ p) * rows, 8), rows)
        for c in range(3):
            kept = slice(c * rows, (c + 1) * rows)
            out_refs[p][kept] = front_ref[span, c * width : (c + 1) * width]
            out_refs[peers - 1 - p][kept] = back_ref[span, c * width : (c + 1) * width]


def exchange_inside(part, weights, start, end):
    rows, columns = part.shape
    right, left, below, above = weights
    row = lax.broadcasted_iota(jnp.int32, part.shape, 0)
    following = jnp.where(row == rows - 1, end, pltpu.roll(part, rows - 1, 0))
    preceding = jnp.where(row == 0, start, pltpu.roll(part, 1, 0))
    total = right * (pltpu.roll(part, columns - 1, 1) - part)
    total = total + left * (pltpu.roll(part, 1, 1) - part)
    total = total + below * (following - part)
    return total + above * (preceding - part)


def field_rates(rank, in_refs, edge_refs, magnet, around_ref, table):
    rows = magnet[0].shape[0]
    spectrum = jnp.concatenate([ref[...] for ref in in_refs], axis=1)
    demag = multiply_rows(split(spectrum), table, transposed=True)
    edges = edge_rows(rank, *edge_refs, rows)
    weights = [around_ref[3 + c] for c in range(4)]
    effective = [
        exchange_inside(magnet[c], weights, *edges[c])
        + demag[c * rows : (c + 1) * rows]
        + around_ref[c]
        for c in range(3)
    ]
    return torque_of(magnet, effective)


def predict_body(peers, rank_ref, *refs):
    in_refs, edge_refs, refs = (refs[:peers], refs[peers : peers + 3], refs[peers + 3 :])
    state_ref, around_ref, table_ref = refs[:3]
    send_refs, (predicted_ref, base_ref) = (refs[3 : 3 + peers], refs[3 + peers :])
    rank = rank_ref[0]
    table = (table_ref[0], table_ref[1])
    magnet = [state_ref[c] for c in range(3)]
    rates = field_rates(rank, in_refs, edge_refs, magnet, around_ref, table)
    predicted = [part + step_time * rate for part, rate in zip(magnet, rates)]
    send_rows(predicted, rank, table, send_refs)
    for c in range(3):
        predicted_ref[c] = predicted[c]
        base_ref[c] = magnet[c] + 0.5 * step_time * rates[c]


def correct_body(peers, rank_ref, *refs):
    in_refs, edge_refs, refs = (refs[:peers], refs[peers : peers + 3], refs[peers + 3 :])
    state_ref, base_ref, around_ref, table_ref = refs[:4]
    send_refs, following_ref = (refs[4 : 4 + peers], refs[4 + peers])
    rank = rank_ref[0]
    table = (table_ref[0], table_ref[1])
    magnet = [state_ref[c] for c in range(3)]
    rates = field_rates(rank, in_refs, edge_refs, magnet, around_ref, table)
    following = [base_ref[c] + 0.5 * step_time * rates[c] for c in range(3)]
    send_rows(following, rank, table, send_refs)
    for c in range(3):
        following_ref[c] = following[c]


def end_body(peers, share, trim, slices, rank_ref, number_ref, *refs):
    in_refs, edge_refs, refs = (refs[:peers], refs[peers : peers + 3], refs[peers + 3 :])
    state_ref, base_ref, around_ref, table_ref = refs[:4]
    strip_refs, margin_refs, end_ref = (refs[4 : 4 + slices], refs[4 + slices : -1], refs[-1])
    rank, number = (rank_ref[0], number_ref[0])
    magnet = [state_ref[c] for c in range(3)]
    rows = magnet[0].shape[0]
    table = (table_ref[0], table_ref[1])
    rates = field_rates(rank, in_refs, edge_refs, magnet, around_ref, table)
    blank = jnp.zeros((trim, magnet[0].shape[1]), jnp.float32)
    for c in range(3):
        end_ref[c, :trim] = blank
        end_ref[c, trim + rows :] = blank
        end_ref[c, trim : trim + rows] = base_ref[c] + 0.5 * step_time * rates[c]
    central = (rank == 3) | (rank == 4)
    for t in range(slices):
        start = pl.multiple_of((number ^ t) * share, 8)
        ending = number == t
        for c in range(3):
            strip_refs[t][c] = end_ref[c, pl.ds(start, strip_refs[t].shape[1])]
            for i in range(trim):
                head = end_ref[c, trim + i : trim + i + 1]
                tail = end_ref[c, rows + i : rows + i + 1]
                mirrored = end_ref[c, trim + rows - 1 - i : trim + rows - i]
                tail = jnp.where(central, mirrored, tail)
                margin_refs[t][c * trim + i : c * trim + i + 1] = jnp.where(ending, tail, head)
        margin_refs[t][3 * trim :] = jnp.zeros_like(margin_refs[t][3 * trim :])


def finish_body(slices, trim, turn_ref, block_ref, *refs):
    in_refs, margin_refs, refs = (refs[:slices], refs[slices : 2 * slices], refs[2 * slices :])
    coarse_ref, strip_ref, out_refs = (refs[0], refs[1], refs[2 : slices + 2])
    fine_ref, edge_ref, end_ref = refs[slices + 2 :]
    turn, block = (turn_ref[0], block_ref[0])
    rows = fine_ref.shape[2]
    share = rows - 2 * trim
    central = (block == 3) | (block == 4)
    straight = (turn == 0) | central
    for t in range(slices):
        fine_ref[turn ^ t] = in_refs[t][...]
        edge_ref[jnp.where(straight, t, t ^ 3)] = margin_refs[t][...]
    row = lax.broadcasted_iota(jnp.int32, (rows, fine_ref.shape[3]), 0)
    patched = ((turn == 0) & (row < trim)) | ((turn == slices - 1) & (row >= rows - trim))
    blank = jnp.zeros((share, fine_ref.shape[3]), jnp.float32)

    def fine(number, c):
        edge = edge_ref[number, c * trim : (c + 1) * trim]
        return jnp.where(patched, jnp.concatenate([edge, blank, edge], axis=0), fine_ref[number, c])

    applied = [strip_ref[c] for c in range(3)]
    weights = [strip_ref[3 + c] for c in range(4)]
    magnet = []
    for number in range(slices):
        first = [coarse_ref[number, c] for c in range(3)]
        ahead = coarse_step(magnet, applied, weights) if number > 0 else first
        magnet = [ahead[c] + (fine(number, c) - first[c]) for c in range(3)]
        for c in range(3):
            end_ref[number, c] = magnet[c][trim : trim + share]
    for t in range(slices):
        out_refs[t][...] = end_ref[turn ^ t]


def gather_body(slices, turn_ref, flip_ref, *refs):
    in_refs, out_ref = (refs[:slices], refs[slices])
    turn, flipped = (turn_ref[0], flip_ref[0])
    share = in_refs[0].shape[1]
    row = lax.broadcasted_iota(jnp.int32, (share, share), 0)
    column = lax.broadcasted_iota(jnp.int32, (share, share), 1)
    row = jnp.where(flipped == 1, share - 1 - row, row)
    matrix = jnp.where(row == column, 1.0, 0.0).astype(jnp.bfloat16)
    for t in range(slices):
        strip = turn ^ t
        strip = jnp.where(flipped == 1, slices - 1 - strip, strip)
        span = pl.ds(pl.multiple_of(strip * share, 8), share)
        for c in range(3):
            out_ref[c, span] = choose(matrix, pieces(in_refs[t][c]))


def shards_by_block(initial_state, applied_field, coupling):
    rows, _, grid = initial_state.shape
    group = ("core", "z_low", "y")
    peers = 8
    slices = 4
    margin, trim, reach = (8, 4, 4)
    width = grid // peers
    space = ("z_high", "z_low", "y")
    blocks = 8
    def scalar(value):
        return value.astype(jnp.int32).reshape(1)

    rank = lax.axis_index(group)
    half = lax.axis_index("z_high")
    turn = lax.axis_index(("x", "core"))
    number = 2 * lax.axis_index("x") + half
    base = jnp.where(rank < peers // 2, rank, peers - 1 - rank)
    scalars = (rank, half, lax.axis_index("core"), turn, number, base, lax.axis_index(space))
    rank, native_flip, fine_flip, turn, number, base, block = lax.optimization_barrier(
        tuple(value.astype(jnp.int32).reshape(1) for value in scalars)
    )

    state_in = jnp.transpose(initial_state, (1, 0, 2))
    applied_in = jnp.transpose(applied_field, (1, 0, 2))
    edge_shape = (-(-7 * reach // 8) * 8, grid)
    native, top, bottom = vmem_call(
        functools.partial(pack_body, reach), [(7, rows, grid), edge_shape, edge_shape], "pack"
    )(state_in, applied_in, coupling)

    def trade(values):
        return lax.ppermute(values, ("core", "z_high"), [(0, 0), (1, 2), (2, 1), (3, 3)])

    def edge_route(step):
        route = []
        for core in range(2):
            for block in range(blocks):
                following = block + step
                if 0 <= following < blocks:
                    target = (following // 4, core, following % 4)
                    route.append((8 * core + block, 8 * target[0] + 4 * target[1] + target[2]))
        return route

    everywhere = ("core",) + space
    before = lax.ppermute(bottom, everywhere, edge_route(1))
    after = lax.ppermute(top, everywhere, edge_route(-1))
    own = (trade(state_in), trade(applied_in), trade(coupling))

    def pair(*shape):
        return jax.ShapeDtypeStruct((2,) + shape, jnp.bfloat16)

    back_rows = grid // 2
    row_table, *column_tables, tensor = vmem_call(
        functools.partial(tables_body, peers, 0),
        [pair(grid, 2 * grid)]
        + [pair(grid, grid // 2)] * 2
        + [pair(back_rows, grid)] * 2
        + [(7, grid, 2 * width)],
        "tables",
        scalars=1,
    )(rank)

    state_shape = (3, rows, grid)
    wide_shape = (7, rows + 2 * margin, grid)
    lanes = 2 * width
    extra = -(-3 * grid // lanes // 8) * 8
    near, far, middle = (1, 3, 7)
    send_shapes = [
        (3 * rows + (extra if slot in (near, far, middle) else 0), lanes) for slot in range(peers)
    ]
    *sent, state, around, pair = vmem_call(
        functools.partial(start_body, reach, slices),
        send_shapes + [state_shape, (7, rows, grid), (2,) + edge_shape],
        "start",
        scalars=3,
        scratch=[wide_shape],
    )(number, fine_flip, rank, *own, before, after, row_table)

    def spread(slots):
        return [slots[0]] + [
            lax.ppermute(slots[k], group, [(i, i ^ k) for i in range(peers)])
            for k in range(1, peers)
        ]

    def demag_blocks(received):
        return received, vmem_call(
            functools.partial(spectrum_body, peers, rows),
            [(3 * rows, lanes)] * peers,
            "spectrum",
            scalars=1,
            scratch=[(back_rows, 3 * lanes)] * 2,
            cost=10**9,
        )(base, *received, tensor, *column_tables)

    def complete(received, blocks_back):
        return spread(blocks_back) + [received[slot] for slot in (near, far, middle)]

    share = rows // slices
    strip_shape = (3, share + 2 * trim, grid)
    swap = [(0, 1), (1, 0)]
    coarse_ends, strip = vmem_call(
        functools.partial(sweep_body, reach, trim),
        [(slices,) + strip_shape, (7,) + strip_shape[1:]],
        "sweep",
        scalars=3,
        scratch=[wide_shape],
    )(
        native_flip,
        fine_flip,
        turn,
        native,
        pair,
        lax.ppermute(pair, "core", swap),
    )
    for repeat in range(FINE):
        received = spread(sent)
        received = complete(*demag_blocks(received))
        *sent, predicted, start = vmem_call(
            functools.partial(predict_body, peers), send_shapes + [state_shape] * 2, "predict", scalars=1, cost=10**9
        )(rank, *received, state, around, row_table)
        received = complete(*demag_blocks(spread(sent)))
        if repeat == 0:
            received[4], coarse_ends = lax.optimization_barrier((received[4], coarse_ends))
        if repeat < FINE - 1:
            *sent, state = vmem_call(
                functools.partial(correct_body, peers), send_shapes + [state_shape], "correct", scalars=1, cost=10**9
            )(rank, *received, predicted, start, around, row_table)
    swap = [(0, 1), (1, 0)]
    margin_shape = (-(-3 * trim // 8) * 8, grid)
    ending = vmem_call(
        functools.partial(end_body, peers, share, trim, slices),
        [strip_shape] * slices + [margin_shape] * slices,
        "end",
        scalars=2,
        scratch=[(3, rows + 2 * trim, grid)],
    )(rank, number, *received, predicted, start, around, row_table)
    strips, margins = (ending[:slices], ending[slices:])

    def margin_route(t):
        route = []
        for s in range(blocks):
            if s in (3, 4):
                beyond = (7 - s, slices - 1)
            else:
                beyond = (s + 1 if s < 4 else s - 1, 0)
            ahead = s - 1 if s < 4 else s + 1
            for n, (block_to, strip) in ((t, beyond), (t ^ 3, (ahead, slices - 1))):
                if 0 <= block_to < blocks:
                    source = 16 * (n // 2) + 8 * (s // 4) + 4 * (n % 2) + s % 4
                    route.append((source, 8 * strip + block_to))
        return route

    def strip_route(t):
        route = []
        for i in range(8):
            x, core, z = (i // 4, i // 2 % 2, i % 2)
            route.append((i, 4 * (x ^ (t // 2)) + 2 * (z ^ (t % 2)) + core))
        return route

    strips = [
        lax.ppermute(strips[t], ("x", "core", "z_high"), strip_route(t)) for t in range(slices)
    ]
    margins = [
        lax.ppermute(margins[t], ("x",) + everywhere, margin_route(t)) for t in range(slices)
    ]
    ends = vmem_call(
        functools.partial(finish_body, slices, trim),
        [(3, share, grid)] * slices,
        "finish",
        scalars=2,
        scratch=[
            (slices,) + strip_shape,
            (slices,) + margin_shape,
            (slices, 3, share, grid),
        ],
    )(turn, block, *strips, *margins, coarse_ends, strip)
    ends = [ends[0]] + [
        lax.ppermute(ends[t], ("x", "core"), [(i, i ^ t) for i in range(slices)])
        for t in range(1, slices)
    ]
    (result,) = vmem_call(
        functools.partial(gather_body, slices), [(3, rows, grid)], "gather", scalars=2
    )(turn, native_flip, *ends)
    return jnp.transpose(result, (1, 0, 2))[None]


def fits_blocks(mesh):
    return mesh.shape["tm"] == 4 and mesh.shape["space"] == 8


def solution(mesh):
    if not fits_blocks(mesh):
        in_specs = (P("space", None, None), P("space", None, None), P("space", None))
        out_specs = P("tm", "space", None, None)
        return jax.shard_map(
            shards, mesh=mesh, in_specs=in_specs, out_specs=out_specs, check_vma=False
        )
    fine_mesh = Mesh(
        mesh.devices.reshape(2, 2, 2, 2, 2), ("x", "core", "z_high", "z_low", "y")
    )
    space = ("z_high", "z_low", "y")
    in_specs = (P(space, None, None), P(space, None, None), P(space, None))
    out_specs = P(("x", "core"), space, None, None)
    return jax.shard_map(
        shards_by_block, mesh=fine_mesh, in_specs=in_specs, out_specs=out_specs, check_vma=False
    )
```
